32 devices in a mesh: gx: 2 (over x), gy: 4 (over y, core), gz: 4 (over z).
Axes of the slice: x: 2, y: 2, z: 4, core: 2. Of those that a mesh axis runs over, the one named last changes fastest.
Arguments:
- ambient_motion_array: float32 [3, 16, 256, 512], P(None, 'gx', 'gy', 'gz'), may hold values from -6 to 6
- ambient_scalar_trio: float32 [3, 16, 256, 512], P(None, 'gx', 'gy', 'gz'), may hold values from 0.2 to 1
- droplet_local_position: float32 [3, 32768], P(None, ('gx', 'gy', 'gz')), may hold values from -0.5 to 0.5
- droplet_motion_array: float32 [3, 32768], P(None, ('gx', 'gy', 'gz')), may hold values from -6 to 6
- droplet_heat_level: float32 [32768], P(('gx', 'gy', 'gz')), may hold values from 0.3 to 0.9
- droplet_size_quadratic: float32 [32768], P(('gx', 'gy', 'gz')), may hold values from 0.25 to 4
- local_i_position: int32 [32768], P(('gx', 'gy', 'gz')), may hold values from 0 to 7
- local_j_position: int32 [32768], P(('gx', 'gy', 'gz')), may hold values from 0 to 63
- local_k_position: int32 [32768], P(('gx', 'gy', 'gz')), may hold values from 0 to 127
- active_group_tally: int32 [32], P(('gx', 'gy', 'gz')), may hold values from 1 to 8, as said below
Outputs:
- gas_source: float32 [5, 16, 256, 512], P(None, 'gx', 'gy', 'gz')
- parcel_state: float32 [5, 32768], P(None, ('gx', 'gy', 'gz'))
The draws below stay inside these ranges and needn't reach their ends.
Inputs may be any that keep to these rules, and one draw needn't show every extreme that they name: `active_group_tally`: tiles of a brick are live from the first one on; in every draw some brick has all 8 tiles live.
All inputs are finite; a program needn't handle non-finite values.
Results may differ from the reference program's by a relative error of at most 0.0003.
Values sent between devices are 32-bit elements; how exact they have to be, the bound alone decides.
A program may use at most 128 MiB of HBM per device.

```python
import math
import jax
import jax.numpy as jnp
from jax import lax

CX = 8
CY = 64
CZ = 128
TILE = 128
TILE_CAP = 8
PAR_DEV = 1024
BRICKS = 32
GRID_EXTENT_I = 16
GRID_EXTENT_J = 256
GRID_EXTENT_K = 512
SPRAY_CAPACITY_N = 32768
N_GY = 4
N_GZ = 4


def draw_active_group_tally(key, part):
    key_base, key_core, key_pick = jax.random.split(key, 3)
    lowest = max(1, TILE_CAP // 4)
    highest = max(lowest + 1, TILE_CAP // 2 + 1)
    base_tiles = jax.random.randint(key_base, (BRICKS,), lowest, highest)
    dense_brick = jax.random.randint(key_core, (BRICKS,), 0, 8) == 0
    chosen = jax.random.randint(key_pick, (), 0, BRICKS)
    dense_brick = dense_brick | (jnp.arange(BRICKS) == chosen)
    return jnp.where(dense_brick, TILE_CAP, base_tiles).astype(jnp.int32)


def plant(array, stream_key, low, top_value):
    dims = array.shape
    spot = [jax.random.randint(jax.random.fold_in(stream_key, axis), (), 0, dims[axis]) for axis in range(len(dims))]
    array = array.at[tuple(spot)].set(low)
    longest = dims.index(max(dims))
    spot[longest] = (spot[longest] + 1) % dims[longest]
    return array.at[tuple(spot)].set(top_value)


def block_scale(stream_key, shape, cuts, smallest, top_value):
    gain = 1.0
    for position, parts in cuts:
        heights = jax.random.uniform(jax.random.fold_in(jax.random.fold_in(stream_key, 6), position), (parts,), jnp.float32, smallest / len(cuts), top_value / len(cuts))
        gain = gain * jnp.repeat(jnp.exp(heights), shape[position] // parts).reshape((-1,) + (1,) * (len(shape) - 1 - position))
    return gain


def normal_values(stream_key, dims, deviation, limit, pieces=(), held_as=jnp.bfloat16):
    entries = jax.random.normal(stream_key, dims, jnp.float32) * deviation
    if len(pieces) > 0:
        entries = block_scale(stream_key, dims, pieces, -0.22, 0.18) * entries
    return jnp.clip(entries, min=-limit, max=limit).astype(held_as)


def setup_inputs(seed: int = 0) -> dict:
    key_of = jax.random.split(jax.random.key(seed), 11)
    ambient_motion_array = normal_values(key_of[0], (3, GRID_EXTENT_I, GRID_EXTENT_J, GRID_EXTENT_K), 1.0, 6.0, ((1, 2), (2, 4), (3, 4)), jnp.float32)
    ambient_scalar_trio = jnp.clip(0.2 + 0.8 * jax.random.uniform(key_of[1], (3, GRID_EXTENT_I, GRID_EXTENT_J, GRID_EXTENT_K), jnp.float32) ** block_scale(key_of[1], (3, GRID_EXTENT_I, GRID_EXTENT_J, GRID_EXTENT_K), ((1, 2), (2, 4), (3, 4)), -0.2, 0.2), 0.2, 1.0)
    droplet_local_position = jnp.clip(jax.random.uniform(key_of[2], (3, SPRAY_CAPACITY_N), jnp.float32, -0.5, 0.5) * block_scale(key_of[2], (3, SPRAY_CAPACITY_N), ((1, 32),), -0.4, 0.0), -0.5, 0.5)
    droplet_motion_array = normal_values(key_of[3], (3, SPRAY_CAPACITY_N), 1.0, 6.0, ((1, 32),), jnp.float32)
    droplet_heat_level = jnp.clip(0.3 + 0.59999996 * jax.random.uniform(key_of[4], (SPRAY_CAPACITY_N,), jnp.float32) ** block_scale(key_of[4], (SPRAY_CAPACITY_N,), ((0, 32),), -0.2, 0.2), 0.3, 0.9)
    droplet_size_quadratic = jnp.clip(jnp.exp(math.log(4.0) - 2.7725887 * jax.random.uniform(key_of[5], (SPRAY_CAPACITY_N,), jnp.float32) ** block_scale(key_of[5], (SPRAY_CAPACITY_N,), ((0, 32),), -0.2, 0.2)), 0.25, 4.0)
    local_i_position = plant(jax.random.randint(key_of[6], (SPRAY_CAPACITY_N,), 0, CX), jax.random.fold_in(key_of[6], 1), 0, CX - 1).astype(jnp.int32)
    local_j_position = plant(jax.random.randint(key_of[7], (SPRAY_CAPACITY_N,), 0, CY), jax.random.fold_in(key_of[7], 1), 0, CY - 1).astype(jnp.int32)
    local_k_position = plant(jax.random.randint(key_of[8], (SPRAY_CAPACITY_N,), 0, CZ), jax.random.fold_in(key_of[8], 1), 0, CZ - 1).astype(jnp.int32)
    active_group_tally = draw_active_group_tally(jax.random.fold_in(key_of[10], 71), 0)
    return {"ambient_motion_array": ambient_motion_array, "ambient_scalar_trio": ambient_scalar_trio, "droplet_local_position": droplet_local_position, "droplet_motion_array": droplet_motion_array, "droplet_heat_level": droplet_heat_level, "droplet_size_quadratic": droplet_size_quadratic, "local_i_position": local_i_position, "local_j_position": local_j_position, "local_k_position": local_k_position, "active_group_tally": active_group_tally}


step_time = 0.25
evap_rate = 1.0
heat_rate = 2.0
boiling_energy_drain = 0.3

def tent_weights(offset_values):
    shifts = jnp.arange(3, dtype=jnp.float32) - 1.0
    return jnp.maximum(0.0, 1.0 - jnp.abs(offset_values[:, None, :] - shifts[None, :, None]))

def integrate_droplets(sampled_ambient_quantities, sampled_motion, sampled_heat_level, diam_quadratic_entry):
    ambient_motion = sampled_ambient_quantities[0:3]
    ambient_heat_level = sampled_ambient_quantities[3]
    ambient_moisture = sampled_ambient_quantities[4]
    ambient_rho_level = sampled_ambient_quantities[5]
    drag_ratio = step_time / (0.5 * diam_quadratic_entry)
    revised_speed = (sampled_motion + drag_ratio * ambient_motion) / (1.0 + drag_ratio)
    blob_weight_kilos = diam_quadratic_entry * jnp.sqrt(diam_quadratic_entry)
    vapour_equilibrium_share = jnp.exp(4.0 * (sampled_heat_level - 1.0))
    decay_multiplier = step_time * evap_rate * ambient_rho_level * (vapour_equilibrium_share - ambient_moisture)
    next_width_power = diam_quadratic_entry - decay_multiplier
    revised_weight = next_width_power * jnp.sqrt(next_width_power)
    conduction_intensity = step_time * heat_rate * ambient_rho_level / diam_quadratic_entry
    fresh_heat_level = (sampled_heat_level + conduction_intensity * ambient_heat_level) / (1.0 + conduction_intensity) - boiling_energy_drain * decay_multiplier / diam_quadratic_entry
    momentum_energy_deposits = jnp.concatenate([blob_weight_kilos[None] * (sampled_motion - revised_speed), (blob_weight_kilos * (sampled_heat_level - fresh_heat_level))[None], (blob_weight_kilos - revised_weight)[None]], axis=0)
    fresh_droplet_entry = jnp.concatenate([revised_speed, fresh_heat_level[None], next_width_power[None]], axis=0)
    return (fresh_droplet_entry, momentum_energy_deposits)

def reference(ambient_motion_array, ambient_scalar_trio, droplet_local_position, droplet_motion_array, droplet_heat_level, droplet_size_quadratic, local_i_position, local_j_position, local_k_position, active_group_tally):
    maximum_droplets_held = droplet_heat_level.shape[0]
    slot_id = jnp.arange(maximum_droplets_held, dtype=jnp.int32)
    brick_id = slot_id // PAR_DEV
    live_slot = slot_id % PAR_DEV // TILE < active_group_tally[brick_id]
    glob_x = brick_id // (N_GY * N_GZ) * CX + local_i_position
    glob_y = brick_id // N_GZ % N_GY * CY + local_j_position
    glob_z = brick_id % N_GZ * CZ + local_k_position
    quantity_bundle = jnp.concatenate([ambient_motion_array, ambient_scalar_trio], axis=0).reshape(6, -1)
    tent_table = tent_weights(droplet_local_position)
    vertex_weightings = jnp.arange(27, dtype=jnp.int32)
    cell_total = GRID_EXTENT_I * GRID_EXTENT_J * GRID_EXTENT_K

    def locate(stencil):
        pos_x = glob_x + stencil // 9 - 1
        pos_y = glob_y + stencil // 3 % 3 - 1
        pos_z = glob_z + stencil % 3 - 1
        inside = (pos_x >= 0) & (pos_x < GRID_EXTENT_I) & (pos_y >= 0) & (pos_y < GRID_EXTENT_J) & (pos_z >= 0) & (pos_z < GRID_EXTENT_K)
        flat_idx = (jnp.clip(pos_x, 0, GRID_EXTENT_I - 1) * GRID_EXTENT_J + jnp.clip(pos_y, 0, GRID_EXTENT_J - 1)) * GRID_EXTENT_K + jnp.clip(pos_z, 0, GRID_EXTENT_K - 1)
        weight = tent_table[0, stencil // 9] * tent_table[1, stencil // 3 % 3] * tent_table[2, stencil % 3]
        weight = jnp.where(inside, weight, 0.0)
        return (flat_idx.astype(jnp.int32), weight, inside)

    def sample_routine(running, stencil):
        flat_idx, weight, inside = locate(stencil)
        return (running + weight[None] * quantity_bundle[:, flat_idx], None)
    sampled_ambient_quantities = lax.scan(sample_routine, jnp.zeros((6, maximum_droplets_held), jnp.float32), vertex_weightings)[0]
    fresh_droplet_entry, momentum_energy_deposits = integrate_droplets(sampled_ambient_quantities, droplet_motion_array, droplet_heat_level, droplet_size_quadratic)
    momentum_energy_deposits = jnp.where(live_slot[None], momentum_energy_deposits, 0.0)

    def deposit_step(running, stencil):
        flat_idx, weight, inside = locate(stencil)
        target = jnp.where(inside, flat_idx, cell_total).astype(jnp.int32)
        return (running.at[:, target].add(weight[None] * momentum_energy_deposits, mode='drop'), None)
    deposit = lax.scan(deposit_step, jnp.zeros((5, cell_total), jnp.float32), vertex_weightings)[0]
    forwarded_carry = jnp.concatenate([droplet_motion_array, droplet_heat_level[None], droplet_size_quadratic[None]], axis=0)
    parcel_state = jnp.where(live_slot[None], fresh_droplet_entry, forwarded_carry)
    return (deposit.reshape(5, GRID_EXTENT_I, GRID_EXTENT_J, GRID_EXTENT_K), parcel_state)
```

```python
import functools

import jax
import jax.numpy as jnp
from jax import lax
from jax.experimental import pallas as pl
from jax.experimental.pallas import tpu as pltpu
from jax.sharding import PartitionSpec as P

TILE = 128
AXES = ("gx", "gy", "gz")
MESH = pl.DeviceIdType.MESH
F32 = jnp.float32
BF16 = jnp.bfloat16

step_time = 0.25
evap_rate = 1.0
heat_rate = 2.0
boiling_energy_drain = 0.3

X_MOVES = ((1, 0, 0, 0), (-1, 0, 0, 1))
Y_MOVES = ((0, 1, 0, 0), (0, -1, 0, 1))
XY_MOVES = ((1, 1, 0, 0), (1, -1, 0, 1), (-1, 1, 0, 2), (-1, -1, 0, 3))
Z_MOVES = ((0, 0, 1, 0), (0, 0, -1, 1))


def split(value):
    high = value.astype(BF16)
    return high, (value - high.astype(F32)).astype(BF16)


def nn(a, b):
    return lax.dot_general(a, b, (((1,), (0,)), ((), ())), preferred_element_type=F32)


def nt(a, b):
    return lax.dot_general(a, b, (((1,), (1,)), ((), ())), preferred_element_type=F32)


def tn(a, b):
    return lax.dot_general(a, b, (((0,), (0,)), ((), ())), preferred_element_type=F32)


def pair_weights(offset):
    lower = jnp.where(offset < 0.0, -1.0, 0.0)
    first = jnp.maximum(0.0, 1.0 - jnp.abs(offset - lower))
    second = jnp.maximum(0.0, 1.0 - jnp.abs(offset - (lower + 1.0)))
    return first, second, jnp.where(offset < 0.0, -1, 0)


def kernel(
    counts,
    vel,
    sca,
    pos_hbm,
    mot_hbm,
    heat_hbm,
    size_hbm,
    li_hbm,
    lj_hbm,
    lk_hbm,
    tally,
    dep,
    state,
    dxr,
    dyr,
    dxyr,
    fields,
    ft_hi,
    ft_lo,
    w_hi,
    w_lo,
    line,
    src_hi,
    src_lo,
    sampled,
    xh,
    yh,
    xyh,
    zh,
    ys,
    xys,
    zs,
    dxs,
    dys,
    dxys,
    dzs,
    dzr,
    pos,
    mot,
    heat,
    size,
    li,
    lj,
    lk,
    load_sem,
    send_sem,
    recv_sem,
):
    ci, cj, ck = vel.shape[1:]
    slots = heat.shape[1]
    inner = ci * cj
    planes = w_hi.shape[0]
    outer = planes - inner
    y_row = 2 * cj
    xy_row = y_row + 2 * ci
    me = [lax.axis_index(axis) for axis in AXES]

    def exists(move, sign):
        good = None
        for d in range(3):
            step = sign * move[d]
            if step == 1:
                test = me[d] < counts[d] - 1
            elif step == -1:
                test = me[d] > 0
            else:
                continue
            good = test if good is None else jnp.logical_and(good, test)
        return good

    def peer(move):
        return tuple(lax.rem(me[d] + move[d] + counts[d], counts[d]) for d in range(3))

    moves = X_MOVES + Y_MOVES + XY_MOVES + Z_MOVES

    class Message:
        def __init__(self, number, move, src, dst):
            self.move = move
            self.dst = dst
            self.copy = pltpu.make_async_remote_copy(
                src_ref=src,
                dst_ref=dst,
                send_sem=send_sem.at[number],
                recv_sem=recv_sem.at[number],
                device_id=peer(move),
                device_id_type=MESH,
            )

        def start(self):
            @pl.when(exists(self.move, 1))
            def _():
                self.copy.start()

        def blank(self):
            @pl.when(jnp.logical_not(exists(self.move, -1)))
            def _():
                self.dst[...] = jnp.zeros(self.dst.shape, F32)

        def arrive(self):
            @pl.when(exists(self.move, -1))
            def _():
                self.copy.wait_recv()

        def leave(self):
            @pl.when(exists(self.move, 1))
            def _():
                self.copy.wait_send()

    x_in, y_in, z_in, x_out, xy_out, z_out = [], [], [], [], [], []
    number = 0

    def add(group, move, src, dst):
        nonlocal number
        group.append(Message(number, move, src, dst))
        number += 1

    for move in X_MOVES:
        row = ci - 1 if move[0] > 0 else 0
        add(x_in, move, vel.at[:, row], xh.at[move[3], 0:3])
        add(x_in, move, sca.at[:, row], xh.at[move[3], 3:6])
    for move in Y_MOVES:
        add(y_in, move, ys.at[move[3]], yh.at[move[3]])
    for move in XY_MOVES:
        add(y_in, move, xys.at[move[3]], xyh.at[move[3]])
    for move in Z_MOVES:
        add(z_in, move, zs.at[move[3]], zh.at[move[3]])
    for move in Z_MOVES:
        add(z_out, move, dzs.at[move[3]], dzr.at[move[3]])
    for move in X_MOVES:
        add(x_out, move, dxs.at[move[3]], dxr.at[move[3]])
    for move in Y_MOVES:
        add(xy_out, move, dys.at[move[3]], dyr.at[move[3]])
    for move in XY_MOVES:
        add(xy_out, move, dxys.at[move[3]], dxyr.at[move[3]])

    barrier = pltpu.get_barrier_semaphore()
    for move in moves:

        @pl.when(exists(move, 1))
        def _():
            pl.semaphore_signal(barrier, inc=1, device_id=peer(move), device_id_type=MESH)

    loads = [
        pltpu.make_async_copy(vel, fields.at[0:3], load_sem.at[0]),
        pltpu.make_async_copy(sca, fields.at[3:6], load_sem.at[1]),
    ]
    small = [
        (pos_hbm, pos),
        (mot_hbm, mot),
        (heat_hbm, heat),
        (size_hbm, size),
        (li_hbm, li),
        (lj_hbm, lj),
        (lk_hbm, lk),
    ]
    for n, (src, dst) in enumerate(small):
        loads.append(pltpu.make_async_copy(src, dst, load_sem.at[2 + n]))
    for load in loads:
        load.start()
    for message in x_in + y_in + z_in + z_out + x_out + xy_out:
        message.blank()

    pl.semaphore_wait(barrier, sum(exists(move, 1).astype(jnp.int32) for move in moves))

    for message in x_in:
        message.start()
    for load in loads:
        load.wait()

    for s in range(2):
        row = cj - 1 if s == 0 else 0
        ys[s] = fields[:, :, row, :]
        for t in range(2):
            plane = ci - 1 if t == 0 else 0
            xys[t * 2 + s] = jnp.concatenate(
                [fields[:, plane, row, :], jnp.zeros((2, ck), F32)], axis=0
            )
    for message in y_in:
        message.start()

    xa, xb, lx = pair_weights(pos[0:1])
    ya, yb, ly = pair_weights(pos[1:2])
    za, zb, lz = pair_weights(pos[2:3])
    i0 = li[...] + lx
    j0 = lj[...] + ly
    k0 = lk[...] + lz
    codes = []
    for a, wa in enumerate((xa, xb)):
        for b, wb in enumerate((ya, yb)):
            i, j = i0 + a, j0 + b
            out_i = (i < 0) | (i >= ci)
            out_j = (j < 0) | (j >= cj)
            si = jnp.where(i < 0, 0, 1)
            sj = jnp.where(j < 0, 0, 1)
            code = jnp.where(
                out_i,
                jnp.where(out_j, inner + xy_row + si * 2 + sj, inner + si * cj + j),
                jnp.where(out_j, inner + y_row + sj * ci + i, i * cj + j),
            )
            codes.append((code, wa * wb))
    block = 128
    for start in range(0, planes, block):
        rows = lax.broadcasted_iota(jnp.int32, (block, slots), 0) + start
        table = jnp.zeros((block, slots), F32)
        for code, weight in codes:
            table = jnp.where(rows == code, weight, table)
        high, low = split(table)
        w_hi[start : start + block] = high
        w_lo[start : start + block] = low
    lines = lax.broadcasted_iota(jnp.int32, (ck, slots), 0)
    line[...] = jnp.where(lines == k0, za, jnp.where(lines == k0 + 1, zb, 0.0))
    rim = (jnp.where(k0 < 0, za, 0.0), jnp.where(k0 + 1 >= ck, zb, 0.0))

    zs[...] = jnp.zeros_like(zs)

    def lay(f, first, flat):
        wide = flat.shape[0]
        turned = flat.T
        high, low = split(turned)
        ft_hi[f * ck : (f + 1) * ck, first : first + wide] = high
        ft_lo[f * ck : (f + 1) * ck, first : first + wide] = low
        zs[0, f : f + 1, first : first + wide] = turned[ck - 1 : ck]
        zs[1, f : f + 1, first : first + wide] = turned[0:1]

    for f in range(6):
        lay(f, 0, fields[f].reshape(inner, ck))

    width = 256

    def sample(first, last, fresh):
        for s in range(0, slots, width):
            here = slice(s, s + width)
            got = nn(ft_hi[:, first:last], w_hi[first:last, here])
            got += nn(ft_hi[:, first:last], w_lo[first:last, here])
            got += nn(ft_lo[:, first:last], w_hi[first:last, here])
            for f in range(6):
                part = jnp.sum(
                    got[f * ck : (f + 1) * ck] * line[:, here], axis=0, keepdims=True
                )
                if fresh:
                    sampled[f : f + 1, here] = part
                else:
                    sampled[f : f + 1, here] += part

    sample(0, inner, True)

    for message in x_in + y_in:
        message.arrive()
    for f in range(6):
        flat = jnp.concatenate(
            [xh[0, f], xh[1, f], yh[0, f], yh[1, f]]
            + [xyh[q, f : f + 1] for q in range(4)]
            + [jnp.zeros((outer - xy_row - 4, ck), F32)],
            axis=0,
        )
        lay(f, inner, flat)
    for message in z_in:
        message.start()
    sample(inner, planes, False)
    for message in z_in:
        message.arrive()
    ends = jnp.concatenate([zh[0], zh[1]], axis=0)
    end_hi, end_lo = split(ends)
    got = nn(end_hi, w_hi[...]) + nn(end_hi, w_lo[...]) + nn(end_lo, w_hi[...])
    gas = sampled[...] + got[0:8] * rim[0] + got[8:16] * rim[1]

    live = lax.broadcasted_iota(jnp.int32, (1, slots), 1) // TILE < tally[0]
    q = size[...]
    tp = heat[...]
    v = mot[...]
    drag = step_time / (0.5 * q)
    v_new = (v + drag * gas[0:3]) / (1.0 + drag)
    mass = q * jnp.sqrt(q)
    share = jnp.exp(4.0 * (tp - 1.0))
    decay = step_time * evap_rate * gas[5:6] * (share - gas[4:5])
    q_new = q - decay
    mass_new = q_new * jnp.sqrt(q_new)
    conduct = step_time * heat_rate * gas[5:6] / q
    tp_new = (tp + conduct * gas[3:4]) / (1.0 + conduct) - boiling_energy_drain * decay / q
    state[0:3] = jnp.where(live, v_new, v)
    state[3:4] = jnp.where(live, tp_new, tp)
    state[4:5] = jnp.where(live, q_new, q)
    push = jnp.where(live, mass * (v - v_new), 0.0)
    terms = [
        push[0:1],
        push[1:2],
        push[2:3],
        jnp.where(live, mass * (tp - tp_new), 0.0),
        jnp.where(live, mass - mass_new, 0.0),
    ]
    stack = jnp.concatenate(terms + [jnp.zeros((3, slots), F32)], axis=0)
    ends = jnp.concatenate([stack * rim[1], stack * rim[0]], axis=0)
    end_hi, end_lo = split(ends)
    got = nt(end_hi, w_hi[...]) + nt(end_hi, w_lo[...]) + nt(end_lo, w_hi[...])
    dzs[0] = got[0:8]
    dzs[1] = got[8:16]
    for message in z_out:
        message.start()

    for c in range(5):
        high, low = split(line[...] * terms[c])
        src_hi[c * ck : (c + 1) * ck] = high
        src_lo[c * ck : (c + 1) * ck] = low

    def spread(first, last, low, high):
        got = nt(w_hi[first:last], src_hi[low:high])
        got += nt(w_hi[first:last], src_lo[low:high])
        got += nt(w_lo[first:last], src_hi[low:high])
        return got

    pick_row = lax.broadcasted_iota(jnp.int32, (32, 5 * ck), 0)
    pick_col = lax.broadcasted_iota(jnp.int32, (32, 5 * ck), 1)
    pick_row = jnp.where(pick_row >= 16, pick_row - 16, pick_row)
    target = jnp.where(pick_row >= 8, (pick_row - 8) * ck + ck - 1, pick_row * ck)
    pick = jnp.where(target == pick_col, 1.0, 0.0).astype(BF16)

    spans = [(c, min(c + 2, 5)) for c in range(0, 5, 2)]
    halo = [spread(inner, planes, a * ck, b * ck) for a, b in spans]
    for message in z_out:
        message.arrive()
    ends = jnp.concatenate([dzr[0], dzr[1]], axis=0)
    end_hi, end_lo = split(ends)
    ends = jnp.concatenate([end_hi, end_lo], axis=0)
    for part, (a, b) in zip(halo, spans):
        part = part + tn(ends[:, inner:], pick[:, a * ck : b * ck])
        for c in range(a, b):
            piece = part[:, (c - a) * ck : (c - a + 1) * ck]
            dxs[1, c] = piece[0:cj]
            dxs[0, c] = piece[cj : 2 * cj]
            dys[1, c] = piece[y_row : y_row + ci]
            dys[0, c] = piece[y_row + ci : y_row + 2 * ci]
            for n in range(4):
                dxys[3 - n, c : c + 1] = piece[xy_row + n : xy_row + n + 1]
    for message in x_out + xy_out:
        message.start()

    for a, b in spans:
        part = spread(0, inner, a * ck, b * ck) + tn(ends[:, :inner], pick[:, a * ck : b * ck])
        for c in range(a, b):
            dep[c] = part[:, (c - a) * ck : (c - a + 1) * ck].reshape(ci, cj, ck)

    for message in x_out + xy_out:
        message.arrive()
    for message in x_in + y_in + z_in + z_out + x_out + xy_out:
        message.leave()


def finish(part, old, dxr, dyr, dxyr, dep_hbm, state_hbm, dep, sem):
    ci, cj = dep.shape[1:3]
    side = pltpu.make_async_copy(old, state_hbm, sem.at[0])
    side.start()
    outs = []
    for c in range(5):
        dep[c] = part[c]
        for s in range(2):
            plane = 0 if s == 0 else ci - 1
            dep[c, plane] += dxr[s, c]
        for s in range(2):
            row = 0 if s == 0 else cj - 1
            dep[c, :, row, :] += dyr[s, c]
            for t in range(2):
                plane = 0 if t == 0 else ci - 1
                dep[c, plane, row : row + 1, :] += dxyr[t * 2 + s, c : c + 1]
        out = pltpu.make_async_copy(dep.at[c], dep_hbm.at[c], sem.at[1 + c])
        out.start()
        outs.append(out)
    for out in outs:
        out.wait()
    side.wait()


def local(counts, vel, sca, pos, mot, heat, size, li, lj, lk, tally):
    ci, cj, ck = vel.shape[1:]
    slots = heat.shape[0]
    outer = 2 * cj + 2 * ci + 4
    planes = ci * cj + -(-outer // 128) * 128
    vmem = pl.BlockSpec(memory_space=pltpu.VMEM)
    row = lambda value: value.reshape(1, slots)
    messages = 24
    scratch = [
        pltpu.VMEM((6, ci, cj, ck), F32),
        pltpu.VMEM((6 * ck, planes), BF16),
        pltpu.VMEM((6 * ck, planes), BF16),
        pltpu.VMEM((planes, slots), BF16),
        pltpu.VMEM((planes, slots), BF16),
        pltpu.VMEM((ck, slots), F32),
        pltpu.VMEM((5 * ck, slots), BF16),
        pltpu.VMEM((5 * ck, slots), BF16),
        pltpu.VMEM((8, slots), F32),
        pltpu.VMEM((2, 6, cj, ck), F32),
        pltpu.VMEM((2, 6, ci, ck), F32),
        pltpu.VMEM((4, 8, ck), F32),
        pltpu.VMEM((2, 8, planes), F32),
        pltpu.VMEM((2, 6, ci, ck), F32),
        pltpu.VMEM((4, 8, ck), F32),
        pltpu.VMEM((2, 8, planes), F32),
        pltpu.VMEM((2, 5, cj, ck), F32),
        pltpu.VMEM((2, 5, ci, ck), F32),
        pltpu.VMEM((4, 8, ck), F32),
        pltpu.VMEM((2, 8, planes), F32),
        pltpu.VMEM((2, 8, planes), F32),
        pltpu.VMEM((3, slots), F32),
        pltpu.VMEM((3, slots), F32),
        pltpu.VMEM((1, slots), F32),
        pltpu.VMEM((1, slots), F32),
        pltpu.VMEM((1, slots), jnp.int32),
        pltpu.VMEM((1, slots), jnp.int32),
        pltpu.VMEM((1, slots), jnp.int32),
        pltpu.SemaphoreType.DMA((9,)),
        pltpu.SemaphoreType.DMA((messages,)),
        pltpu.SemaphoreType.DMA((messages,)),
    ]
    any_ = pl.BlockSpec(memory_space=pl.ANY)
    pin = lambda value: pltpu.with_memory_space_constraint(value, pltpu.HBM)
    arrays = (vel, sca, pos, mot, row(heat), row(size), row(li), row(lj), row(lk))
    part, state, dxr, dyr, dxyr = pl.pallas_call(
        functools.partial(kernel, counts),
        out_shape=(
            jax.ShapeDtypeStruct((5, ci, cj, ck), F32),
            jax.ShapeDtypeStruct((5, slots), F32),
            jax.ShapeDtypeStruct((2, 5, cj, ck), F32),
            jax.ShapeDtypeStruct((2, 5, ci, ck), F32),
            jax.ShapeDtypeStruct((4, 8, ck), F32),
        ),
        in_specs=[pl.BlockSpec(memory_space=pltpu.HBM)] * 9 + [pl.BlockSpec(memory_space=pltpu.SMEM)],
        out_specs=(vmem,) * 5,
        scratch_shapes=scratch,
        compiler_params=pltpu.CompilerParams(
            collective_id=0, has_side_effects=True, vmem_limit_bytes=24 * 2**20
        ),
    )(*[pin(x) for x in arrays], tally)
    return pl.pallas_call(
        finish,
        out_shape=(
            jax.ShapeDtypeStruct((5, ci, cj, ck), F32),
            jax.ShapeDtypeStruct((5, slots), F32),
        ),
        in_specs=[vmem] * 5,
        out_specs=(any_, any_),
        scratch_shapes=[pltpu.VMEM((5, ci, cj, ck), F32), pltpu.SemaphoreType.DMA((6,))],
        compiler_params=pltpu.CompilerParams(vmem_limit_bytes=12 * 2**20),
    )(part, state, dxr, dyr, dxyr)


def solution(mesh):
    bricks = P(None, AXES[0], AXES[1], AXES[2])
    rows = P(None, AXES)
    flat = P(AXES)
    counts = tuple(mesh.shape[axis] for axis in AXES)
    return jax.shard_map(
        functools.partial(local, counts),
        mesh=mesh,
        in_specs=(bricks, bricks, rows, rows) + (flat,) * 6,
        out_specs=(bricks, rows),
        check_vma=False,
    )
```

```python
import functools

import jax
import jax.numpy as jnp
from jax import lax
from jax.experimental import pallas as pl
from jax.experimental.pallas import tpu as pltpu
from jax.sharding import PartitionSpec as P

TILE = 128
AXES = ("gx", "gy", "gz")
MESH = pl.DeviceIdType.MESH
F32 = jnp.float32
BF16 = jnp.bfloat16

step_time = 0.25
evap_rate = 1.0
heat_rate = 2.0
boiling_energy_drain = 0.3

STEPS = ((1, 0), (-1, 1))
NUM_TERMS = 5
NUM_FIELDS = 6


def split(value):
    high = value.astype(BF16)
    return high, (value - high.astype(F32)).astype(BF16)


def nn(a, b):
    return lax.dot_general(a, b, (((1,), (0,)), ((), ())), preferred_element_type=F32)


def nt(a, b):
    return lax.dot_general(a, b, (((1,), (1,)), ((), ())), preferred_element_type=F32)


def pair_weights(offset):
    lower = jnp.where(offset < 0.0, -1.0, 0.0)
    first = jnp.maximum(0.0, 1.0 - jnp.abs(offset - lower))
    second = jnp.maximum(0.0, 1.0 - jnp.abs(offset - (lower + 1.0)))
    return first, second, lower


def lanes_of(shape):
    return lax.broadcasted_iota(jnp.int32, shape, len(shape) - 1)


def spots(first, count, base, wa, wb):
    rows = (lax.broadcasted_iota(jnp.int32, (count, base.shape[1]), 0) + first).astype(F32)
    return jnp.where(rows == base, wa, jnp.where(rows == base + 1.0, wb, 0.0))


def kernel(
    counts,
    vel,
    sca,
    pos_in,
    mot_in,
    heat_in,
    size_in,
    li_in,
    lj_in,
    lk_in,
    tally,
    dep,
    state,
    dyr,
    dxyr,
    dzr,
    dxzr,
    dyzr,
    dxyzr,
    fields,
    pos,
    mot,
    heat,
    size,
    li,
    lj,
    lk,
    ft_hi,
    ft_lo,
    w_hi,
    w_lo,
    wx,
    wy,
    xt,
    yt_hi,
    yt_lo,
    line,
    line_hi,
    line_lo,
    ztable,
    src_hi,
    src_lo,
    sampled,
    geo,
    terms,
    xh,
    yh,
    xyh,
    zh,
    xzh,
    yzh,
    xyzh,
    geor,
    termr,
    ys,
    xys,
    zs,
    ez,
    dys,
    dxys,
    dzs,
    dxzs,
    dyzs,
    load_sem,
    send_sem,
    recv_sem,
):
    ci, cj, ck = vel.shape[1:]
    slots = heat.shape[1]
    inner = ci * cj
    me = [lax.axis_index(axis) for axis in AXES]

    def exists(move, sign):
        good = None
        for d in range(3):
            step = sign * move[d]
            if step == 1:
                test = me[d] < counts[d] - 1
            elif step == -1:
                test = me[d] > 0
            else:
                continue
            good = test if good is None else jnp.logical_and(good, test)
        return good

    def peer(move):
        return tuple(lax.rem(me[d] + move[d] + counts[d], counts[d]) for d in range(3))

    class Message:
        def __init__(self, number, move, src, dst):
            self.move = move
            self.dst = dst
            self.copy = pltpu.make_async_remote_copy(
                src_ref=src,
                dst_ref=dst,
                send_sem=send_sem.at[number],
                recv_sem=recv_sem.at[number],
                device_id=peer(move),
                device_id_type=MESH,
            )

        def start(self):
            @pl.when(exists(self.move, 1))
            def _():
                self.copy.start()

        def blank(self):
            @pl.when(jnp.logical_not(exists(self.move, -1)))
            def _():
                self.dst[...] = jnp.zeros(self.dst.shape, F32)

        def arrive(self):
            @pl.when(exists(self.move, -1))
            def _():
                self.copy.wait_recv()

        def leave(self):
            @pl.when(exists(self.move, 1))
            def _():
                self.copy.wait_send()

    made = []

    def add(group, move, src, dst):
        message = Message(len(made), move, src, dst)
        made.append(message)
        group.append(message)

    face = lambda n, extent: extent - 1 if n == 0 else 0
    edge_tile = lambda n: pl.ds(face(n, ci) * cj // 128 * 128, 128)
    moves = []
    x_in, y_in, z_in, geo_in, x_out, y_out, z_out = [], [], [], [], [], [], []
    for mx, x in STEPS:
        add(x_in, (mx, 0, 0), fields.at[:, face(x, ci)], xh.at[x])
        add(geo_in, (mx, 0, 0), geo, geor.at[x])
        add(x_out, (mx, 0, 0), terms, termr.at[x])
        moves.append((mx, 0, 0))
        for my, y in STEPS:
            add(y_in, (mx, my, 0), xys.at[2 * x + y], xyh.at[2 * x + y])
            add(y_out, (mx, my, 0), dxys.at[2 * x + y], dxyr.at[2 * x + y])
            moves.append((mx, my, 0))
            for mz, z in STEPS:
                n = 4 * x + 2 * y + z
                add(z_in, (mx, my, mz), ez.at[z], xyzh.at[n])
                add(z_out, (mx, my, mz), dxzs.at[2 * x + z], dxyzr.at[n])
                moves.append((mx, my, mz))
        for mz, z in STEPS:
            n = 2 * x + z
            add(z_in, (mx, 0, mz), zs.at[z, :, edge_tile(x)], xzh.at[n])
            add(z_out, (mx, 0, mz), dxzs.at[n], dxzr.at[n])
            moves.append((mx, 0, mz))
    for my, y in STEPS:
        add(y_in, (0, my, 0), ys.at[y], yh.at[y])
        add(y_out, (0, my, 0), dys.at[y, :, 0:ci], dyr.at[y])
        moves.append((0, my, 0))
        for mz, z in STEPS:
            add(z_in, (0, my, mz), ez.at[z], yzh.at[2 * y + z])
            add(z_out, (0, my, mz), dyzs.at[z], dyzr.at[2 * y + z])
            moves.append((0, my, mz))
    for mz, z in STEPS:
        add(z_in, (0, 0, mz), zs.at[z], zh.at[z])
        add(z_out, (0, 0, mz), dzs.at[z, :, 0:ci], dzr.at[z])
        moves.append((0, 0, mz))

    barrier = pltpu.get_barrier_semaphore()
    for move in moves:

        @pl.when(exists(move, 1))
        def _():
            pl.semaphore_signal(barrier, inc=1, device_id=peer(move), device_id_type=MESH)

    small = [
        pltpu.make_async_copy(src, dst, load_sem.at[2 + n])
        for n, (src, dst) in enumerate(
            [
                (pos_in, pos),
                (li_in, li),
                (lj_in, lj),
                (lk_in, lk),
                (mot_in, mot),
                (heat_in, heat),
                (size_in, size),
            ]
        )
    ]
    loads = [
        pltpu.make_async_copy(vel, fields.at[0:3], load_sem.at[0]),
        pltpu.make_async_copy(sca, fields.at[3:6], load_sem.at[1]),
    ]
    for load in small + loads:
        load.start()
    for message in y_in + z_in + y_out + z_out:
        message.blank()
    zs[...] = jnp.zeros_like(zs)
    xys[...] = jnp.zeros_like(xys)
    dxys[...] = jnp.zeros_like(dxys)
    dxzs[...] = jnp.zeros_like(dxzs)

    for load in small:
        load.wait()
    xa, xb, lx = pair_weights(pos[0:1])
    ya, yb, ly = pair_weights(pos[1:2])
    za, zb, lz = pair_weights(pos[2:3])
    i0 = li[...].astype(F32) + lx
    j0 = lj[...].astype(F32) + ly
    k0 = lk[...].astype(F32) + lz

    def at(index, base, wa, wb):
        return jnp.where(base == index, wa, jnp.where(base + 1.0 == index, wb, 0.0))

    x_low, x_high = at(-1.0, i0, xa, xb), at(float(ci), i0, xa, xb)
    y_low, y_high = at(-1.0, j0, ya, yb), at(float(cj), j0, ya, yb)
    z_low, z_high = at(-1.0, k0, za, zb), at(float(ck), k0, za, zb)
    for n, row in enumerate((x_high, x_low, j0, k0, ya, yb, za, zb)):
        geo[n : n + 1] = row
    xt[0:ci] = spots(0, ci, i0, xa, xb)
    xt[ci : 2 * ci] = jnp.concatenate([x_low, x_high, jnp.zeros((ci - 2, slots), F32)], axis=0)
    across = spots(0, cj, j0, ya, yb)
    rims = [
        jnp.broadcast_to(y_low, (8, slots)),
        jnp.broadcast_to(y_high, (8, slots)),
        jnp.zeros((yt_hi.shape[0] - cj - 16, slots), F32),
    ]
    yt_hi[...], yt_lo[...] = split(jnp.concatenate([across] + rims, axis=0))
    for i in range(ci):
        high, low = split(xt[i : i + 1] * across)
        w_hi[i * cj : (i + 1) * cj] = high
        w_lo[i * cj : (i + 1) * cj] = low
    for n, row in enumerate((x_low, x_high)):
        high, low = split(row * across)
        wx[n, 0:cj] = high
        wx[n, cj : 2 * cj] = high
        wx[n, 2 * cj : 3 * cj] = low
    corners = [a * b for a in (x_low, x_high) for b in (y_low, y_high)]
    sides = [xt[0:ci] * y_low, xt[0:ci] * y_high]
    group = wy.shape[0] // 4
    filler = [jnp.zeros((group - 2 * ci - 4, slots), F32)]
    high, low = split(jnp.concatenate(sides + corners + filler, axis=0))
    wy[0:group] = high
    wy[group : 2 * group] = high
    wy[2 * group : 3 * group] = low
    wy[3 * group : 4 * group] = jnp.zeros((group, slots), BF16)
    line[...] = spots(0, ck, k0, za, zb)
    line_hi[...], line_lo[...] = split(line[...])

    for load in loads:
        load.wait()
    for y in range(2):
        row = face(y, cj)
        ys[y] = fields[:, :, row, :]
        for x in range(2):
            xys[2 * x + y, 0:NUM_FIELDS] = fields[:, face(x, ci), row, :]
    pl.semaphore_wait(barrier, sum(exists(move, 1).astype(jnp.int32) for move in moves))

    for message in x_in + y_in + geo_in:
        message.start()

    for f in range(NUM_FIELDS):
        turned = fields[f].reshape(inner, ck).T
        high, low = split(turned)
        ft_hi[f * ck : (f + 1) * ck] = high
        ft_lo[f * ck : (f + 1) * ck] = low
        zs[0, f : f + 1] = turned[ck - 1 : ck]
        zs[1, f : f + 1] = turned[0:1]
    rows = lax.broadcasted_iota(jnp.int32, (inner, 128), 0)
    cols = lanes_of((inner, 128))
    target = jnp.where(cols < cj + 8, (cols - cj) * cj + cj - 1, (cols - cj - 8) * cj)
    chosen = (rows == target) & (cols >= cj) & (cols < cj + 16)
    chosen = jnp.where(chosen, 1.0, 0.0).astype(BF16)
    high, low = split(zs[...].reshape(16, inner))
    ez[...] = (nn(high, chosen) + nn(low, chosen)).reshape(2, 8, 128)
    for message in z_in:
        message.start()

    width = 256

    def collect(got, here):
        return [
            jnp.sum(got[f * ck : (f + 1) * ck] * line[:, here], axis=0, keepdims=True)
            for f in range(NUM_FIELDS)
        ]

    for s in range(0, slots, width):
        here = slice(s, s + width)
        got = nn(ft_hi[...], w_hi[:, here])
        got += nn(ft_hi[...], w_lo[:, here])
        got += nn(ft_lo[...], w_hi[:, here])
        for f, part in enumerate(collect(got, here)):
            sampled[f : f + 1, here] = part

    for message in y_in:
        message.arrive()

    def turn(flats):
        out = []
        for flat in flats:
            high = flat.astype(BF16).astype(F32)
            out.append(jnp.concatenate([high, flat - high, high], axis=0).T.astype(BF16))
        return jnp.concatenate(out, axis=0)

    def more(left, right):
        for s in range(0, slots, width):
            here = slice(s, s + width)
            for f, part in enumerate(collect(nn(left, right[:, here]), here)):
                sampled[f : f + 1, here] += part

    empty = jnp.zeros((group - 2 * ci - 4, ck), F32)
    left = turn(
        [
            jnp.concatenate(
                [yh[0, f], yh[1, f]] + [xyh[q, f : f + 1] for q in range(4)] + [empty], axis=0
            )
            for f in range(NUM_FIELDS)
        ]
    )
    more(left, wy[0 : 3 * group])

    for message in z_in:
        message.arrive()
    lanes = lanes_of((8, 128))
    body = lanes < cj

    def half(tile, odd):
        return jnp.where(body, pltpu.roll(tile, 128 - cj, 1) if odd else tile, 0.0)

    def pick(tile, lane):
        return jnp.where(lanes == lane, tile, 0.0)

    for z in range(2):
        for i in range(ci):
            first = i * cj // 128 * 128
            block = half(zh[z, :, first : first + 128], i * cj % 128 != 0)
            block += pick(yzh[z], cj + i) + pick(yzh[2 + z], cj + 8 + i)
            ztable[z, i] = block
        for x in range(2):
            i = face(x, ci)
            block = half(xzh[2 * x + z], i * cj % 128 != 0)
            block += pick(xyzh[4 * x + z], cj + i) + pick(xyzh[4 * x + 2 + z], cj + 8 + i)
            ztable[z, ci + x] = block
    blocks = ci + 2
    high, low = split(ztable[...].reshape(2 * blocks * 8, 128))
    got = nn(high, yt_hi[...]) + nn(high, yt_lo[...]) + nn(low, yt_hi[...])
    for z, rim in enumerate((z_low, z_high)):
        total = None
        for b in range(blocks):
            first = (z * blocks + b) * 8
            part = got[first : first + 8] * xt[b : b + 1]
            total = part if total is None else total + part
        sampled[...] += total * rim

    for x, message in enumerate(x_in):

        @pl.when(exists(message.move, -1))
        def _():
            message.copy.wait_recv()
            more(turn([xh[x, f] for f in range(NUM_FIELDS)]), wx[x])

    gas = sampled[...]
    live = lanes_of((1, slots)) // TILE < tally[0]
    q = size[...]
    tp = heat[...]
    v = mot[...]
    drag = step_time / (0.5 * q)
    v_new = (v + drag * gas[0:3]) / (1.0 + drag)
    mass = q * jnp.sqrt(q)
    share = jnp.exp(4.0 * (tp - 1.0))
    decay = step_time * evap_rate * gas[5:6] * (share - gas[4:5])
    q_new = q - decay
    mass_new = q_new * jnp.sqrt(q_new)
    conduct = step_time * heat_rate * gas[5:6] / q
    tp_new = (tp + conduct * gas[3:4]) / (1.0 + conduct) - boiling_energy_drain * decay / q
    state[0:3] = jnp.where(live, v_new, v)
    state[3:4] = jnp.where(live, tp_new, tp)
    state[4:5] = jnp.where(live, q_new, q)
    terms[0:3] = jnp.where(live, mass * (v - v_new), 0.0)
    terms[3:4] = jnp.where(live, mass * (tp - tp_new), 0.0)
    terms[4:5] = jnp.where(live, mass - mass_new, 0.0)
    for message in x_out:
        message.start()

    part_rows = 2 * ci
    pieces = [xt[...] * terms[c : c + 1] for c in range(NUM_TERMS)]

    def fan(rims):
        return split(jnp.concatenate([piece * rim for rim in rims for piece in pieces], axis=0))

    def both(high, low, right_hi, right_lo):
        return nt(high, right_hi) + nt(high, right_lo) + nt(low, right_hi)

    shape = (2, NUM_TERMS, part_rows, 128)
    high, low = fan((y_high, y_low))
    dys[...] = both(high, low, line_hi[...], line_lo[...]).reshape(shape)
    for x in range(2):
        row = ci + 1 - x
        for y in range(2):
            for c in range(NUM_TERMS):
                dxys[2 * x + y, c : c + 1] = dys[y, c, row : row + 1]
    for message in y_out:
        message.start()
    high, low = fan((z_high, z_low))
    dzs[...] = both(high, low, yt_hi[...], yt_lo[...]).reshape(shape)
    for z in range(2):
        for x in range(2):
            row = ci + 1 - x
            for c in range(NUM_TERMS):
                dxzs[2 * x + z, c : c + 1] = dzs[z, c, row : row + 1]
        tile = jnp.zeros((8, 128), F32)
        for c in range(NUM_TERMS):
            keep = (lanes == cj + c) | (lanes == cj + 8 + c)
            tile = jnp.where(keep, dzs[z, c, 0:ci], tile)
        dyzs[z] = tile
    for message in z_out:
        message.start()

    for c in range(NUM_TERMS):
        high, low = split(line[...] * terms[c : c + 1])
        src_hi[c * ck : (c + 1) * ck] = high
        src_lo[c * ck : (c + 1) * ck] = low
    for a in range(0, NUM_TERMS, 2):
        b = min(a + 2, NUM_TERMS)
        span = slice(a * ck, b * ck)
        got = nt(w_hi[...], src_hi[span])
        got += nt(w_hi[...], src_lo[span])
        got += nt(w_lo[...], src_hi[span])
        for c in range(a, b):
            dep[c] = got[:, (c - a) * ck : (c - a + 1) * ck].reshape(ci, cj, ck)

    for x, (places, deposits) in enumerate(zip(geo_in, x_out)):
        plane = 0 if x == 0 else ci - 1

        @pl.when(exists(places.move, -1))
        def _():
            places.copy.wait_recv()
            rows = [geor[x, n : n + 1] for n in range(8)]
            there = spots(0, cj, rows[2], rows[4], rows[5]) * rows[x]
            along_hi, along_lo = split(spots(0, ck, rows[3], rows[6], rows[7]))
            deposits.copy.wait_recv()
            high, low = split(
                jnp.concatenate([there * termr[x, c : c + 1] for c in range(NUM_TERMS)], axis=0)
            )
            got = both(high, low, along_hi, along_lo)
            for c in range(NUM_TERMS):
                dep[c, plane] += got[c * cj : (c + 1) * cj]

    for message in y_out + z_out:
        message.arrive()
    for message in made:
        message.leave()


def finish(
    part, old, dyr, dxyr, dzr, dxzr, dyzr, dxyzr, dep_out, state_out, dep, sem
):
    ci, cj, ck = dep.shape[1:]
    terms = dep.shape[0]
    side = pltpu.make_async_copy(old, state_out, sem.at[terms])
    side.start()
    lanes = lanes_of((8, 128))
    rows = lax.broadcasted_iota(jnp.int32, (8, 128), 0)
    ends = (0, ck - 1)

    def at_ends(first, second, where):
        return jnp.where(where == ends[0], first, jnp.where(where == ends[1], second, 0.0))

    corner = []
    for x in range(2):
        for y in range(2):
            lane = cj + 8 if y == 0 else cj
            first, second = (dxyzr[4 * x + 2 * y + z, :, lane : lane + 1] for z in range(2))
            corner.append(dxyr[2 * x + y] + at_ends(first, second, lanes))
    wide = lanes_of((cj, ck))
    outs = []
    for c in range(terms):
        turned = []
        for z in range(2):
            block = dzr[z, c]
            for x in range(2):
                plane = 0 if x == 0 else ci - 1
                block += jnp.where(rows == plane, dxzr[2 * x + z, c : c + 1], 0.0)
            turned.append(block)
        turned = jnp.concatenate(turned, axis=0).T
        for i in range(ci):
            first, second = turned[0:cj, i : i + 1], turned[0:cj, ci + i : ci + i + 1]
            dep[c, i] = part[c, i] + at_ends(first, second, wide)
        for y in range(2):
            row = 0 if y == 0 else cj - 1
            lane = cj + 8 + c if y == 0 else cj + c
            first, second = (dyzr[2 * y + z, :, lane : lane + 1] for z in range(2))
            dep[c, :, row, :] += dyr[y, c] + at_ends(first, second, lanes)
            for x in range(2):
                plane = 0 if x == 0 else ci - 1
                dep[c, plane, row : row + 1, :] += corner[2 * x + y][c : c + 1]
        out = pltpu.make_async_copy(dep.at[c], dep_out.at[c], sem.at[c])
        out.start()
        outs.append(out)
    for out in outs:
        out.wait()
    side.wait()


def local(counts, vel, sca, pos, mot, heat, size, li, lj, lk, tally):
    ci, cj, ck = vel.shape[1:]
    slots = heat.shape[0]
    inner = ci * cj
    vmem = pl.BlockSpec(memory_space=pltpu.VMEM)
    hbm = pl.BlockSpec(memory_space=pltpu.HBM)
    row = lambda value: value.reshape(1, slots)
    pin = lambda value: pltpu.with_memory_space_constraint(value, pltpu.HBM)
    tile = (8, 128)
    group = -(-(2 * ci + 4) // 16) * 16
    messages = 54
    f32 = lambda *shape: pltpu.VMEM(shape, F32)
    i32 = lambda *shape: pltpu.VMEM(shape, jnp.int32)
    b16 = lambda *shape: pltpu.VMEM(shape, BF16)
    struct = lambda *shape: jax.ShapeDtypeStruct(shape, F32)
    scratch = [
        f32(NUM_FIELDS, ci, cj, ck),
        f32(3, slots),
        f32(3, slots),
        f32(1, slots),
        f32(1, slots),
        i32(1, slots),
        i32(1, slots),
        i32(1, slots),
        b16(NUM_FIELDS * ck, inner),
        b16(NUM_FIELDS * ck, inner),
        b16(inner, slots),
        b16(inner, slots),
        b16(2, 3 * cj, slots),
        b16(4 * group, slots),
        f32(2 * ci, slots),
        b16(128, slots),
        b16(128, slots),
        f32(ck, slots),
        b16(ck, slots),
        b16(ck, slots),
        f32(2, ci + 2, *tile),
        b16(NUM_TERMS * ck, slots),
        b16(NUM_TERMS * ck, slots),
        f32(8, slots),
        f32(8, slots),
        f32(NUM_TERMS, slots),
        f32(2, NUM_FIELDS, cj, ck),
        f32(2, NUM_FIELDS, ci, ck),
        f32(4, *tile),
        f32(2, 8, inner),
        f32(4, *tile),
        f32(4, *tile),
        f32(8, *tile),
        f32(2, 8, slots),
        f32(2, NUM_TERMS, slots),
        f32(2, NUM_FIELDS, ci, ck),
        f32(4, *tile),
        f32(2, 8, inner),
        f32(2, *tile),
        f32(2, NUM_TERMS, 2 * ci, ck),
        f32(4, *tile),
        f32(2, NUM_TERMS, 2 * ci, ck),
        f32(4, *tile),
        f32(2, *tile),
        pltpu.SemaphoreType.DMA((9,)),
        pltpu.SemaphoreType.DMA((messages,)),
        pltpu.SemaphoreType.DMA((messages,)),
    ]
    results = (
        struct(NUM_TERMS, ci, cj, ck),
        struct(NUM_TERMS, slots),
        struct(2, NUM_TERMS, ci, ck),
        struct(4, *tile),
        struct(2, NUM_TERMS, ci, ck),
        struct(4, *tile),
        struct(4, *tile),
        struct(8, *tile),
    )
    arrays = (vel, sca, pos, mot, row(heat), row(size), row(li), row(lj), row(lk))
    parts = pl.pallas_call(
        functools.partial(kernel, counts),
        out_shape=results,
        in_specs=[hbm] * len(arrays) + [pl.BlockSpec(memory_space=pltpu.SMEM)],
        out_specs=(vmem,) * len(results),
        scratch_shapes=scratch,
        compiler_params=pltpu.CompilerParams(
            collective_id=0, has_side_effects=True, vmem_limit_bytes=32 * 2**20
        ),
    )(*[pin(value) for value in arrays], tally)
    return pl.pallas_call(
        finish,
        out_shape=results[0:2],
        in_specs=[vmem] * len(results),
        out_specs=(pl.BlockSpec(memory_space=pl.ANY),) * 2,
        scratch_shapes=[
            f32(NUM_TERMS, ci, cj, ck),
            pltpu.SemaphoreType.DMA((NUM_TERMS + 1,)),
        ],
        compiler_params=pltpu.CompilerParams(vmem_limit_bytes=12 * 2**20),
    )(*parts)


def solution(mesh):
    bricks = P(None, AXES[0], AXES[1], AXES[2])
    rows = P(None, AXES)
    flat = P(AXES)
    counts = tuple(mesh.shape[axis] for axis in AXES)
    return jax.shard_map(
        functools.partial(local, counts),
        mesh=mesh,
        in_specs=(bricks, bricks, rows, rows) + (flat,) * 6,
        out_specs=(bricks, rows),
        check_vma=False,
    )
```

```python
import functools
import itertools

import jax
import jax.numpy as jnp
from jax import lax
from jax.experimental import pallas as pl
from jax.experimental.pallas import tpu as pltpu
from jax.sharding import PartitionSpec as P

TILE = 128
AXES = ("gx", "gy", "gz")
MESH = pl.DeviceIdType.MESH
F32 = jnp.float32
BF16 = jnp.bfloat16

step_time = 0.25
evap_rate = 1.0
heat_rate = 2.0
boiling_energy_drain = 0.3

STEPS = ((1, 0), (-1, 1))
NUM_TERMS = 5
NUM_FIELDS = 6
PARTS = 3
CHUNK = NUM_FIELDS // PARTS


def split(value):
    high = value.astype(BF16)
    return high, (value - high.astype(F32)).astype(BF16)


def nn(a, b):
    return lax.dot_general(a, b, (((1,), (0,)), ((), ())), preferred_element_type=F32)


def nt(a, b):
    return lax.dot_general(a, b, (((1,), (1,)), ((), ())), preferred_element_type=F32)


def pair_weights(offset):
    lower = jnp.where(offset < 0.0, -1.0, 0.0)
    first = jnp.maximum(0.0, 1.0 - jnp.abs(offset - lower))
    second = jnp.maximum(0.0, 1.0 - jnp.abs(offset - (lower + 1.0)))
    return first, second, lower


def lanes_of(shape):
    return lax.broadcasted_iota(jnp.int32, shape, len(shape) - 1)


def spots(first, count, base, wa, wb):
    rows = (lax.broadcasted_iota(jnp.int32, (count, base.shape[1]), 0) + first).astype(F32)
    return jnp.where(rows == base, wa, jnp.where(rows == base + 1.0, wb, 0.0))


def kernel(
    counts,
    vel,
    sca,
    pos_in,
    mot_in,
    heat_in,
    size_in,
    li_in,
    lj_in,
    lk_in,
    tally,
    dep,
    state,
    dyr,
    dxyr,
    dzr,
    dxzr,
    dyzr,
    dxyzr,
    fields,
    pos,
    mot,
    heat,
    size,
    li,
    lj,
    lk,
    ft_hi,
    ft_lo,
    w_hi,
    w_lo,
    wx,
    wy,
    xt,
    cw,
    yt,
    line,
    lines,
    ztable,
    src_hi,
    src_lo,
    sampled,
    geo,
    terms,
    xh,
    yh,
    xyh,
    zh,
    xzh,
    yzh,
    xyzh,
    geor,
    termr,
    ys,
    xys,
    zs,
    ez,
    dys,
    dxys,
    dzs,
    dxzs,
    dyzs,
    gauge,
    load_sem,
    send_sem,
    recv_sem,
):
    ci, cj, ck = vel.shape[1:]
    slots = heat.shape[1]
    inner = ci * cj
    me = [lax.axis_index(axis) for axis in AXES]

    def exists(move, sign):
        good = None
        for d in range(3):
            step = sign * move[d]
            if step == 1:
                test = me[d] < counts[d] - 1
            elif step == -1:
                test = me[d] > 0
            else:
                continue
            good = test if good is None else jnp.logical_and(good, test)
        return good

    def peer(move):
        return tuple(lax.rem(me[d] + move[d] + counts[d], counts[d]) for d in range(3))

    class Message:
        def __init__(self, number, move, src, dst, tiles, post):
            self.move = move
            self.dst = dst
            self.tiles = tiles
            self.number = number
            self.copy = pltpu.make_async_remote_copy(
                src_ref=src,
                dst_ref=dst,
                send_sem=send_sem.at[post],
                recv_sem=recv_sem.at[number],
                device_id=peer(move),
                device_id_type=MESH,
            )

        def start(self):
            @pl.when(exists(self.move, 1))
            def _():
                self.copy.start()

        def blank(self):
            @pl.when(jnp.logical_not(exists(self.move, -1)))
            def _():
                self.dst[...] = jnp.zeros(self.dst.shape, F32)

        def leave(self):
            @pl.when(exists(self.move, 1))
            def _():
                self.copy.wait_send()

    def totals(messages, sign):
        sides = []
        for extent in counts:
            low, high = (-1,), (1,)
            sides.append([()] if extent == 1 else [low, high] + [low + high] * (extent > 2))
        found = set()
        for place in itertools.product(*sides):
            there = [
                message.tiles
                for message in messages
                if all(
                    step == 0 or sign * step in side for step, side in zip(message.move, place)
                )
            ]
            found.add(sum(there))
        return sorted(found - {0})

    def drain(sem, messages, sign):
        count = sum(
            jnp.where(exists(message.move, sign), message.tiles, 0) for message in messages
        )
        for total in totals(messages, sign):

            @pl.when(count == total)
            def _():
                some = gauge.at[0:total]
                pltpu.make_async_copy(some, some, sem).wait()

    def arrive(messages):
        drain(recv_sem.at[messages[0].number], messages, -1)

    made = []

    def add(group, number, move, src, dst, tiles=1, post=0):
        message = Message(number, move, src, dst, tiles, post)
        made.append(message)
        group.append(message)

    Y_IN, Z_IN, OUT, GEO, TERMS, RIM, FACE = 0, 1, 2, 3, 5, 7, 9
    face = lambda n, extent: extent - 1 if n == 0 else 0
    edge_tile = lambda n: pl.ds(face(n, ci) * cj // 128 * 128, 128)
    moves = []
    y_in, z_in, geo_in, x_out, out = [], [], [], [], []
    faces, rim_in = [[], []], [[], []]
    for mx, x in STEPS:
        for my, y in STEPS:
            add(y_in, Y_IN, (mx, my, 0), xys.at[2 * x + y], xyh.at[2 * x + y])
            add(out, OUT, (mx, my, 0), dxys.at[2 * x + y], dxyr.at[2 * x + y])
            for mz, z in STEPS:
                n = 4 * x + 2 * y + z
                add(rim_in[x], RIM + x, (mx, my, mz), ez.at[z], xyzh.at[n])
                add(out, OUT, (mx, my, mz), dxzs.at[2 * x + z], dxyzr.at[n])
                moves.append((mx, my, mz))
            moves.append((mx, my, 0))
        for part in range(PARTS):
            span = slice(part * CHUNK, (part + 1) * CHUNK)
            here = fields.at[span, face(x, ci)]
            add(faces[x], FACE + PARTS * x + part, (mx, 0, 0), here, xh.at[x, span], CHUNK * cj // 8)
        add(geo_in, GEO + x, (mx, 0, 0), geo, geor.at[x], slots // 128)
        add(x_out, TERMS + x, (mx, 0, 0), terms, termr.at[x], 0, 1 + x)
        for mz, z in STEPS:
            n = 2 * x + z
            add(rim_in[x], RIM + x, (mx, 0, mz), zs.at[z, :, edge_tile(x)], xzh.at[n])
            add(out, OUT, (mx, 0, mz), dxzs.at[n], dxzr.at[n])
            moves.append((mx, 0, mz))
        moves.append((mx, 0, 0))
    for my, y in STEPS:
        add(y_in, Y_IN, (0, my, 0), ys.at[y], yh.at[y], NUM_FIELDS)
        add(out, OUT, (0, my, 0), dys.at[y, :, 0:ci], dyr.at[y], NUM_TERMS)
        for mz, z in STEPS:
            add(z_in, Z_IN, (0, my, mz), ez.at[z], yzh.at[2 * y + z])
            add(out, OUT, (0, my, mz), dyzs.at[z], dyzr.at[2 * y + z])
            moves.append((0, my, mz))
        moves.append((0, my, 0))
    for mz, z in STEPS:
        add(z_in, Z_IN, (0, 0, mz), zs.at[z], zh.at[z], inner // 128)
        add(out, OUT, (0, 0, mz), dzs.at[z, :, 0:ci], dzr.at[z], NUM_TERMS)
        moves.append((0, 0, mz))
    moves.sort(key=lambda move: -sum(abs(step) for step in move))

    barrier = pltpu.get_barrier_semaphore()
    for move in moves:

        @pl.when(exists(move, 1))
        def _():
            pl.semaphore_signal(barrier, inc=1, device_id=peer(move), device_id_type=MESH)

    loads = [
        pltpu.make_async_copy(vel, fields.at[0:3], load_sem.at[0]),
        pltpu.make_async_copy(sca, fields.at[3:6], load_sem.at[1]),
    ]
    small = [
        pltpu.make_async_copy(src, dst, load_sem.at[2 + n])
        for n, (src, dst) in enumerate(
            [
                (pos_in, pos),
                (li_in, li),
                (lj_in, lj),
                (lk_in, lk),
                (mot_in, mot),
                (heat_in, heat),
                (size_in, size),
            ]
        )
    ]
    for load in loads + small:
        load.start()
    xys[...] = jnp.zeros_like(xys)
    for load in loads:
        load.wait()
    for y in range(2):
        row = face(y, cj)
        ys[y] = fields[:, :, row, :]
        for x in range(2):
            xys[2 * x + y, 0:NUM_FIELDS] = fields[:, face(x, ci), row, :]
    pl.semaphore_wait(barrier, sum(exists(move, 1).astype(jnp.int32) for move in moves))
    for message in y_in + faces[0] + faces[1]:
        message.start()

    zs[...] = jnp.zeros_like(zs)
    dxys[...] = jnp.zeros_like(dxys)
    dxzs[...] = jnp.zeros_like(dxzs)
    for message in y_in + z_in + rim_in[0] + rim_in[1] + out:
        message.blank()
    for f in range(NUM_FIELDS):
        turned = fields[f].reshape(inner, ck).T
        high, low = split(turned)
        ft_hi[f * ck : (f + 1) * ck] = high
        ft_lo[f * ck : (f + 1) * ck] = low
        zs[0, f : f + 1] = turned[ck - 1 : ck]
        zs[1, f : f + 1] = turned[0:1]
    rows = lax.broadcasted_iota(jnp.int32, (inner, 128), 0)
    cols = lanes_of((inner, 128))
    target = jnp.where(cols < cj + 8, (cols - cj) * cj + cj - 1, (cols - cj - 8) * cj)
    chosen = (rows == target) & (cols >= cj) & (cols < cj + 16)
    chosen = jnp.where(chosen, 1.0, 0.0).astype(BF16)
    high, low = split(zs[...].reshape(16, inner))
    ez[...] = (nn(high, chosen) + nn(low, chosen)).reshape(2, 8, 128)
    for message in z_in + rim_in[0] + rim_in[1]:
        message.start()

    for load in small:
        load.wait()
    xa, xb, lx = pair_weights(pos[0:1])
    ya, yb, ly = pair_weights(pos[1:2])
    za, zb, lz = pair_weights(pos[2:3])
    i0 = li[...].astype(F32) + lx
    j0 = lj[...].astype(F32) + ly
    k0 = lk[...].astype(F32) + lz

    def at(index, base, wa, wb):
        return jnp.where(base == index, wa, jnp.where(base + 1.0 == index, wb, 0.0))

    x_low, x_high = at(-1.0, i0, xa, xb), at(float(ci), i0, xa, xb)
    y_low, y_high = at(-1.0, j0, ya, yb), at(float(cj), j0, ya, yb)
    z_low, z_high = at(-1.0, k0, za, zb), at(float(ck), k0, za, zb)
    for n, row in enumerate((x_high, x_low, j0, k0, ya, yb, za, zb)):
        geo[n : n + 1] = row
    xt[0:ci] = spots(0, ci, i0, xa, xb)
    xt[ci : 2 * ci] = jnp.concatenate([x_low, x_high, jnp.zeros((ci - 2, slots), F32)], axis=0)
    across = spots(0, cj, j0, ya, yb)
    rims = [
        jnp.broadcast_to(y_low, (8, slots)),
        jnp.broadcast_to(y_high, (8, slots)),
        jnp.zeros((128 - cj - 16, slots), F32),
    ]
    high, low = split(jnp.concatenate([across] + rims, axis=0))
    yt[0:128] = high
    yt[128:256] = low
    for i in range(ci):
        high, low = split(xt[i : i + 1] * across)
        w_hi[i * cj : (i + 1) * cj] = high
        w_lo[i * cj : (i + 1) * cj] = low
    for n, row in enumerate((x_low, x_high)):
        high, low = split(row * across)
        wx[n, 0:cj] = high
        wx[n, cj : 2 * cj] = high
        wx[n, 2 * cj : 3 * cj] = low
    corners = [a * b for a in (x_low, x_high) for b in (y_low, y_high)]
    for n, row in enumerate(corners):
        cw[n : n + 1] = row
    sides = [xt[0:ci] * y_low, xt[0:ci] * y_high]
    group = wy.shape[0] // 4
    filler = [jnp.zeros((group - 2 * ci - 4, slots), F32)]
    high, low = split(jnp.concatenate(sides + corners + filler, axis=0))
    wy[0:group] = high
    wy[group : 2 * group] = high
    wy[2 * group : 3 * group] = low
    wy[3 * group : 4 * group] = jnp.zeros((group, slots), BF16)
    line[...] = spots(0, ck, k0, za, zb)
    high, low = split(line[...])
    lines[0:ck] = high
    lines[ck : 2 * ck] = low

    for message in geo_in:
        message.start()

    width = 256

    def collect(got, here, number):
        return [
            jnp.sum(got[n * ck : (n + 1) * ck] * line[:, here], axis=0, keepdims=True)
            for n in range(number)
        ]

    for s in range(0, slots, width):
        here = slice(s, s + width)
        got = nn(ft_hi[...], w_hi[:, here])
        got += nn(ft_hi[...], w_lo[:, here])
        got += nn(ft_lo[...], w_hi[:, here])
        for f, part in enumerate(collect(got, here, NUM_FIELDS)):
            sampled[f : f + 1, here] = part

    arrive(y_in)

    def turn(flats):
        out = []
        for flat in flats:
            high = flat.astype(BF16).astype(F32)
            out.append(jnp.concatenate([high, flat - high, high], axis=0).T.astype(BF16))
        return jnp.concatenate(out, axis=0)

    def more(left, right, span):
        rest = []
        for s in range(0, slots, width):
            here = slice(s, s + width)
            got = nn(left, right[:, here])
            for f, part in zip(span, collect(got, here, len(span))):
                sampled[f : f + 1, here] += part
            rest.append(got[len(span) * ck :])
        return jnp.concatenate(rest, axis=1) if left.shape[0] > len(span) * ck else None

    empty = jnp.zeros((group - 2 * ci - 4, ck), F32)
    left = turn(
        [
            jnp.concatenate(
                [yh[0, f], yh[1, f]] + [xyh[q, f : f + 1] for q in range(4)] + [empty], axis=0
            )
            for f in range(NUM_FIELDS)
        ]
    )
    more(left, wy[0 : 3 * group], range(NUM_FIELDS))

    arrive(z_in)
    lanes = lanes_of((8, 128))
    body = lanes < cj

    def half(tile, odd):
        return jnp.where(body, pltpu.roll(tile, 128 - cj, 1) if odd else tile, 0.0)

    def pick(tile, lane):
        return jnp.where(lanes == lane, tile, 0.0)

    for z in range(2):
        for i in range(ci):
            first = i * cj // 128 * 128
            block = half(zh[z, :, first : first + 128], i * cj % 128 != 0)
            block += pick(yzh[z], cj + i) + pick(yzh[2 + z], cj + 8 + i)
            ztable[z, i] = block
    high, low = split(ztable[...].reshape(2 * ci * 8, 128))
    got = nn(jnp.concatenate([high, low], axis=0), yt[0:128])
    got = got[0 : 2 * ci * 8] + got[2 * ci * 8 :] + nn(high, yt[128:256])
    for z, rim in enumerate((z_low, z_high)):
        total = None
        for i in range(ci):
            first = (z * ci + i) * 8
            part = got[first : first + 8] * xt[i : i + 1]
            total = part if total is None else total + part
        sampled[...] += total * rim

    for x in range(2):

        @pl.when(exists(faces[x][0].move, -1))
        def _():
            i = face(x, ci)
            for part in range(PARTS):
                span = range(part * CHUNK, (part + 1) * CHUNK)
                faces[x][part].copy.wait_recv()
                if part < PARTS - 1:
                    more(turn([xh[x, f] for f in span]), wx[x], span)
                    continue
                arrive(rim_in[x])
                ends = []
                for z in range(2):
                    block = half(xzh[2 * x + z], i * cj % 128 != 0)
                    high = block.astype(BF16).astype(F32)
                    beside = jnp.where(body, high, pltpu.roll(block - high, cj, 1))
                    ends.append(jnp.concatenate([beside, high[:, 0:cj]], axis=1))
                ends = jnp.concatenate(ends, axis=0).astype(BF16)
                left = jnp.concatenate([turn([xh[x, f] for f in span]), ends], axis=0)
                rest = more(left, wx[x], span)
                for z, rim in enumerate((z_low, z_high)):
                    total = rest[z * 8 : z * 8 + 8]
                    for y in range(2):
                        lane = cj + 8 * y + i
                        tile = xyzh[4 * x + 2 * y + z]
                        total += tile[:, lane : lane + 1] * cw[2 * x + y : 2 * x + y + 1]
                    sampled[...] += total * rim

    gas = sampled[...]
    live = lanes_of((1, slots)) // TILE < tally[0]
    q = size[...]
    tp = heat[...]
    v = mot[...]
    drag = step_time / (0.5 * q)
    v_new = (v + drag * gas[0:3]) / (1.0 + drag)
    mass = q * jnp.sqrt(q)
    share = jnp.exp(4.0 * (tp - 1.0))
    decay = step_time * evap_rate * gas[5:6] * (share - gas[4:5])
    q_new = q - decay
    mass_new = q_new * jnp.sqrt(q_new)
    conduct = step_time * heat_rate * gas[5:6] / q
    tp_new = (tp + conduct * gas[3:4]) / (1.0 + conduct) - boiling_energy_drain * decay / q
    state[0:3] = jnp.where(live, v_new, v)
    state[3:4] = jnp.where(live, tp_new, tp)
    state[4:5] = jnp.where(live, q_new, q)
    terms[0:3] = jnp.where(live, mass * (v - v_new), 0.0)
    terms[3:4] = jnp.where(live, mass * (tp - tp_new), 0.0)
    terms[4:5] = jnp.where(live, mass - mass_new, 0.0)
    for message in x_out:
        message.start()

    part_rows = 2 * ci
    pieces = [xt[...] * terms[c : c + 1] for c in range(NUM_TERMS)]

    def fan(rims):
        return split(jnp.concatenate([piece * rim for rim in rims for piece in pieces], axis=0))

    def both(high, low, right):
        wide = nt(high, right)
        return wide[:, 0:128] + wide[:, 128:256] + nt(low, right[0:128])

    shape = (2, NUM_TERMS, part_rows, 128)
    high, low = fan((y_high, y_low))
    dys[...] = both(high, low, lines[...]).reshape(shape)
    for x in range(2):
        row = ci + 1 - x
        for y in range(2):
            for c in range(NUM_TERMS):
                dxys[2 * x + y, c : c + 1] = dys[y, c, row : row + 1]
    for message in out:
        if message.move[2] == 0:
            message.start()
    high, low = fan((z_high, z_low))
    dzs[...] = both(high, low, yt[...]).reshape(shape)
    for z in range(2):
        for x in range(2):
            row = ci + 1 - x
            for c in range(NUM_TERMS):
                dxzs[2 * x + z, c : c + 1] = dzs[z, c, row : row + 1]
        tile = jnp.zeros((8, 128), F32)
        for c in range(NUM_TERMS):
            keep = (lanes == cj + c) | (lanes == cj + 8 + c)
            tile = jnp.where(keep, dzs[z, c, 0:ci], tile)
        dyzs[z] = tile
    for message in out:
        if message.move[2] != 0:
            message.start()

    for a in range(0, NUM_TERMS, 2):
        b = min(a + 2, NUM_TERMS)
        for c in range(a, b):
            high, low = split(line[...] * terms[c : c + 1])
            src_hi[c * ck : (c + 1) * ck] = high
            src_lo[c * ck : (c + 1) * ck] = low
        span = slice(a * ck, b * ck)
        if b - a == 2:
            got = nt(w_hi[...], src_hi[span])
            got += nt(w_hi[...], src_lo[span])
            got += nt(w_lo[...], src_hi[span])
        else:
            got = nt(w_hi[...], jnp.concatenate([src_hi[span], src_lo[span]], axis=0))
            got = got[:, 0:ck] + got[:, ck:] + nt(w_lo[...], src_hi[span])
        for c in range(a, b):
            dep[c] = got[:, (c - a) * ck : (c - a + 1) * ck].reshape(ci, cj, ck)

    for x, (places, deposits) in enumerate(zip(geo_in, x_out)):
        plane = 0 if x == 0 else ci - 1

        @pl.when(exists(places.move, -1))
        def _():
            places.copy.wait_recv()
            rows = [geor[x, n : n + 1] for n in range(8)]
            there = spots(0, cj, rows[2], rows[4], rows[5]) * rows[x]
            along = jnp.concatenate(split(spots(0, ck, rows[3], rows[6], rows[7])), axis=0)
            deposits.copy.wait_recv()
            high, low = split(
                jnp.concatenate([there * termr[x, c : c + 1] for c in range(NUM_TERMS)], axis=0)
            )
            got = both(high, low, along)
            for c in range(NUM_TERMS):
                dep[c, plane] += got[c * cj : (c + 1) * cj]

    arrive(out)
    drain(send_sem.at[0], made, 1)
    for message in x_out:
        message.leave()


def finish(
    part, old, dyr, dxyr, dzr, dxzr, dyzr, dxyzr, dep_out, state_out, dep, sem
):
    ci, cj, ck = dep.shape[1:]
    terms = dep.shape[0]
    side = pltpu.make_async_copy(old, state_out, sem.at[terms])
    side.start()
    lanes = lanes_of((8, 128))
    rows = lax.broadcasted_iota(jnp.int32, (8, 128), 0)
    ends = (0, ck - 1)

    def at_ends(first, second, where):
        return jnp.where(where == ends[0], first, jnp.where(where == ends[1], second, 0.0))

    corner = []
    for x in range(2):
        for y in range(2):
            lane = cj + 8 if y == 0 else cj
            first, second = (dxyzr[4 * x + 2 * y + z, :, lane : lane + 1] for z in range(2))
            corner.append(dxyr[2 * x + y] + at_ends(first, second, lanes))
    row = lax.broadcasted_iota(jnp.int32, (32, ci * ck), 0)
    row = jnp.where(row < 16, row, row - 16)
    lane = jnp.where(row < 8, row * ck, (row - 8) * ck + ck - 1)
    spot = jnp.where(lanes_of((32, ci * ck)) == lane, 1.0, 0.0).astype(BF16)
    outs = []
    for c in range(terms):
        block = []
        for z in range(2):
            total = dzr[z, c]
            for x in range(2):
                plane = 0 if x == 0 else ci - 1
                total += jnp.where(rows == plane, dxzr[2 * x + z, c : c + 1], 0.0)
            block.append(total)
        block = jnp.concatenate(block, axis=0)
        high = block.astype(BF16).astype(F32)
        turned = jnp.concatenate([high, block - high], axis=0).T[0:cj].astype(BF16)
        ends_of = nn(turned, spot)
        for i in range(ci):
            dep[c, i] = part[c, i] + ends_of[:, i * ck : (i + 1) * ck]
        for y in range(2):
            row = 0 if y == 0 else cj - 1
            lane = cj + 8 + c if y == 0 else cj + c
            first, second = (dyzr[2 * y + z, :, lane : lane + 1] for z in range(2))
            dep[c, :, row, :] += dyr[y, c] + at_ends(first, second, lanes)
            for x in range(2):
                plane = 0 if x == 0 else ci - 1
                dep[c, plane, row : row + 1, :] += corner[2 * x + y][c : c + 1]
        out = pltpu.make_async_copy(dep.at[c], dep_out.at[c], sem.at[c])
        out.start()
        outs.append(out)
    for out in outs:
        out.wait()
    side.wait()


def local(counts, vel, sca, pos, mot, heat, size, li, lj, lk, tally):
    ci, cj, ck = vel.shape[1:]
    slots = heat.shape[0]
    inner = ci * cj
    vmem = pl.BlockSpec(memory_space=pltpu.VMEM)
    hbm = pl.BlockSpec(memory_space=pltpu.HBM)
    row = lambda value: value.reshape(1, slots)
    pin = lambda value: pltpu.with_memory_space_constraint(value, pltpu.HBM)
    tile = (8, 128)
    group = -(-(2 * ci + 4) // 16) * 16
    f32 = lambda *shape: pltpu.VMEM(shape, F32)
    i32 = lambda *shape: pltpu.VMEM(shape, jnp.int32)
    b16 = lambda *shape: pltpu.VMEM(shape, BF16)
    struct = lambda *shape: jax.ShapeDtypeStruct(shape, F32)
    scratch = [
        f32(NUM_FIELDS, ci, cj, ck),
        f32(3, slots),
        f32(3, slots),
        f32(1, slots),
        f32(1, slots),
        i32(1, slots),
        i32(1, slots),
        i32(1, slots),
        b16(NUM_FIELDS * ck, inner),
        b16(NUM_FIELDS * ck, inner),
        b16(inner, slots),
        b16(inner, slots),
        b16(2, 3 * cj, slots),
        b16(4 * group, slots),
        f32(2 * ci, slots),
        f32(4, slots),
        b16(256, slots),
        f32(ck, slots),
        b16(2 * ck, slots),
        f32(2, ci, *tile),
        b16(NUM_TERMS * ck, slots),
        b16(NUM_TERMS * ck, slots),
        f32(8, slots),
        f32(8, slots),
        f32(NUM_TERMS, slots),
        f32(2, NUM_FIELDS, cj, ck),
        f32(2, NUM_FIELDS, ci, ck),
        f32(4, *tile),
        f32(2, 8, inner),
        f32(4, *tile),
        f32(4, *tile),
        f32(8, *tile),
        f32(2, 8, slots),
        f32(2, NUM_TERMS, slots),
        f32(2, NUM_FIELDS, ci, ck),
        f32(4, *tile),
        f32(2, 8, inner),
        f32(2, *tile),
        f32(2, NUM_TERMS, 2 * ci, ck),
        f32(4, *tile),
        f32(2, NUM_TERMS, 2 * ci, ck),
        f32(4, *tile),
        f32(2, *tile),
        f32(256, *tile),
        pltpu.SemaphoreType.DMA((9,)),
        pltpu.SemaphoreType.DMA((3,)),
        pltpu.SemaphoreType.DMA((9 + 2 * PARTS,)),
    ]
    results = (
        struct(NUM_TERMS, ci, cj, ck),
        struct(NUM_TERMS, slots),
        struct(2, NUM_TERMS, ci, ck),
        struct(4, *tile),
        struct(2, NUM_TERMS, ci, ck),
        struct(4, *tile),
        struct(4, *tile),
        struct(8, *tile),
    )
    arrays = (vel, sca, pos, mot, row(heat), row(size), row(li), row(lj), row(lk))
    parts = pl.pallas_call(
        functools.partial(kernel, counts),
        out_shape=results,
        in_specs=[hbm] * len(arrays) + [pl.BlockSpec(memory_space=pltpu.SMEM)],
        out_specs=(vmem,) * len(results),
        scratch_shapes=scratch,
        compiler_params=pltpu.CompilerParams(
            collective_id=0, has_side_effects=True, vmem_limit_bytes=32 * 2**20
        ),
    )(*[pin(value) for value in arrays], tally)
    return pl.pallas_call(
        finish,
        out_shape=results[0:2],
        in_specs=[vmem] * len(results),
        out_specs=(pl.BlockSpec(memory_space=pl.ANY),) * 2,
        scratch_shapes=[
            f32(NUM_TERMS, ci, cj, ck),
            pltpu.SemaphoreType.DMA((NUM_TERMS + 1,)),
        ],
        compiler_params=pltpu.CompilerParams(vmem_limit_bytes=12 * 2**20),
    )(*parts)


def solution(mesh):
    bricks = P(None, AXES[0], AXES[1], AXES[2])
    rows = P(None, AXES)
    flat = P(AXES)
    counts = tuple(mesh.shape[axis] for axis in AXES)
    return jax.shard_map(
        functools.partial(local, counts),
        mesh=mesh,
        in_specs=(bricks, bricks, rows, rows) + (flat,) * 6,
        out_specs=(bricks, rows),
        check_vma=False,
    )
```

```python
import functools
import itertools

import jax
import jax.numpy as jnp
from jax import lax
from jax.experimental import pallas as pl
from jax.experimental.pallas import tpu as pltpu
from jax.sharding import PartitionSpec as P

TILE = 128
AXES = ("gx", "gy", "gz")
MESH = pl.DeviceIdType.MESH
F32 = jnp.float32
BF16 = jnp.bfloat16

step_time = 0.25
evap_rate = 1.0
heat_rate = 2.0
boiling_energy_drain = 0.3

STEPS = ((1, 0), (-1, 1))
NUM_TERMS = 5
NUM_FIELDS = 6
PARTS = 3
CHUNK = NUM_FIELDS // PARTS


def split(value):
    high = value.astype(BF16)
    return high, (value - high.astype(F32)).astype(BF16)


def nn(a, b):
    return lax.dot_general(a, b, (((1,), (0,)), ((), ())), preferred_element_type=F32)


def nt(a, b):
    return lax.dot_general(a, b, (((1,), (1,)), ((), ())), preferred_element_type=F32)


def pair_weights(offset):
    lower = jnp.where(offset < 0.0, -1.0, 0.0)
    first = jnp.maximum(0.0, 1.0 - jnp.abs(offset - lower))
    second = jnp.maximum(0.0, 1.0 - jnp.abs(offset - (lower + 1.0)))
    return first, second, lower


def lanes_of(shape):
    return lax.broadcasted_iota(jnp.int32, shape, len(shape) - 1)


def spots(first, count, base, wa, wb):
    rows = (lax.broadcasted_iota(jnp.int32, (count, base.shape[1]), 0) + first).astype(F32)
    return jnp.where(rows == base, wa, jnp.where(rows == base + 1.0, wb, 0.0))


def kernel(
    counts,
    vel,
    sca,
    pos_in,
    mot_in,
    heat_in,
    size_in,
    li_in,
    lj_in,
    lk_in,
    tally,
    dep,
    state,
    dyr,
    dxyr,
    dzr,
    dxzr,
    dyzr,
    dxyzr,
    fields,
    pos,
    mot,
    heat,
    size,
    li,
    lj,
    lk,
    ft_hi,
    ft_lo,
    w_hi,
    w_lo,
    wx,
    xt,
    cw,
    yt,
    line,
    lines,
    ztable,
    src_hi,
    src_lo,
    sampled,
    geo,
    terms,
    xh,
    yh,
    xyh,
    zh,
    xzh,
    yzh,
    xyzh,
    geor,
    termr,
    ys,
    xys,
    zs,
    ez,
    dys,
    dxys,
    dzs,
    dxzs,
    dyzs,
    xs,
    edges,
    fan_hi,
    fan_lo,
    gauge,
    load_sem,
    send_sem,
    recv_sem,
    near,
    far,
):
    ci, cj, ck = vel.shape[1:]
    slots = heat.shape[1]
    inner = ci * cj
    y_rows = wx.shape[1] - 3 * cj
    me = [lax.axis_index(axis) for axis in AXES]

    def exists(move, sign):
        good = None
        for d in range(3):
            step = sign * move[d]
            if step == 1:
                test = me[d] < counts[d] - 1
            elif step == -1:
                test = me[d] > 0
            else:
                continue
            good = test if good is None else jnp.logical_and(good, test)
        return good

    def peer(move):
        return tuple(lax.rem(me[d] + move[d] + counts[d], counts[d]) for d in range(3))

    class Message:
        def __init__(self, number, move, src, dst, tiles, post):
            self.move = move
            self.dst = dst
            self.tiles = tiles
            self.number = number
            self.copy = pltpu.make_async_remote_copy(
                src_ref=src,
                dst_ref=dst,
                send_sem=send_sem.at[post],
                recv_sem=recv_sem.at[number],
                device_id=peer(move),
                device_id_type=MESH,
            )

        def start(self):
            @pl.when(exists(self.move, 1))
            def _():
                self.copy.start()

        def blank(self):
            @pl.when(jnp.logical_not(exists(self.move, -1)))
            def _():
                self.dst[...] = jnp.zeros(self.dst.shape, F32)

        def leave(self):
            @pl.when(exists(self.move, 1))
            def _():
                self.copy.wait_send()

    def totals(messages, sign):
        sides = []
        for extent in counts:
            low, high = (-1,), (1,)
            sides.append([()] if extent == 1 else [low, high] + [low + high] * (extent > 2))
        found = set()
        for place in itertools.product(*sides):
            there = [
                message.tiles
                for message in messages
                if all(
                    step == 0 or sign * step in side for step, side in zip(message.move, place)
                )
            ]
            found.add(sum(there))
        return sorted(found - {0})

    def drain(sem, messages, sign):
        count = sum(
            jnp.where(exists(message.move, sign), message.tiles, 0) for message in messages
        )
        for total in totals(messages, sign):

            @pl.when(count == total)
            def _():
                some = gauge.at[0:total]
                pltpu.make_async_copy(some, some, sem).wait()

    def arrive(messages):
        drain(recv_sem.at[messages[0].number], messages, -1)

    made = []

    def add(group, number, move, src, dst, tiles=1, post=0):
        message = Message(number, move, src, dst, tiles, post)
        made.append(message)
        group.append(message)

    Y_IN, Z_IN, OUT, GEO, TERMS, RIM, FACE = 0, 1, 2, 3, 5, 7, 9
    face = lambda n, extent: extent - 1 if n == 0 else 0
    edge_tile = lambda n: pl.ds(face(n, ci) * cj // 128 * 128, 128)
    y_in, xy_in, z_in, yz_in, geo_in, x_out, out = [], [], [], [], [], [], []
    faces, rim_in = [[], []], [[], []]
    for mx, x in STEPS:
        for my, y in STEPS:
            add(xy_in, Y_IN, (mx, my, 0), xys.at[2 * x + y], xyh.at[2 * x + y])
            add(out, OUT, (mx, my, 0), dxys.at[2 * x + y], dxyr.at[2 * x + y])
            for mz, z in STEPS:
                n = 4 * x + 2 * y + z
                add(rim_in[x], RIM + x, (mx, my, mz), ez.at[z], xyzh.at[n])
                add(out, OUT, (mx, my, mz), dxzs.at[2 * x + z], dxyzr.at[n])
        for part in range(PARTS):
            span = slice(part * CHUNK, (part + 1) * CHUNK)
            here = xs.at[x, span]
            add(faces[x], FACE + PARTS * x + part, (mx, 0, 0), here, xh.at[x, span], CHUNK * cj // 8)
        add(geo_in, GEO + x, (mx, 0, 0), geo, geor.at[x], slots // 128)
        add(x_out, TERMS + x, (mx, 0, 0), terms, termr.at[x], 0, 1 + x)
        for mz, z in STEPS:
            n = 2 * x + z
            add(rim_in[x], RIM + x, (mx, 0, mz), zs.at[z, :, edge_tile(x)], xzh.at[n])
            add(out, OUT, (mx, 0, mz), dxzs.at[n], dxzr.at[n])
    for my, y in STEPS:
        add(y_in, Y_IN, (0, my, 0), ys.at[y], yh.at[y], NUM_FIELDS)
        add(out, OUT, (0, my, 0), dys.at[y, :, 0:ci], dyr.at[y], NUM_TERMS)
        for mz, z in STEPS:
            add(yz_in, Z_IN, (0, my, mz), ez.at[z], yzh.at[2 * y + z])
            add(out, OUT, (0, my, mz), dyzs.at[z], dyzr.at[2 * y + z])
    for mz, z in STEPS:
        add(z_in, Z_IN, (0, 0, mz), zs.at[z], zh.at[z], inner // 128)
        add(out, OUT, (0, 0, mz), dzs.at[z, :, 0:ci], dzr.at[z], NUM_TERMS)

    def signal(sem, move):
        @pl.when(exists(move, 1))
        def _():
            pl.semaphore_signal(sem, inc=1, device_id=peer(move), device_id_type=MESH)

    def heard(sem, moves):
        pl.semaphore_wait(sem, sum(exists(move, -1).astype(jnp.int32) for move in moves))


    x_moves = [(step, 0, 0) for step, _ in STEPS]
    y_moves = [(0, step, 0) for step, _ in STEPS]
    z_moves = [(0, 0, step) for step, _ in STEPS]
    barrier = pltpu.get_barrier_semaphore()
    for move in z_moves + x_moves + y_moves:
        signal(barrier, move)

    def load(src, dst, number):
        copy = pltpu.make_async_copy(src, dst, load_sem.at[number])
        copy.start()
        return copy

    def loaded(whole, number):
        pltpu.make_async_copy(whole, whole, load_sem.at[number]).wait()

    for x, move in enumerate(x_moves):

        @pl.when(exists(move, 1))
        def _():
            load(vel.at[:, face(x, ci)], xs.at[x, 0:3], x)
            load(sca.at[:, face(x, ci)], xs.at[x, 3:6], x)

    load(vel, fields.at[0:3], 2)
    load(sca, fields.at[3:6], 2)
    pairs = [(pos_in, pos), (mot_in, mot), (li_in, li), (lj_in, lj), (lk_in, lk)]
    pairs += [(heat_in, heat), (size_in, size)]
    small = [load(src, dst, 3 + n) for n, (src, dst) in enumerate(pairs)]

    xys[...] = jnp.zeros_like(xys)
    zs[...] = jnp.zeros_like(zs)
    dxys[...] = jnp.zeros_like(dxys)
    dxzs[...] = jnp.zeros_like(dxzs)
    for message in y_in + xy_in + z_in + yz_in + rim_in[0] + rim_in[1] + out:
        message.blank()
    rows = lax.broadcasted_iota(jnp.int32, (inner, 128), 0)
    cols = lanes_of((inner, 128))
    target = jnp.where(cols < cj + 8, (cols - cj) * cj + cj - 1, (cols - cj - 8) * cj)
    chosen = (rows == target) & (cols >= cj) & (cols < cj + 16)
    edges[...] = jnp.where(chosen, 1.0, 0.0).astype(BF16)

    for x, move in enumerate(x_moves):

        @pl.when(exists(move, 1))
        def _():
            loaded(xs.at[x], x)

    heard(barrier, x_moves + y_moves + z_moves)
    for move in y_moves:
        signal(near, move)
    for part in range(PARTS - 1):
        for x in range(2):
            faces[x][part].start()
    loaded(fields, 2)
    for y in range(2):
        row = face(y, cj)
        ys[y] = fields[:, :, row, :]
        for x in range(2):
            xys[2 * x + y, 0:NUM_FIELDS] = fields[:, face(x, ci), row, :]
    for message in y_in:
        message.start()
    heard(near, y_moves)
    for move in z_moves:
        signal(far, move)
    for message in xy_in + [faces[0][PARTS - 1], faces[1][PARTS - 1]]:
        message.start()

    for f in range(NUM_FIELDS):
        turned = fields[f].reshape(inner, ck).T
        high, low = split(turned)
        ft_hi[f * ck : (f + 1) * ck] = high
        ft_lo[f * ck : (f + 1) * ck] = low
        zs[0, f : f + 1] = turned[ck - 1 : ck]
        zs[1, f : f + 1] = turned[0:1]
    for message in z_in:
        message.start()
    high, low = split(zs[...].reshape(16, inner))
    ez[...] = (nn(high, edges[...]) + nn(low, edges[...])).reshape(2, 8, 128)
    heard(far, z_moves)
    for message in yz_in + rim_in[0] + rim_in[1]:
        message.start()

    for copy in small:
        copy.wait()
    xa, xb, lx = pair_weights(pos[0:1])
    ya, yb, ly = pair_weights(pos[1:2])
    za, zb, lz = pair_weights(pos[2:3])
    i0 = li[...].astype(F32) + lx
    j0 = lj[...].astype(F32) + ly
    k0 = lk[...].astype(F32) + lz

    def at(index, base, wa, wb):
        return jnp.where(base == index, wa, jnp.where(base + 1.0 == index, wb, 0.0))

    x_low, x_high = at(-1.0, i0, xa, xb), at(float(ci), i0, xa, xb)
    y_low, y_high = at(-1.0, j0, ya, yb), at(float(cj), j0, ya, yb)
    z_low, z_high = at(-1.0, k0, za, zb), at(float(ck), k0, za, zb)
    for n, row in enumerate((x_high, x_low, j0, k0, ya, yb, za, zb)):
        geo[n : n + 1] = row
    xt[0:ci] = spots(0, ci, i0, xa, xb)
    xt[ci : 2 * ci] = jnp.concatenate([x_low, x_high, jnp.zeros((ci - 2, slots), F32)], axis=0)
    across = spots(0, cj, j0, ya, yb)
    rims = [
        jnp.broadcast_to(y_low, (8, slots)),
        jnp.broadcast_to(y_high, (8, slots)),
        jnp.zeros((128 - cj - 16, slots), F32),
    ]
    high, low = split(jnp.concatenate([across] + rims, axis=0))
    yt[0:128] = high
    yt[128:256] = low
    for i in range(ci):
        high, low = split(xt[i : i + 1] * across)
        w_hi[i * cj : (i + 1) * cj] = high
        w_lo[i * cj : (i + 1) * cj] = low
    corners = [a * b for a in (x_low, x_high) for b in (y_low, y_high)]
    for n, row in enumerate(corners):
        cw[n : n + 1] = row
    ends = jnp.concatenate([xt[0:ci] * y_low, xt[0:ci] * y_high] + corners, axis=0)
    high = ends.astype(BF16).astype(F32)
    filler = jnp.zeros((y_rows - 3 * ends.shape[0], slots), F32)
    ends = jnp.concatenate([high, high, ends - high, filler], axis=0)
    first = exists(x_moves[0], -1)
    for n, row in enumerate((x_low, x_high)):
        high, low = split(row * across)
        wx[n, 0:cj] = high
        wx[n, cj : 2 * cj] = high
        wx[n, 2 * cj : 3 * cj] = low
        share = jnp.where(first, 1.0 - n, float(n))
        wx[n, 3 * cj :] = (ends * share).astype(BF16)
    line[...] = spots(0, ck, k0, za, zb)
    high, low = split(line[...])
    lines[0:ck] = high
    lines[ck : 2 * ck] = low

    for message in geo_in:
        message.start()

    width = 256

    def collect(got, here, number):
        return [
            jnp.sum(got[n * ck : (n + 1) * ck] * line[:, here], axis=0, keepdims=True)
            for n in range(number)
        ]

    for s in range(0, slots, width):
        here = slice(s, s + width)
        got = nn(ft_hi[...], w_hi[:, here])
        got += nn(ft_hi[...], w_lo[:, here])
        got += nn(ft_lo[...], w_hi[:, here])
        for f, part in enumerate(collect(got, here, NUM_FIELDS)):
            sampled[f : f + 1, here] = part


    def turn(x, f):
        beyond = xh[x, f]
        ends = jnp.concatenate(
            [yh[0, f], yh[1, f]] + [xyh[q, f : f + 1] for q in range(4)], axis=0
        )
        parts = []
        for flat in (beyond, ends):
            high = flat.astype(BF16).astype(F32)
            parts += [high, flat - high, high]
        parts.append(jnp.zeros((y_rows - 3 * ends.shape[0], ck), F32))
        return jnp.concatenate(parts, axis=0).T.astype(BF16)

    def more(left, right, span):
        rest = []
        for s in range(0, slots, width):
            here = slice(s, s + width)
            got = nn(left, right[:, here])
            for f, part in zip(span, collect(got, here, len(span))):
                sampled[f : f + 1, here] += part
            rest.append(got[len(span) * ck :])
        return jnp.concatenate(rest, axis=1) if left.shape[0] > len(span) * ck else None

    arrive(z_in + yz_in)
    lanes = lanes_of((8, 128))
    body = lanes < cj

    def half(tile, odd):
        return jnp.where(body, pltpu.roll(tile, 128 - cj, 1) if odd else tile, 0.0)

    def pick(tile, lane):
        return jnp.where(lanes == lane, tile, 0.0)

    for z in range(2):
        for i in range(ci):
            first = i * cj // 128 * 128
            block = half(zh[z, :, first : first + 128], i * cj % 128 != 0)
            block += pick(yzh[z], cj + i) + pick(yzh[2 + z], cj + 8 + i)
            ztable[z, i] = block
    high, low = split(ztable[...].reshape(2 * ci * 8, 128))
    got = nn(jnp.concatenate([high, low], axis=0), yt[0:128])
    got = got[0 : 2 * ci * 8] + got[2 * ci * 8 :] + nn(high, yt[128:256])
    for z, rim in enumerate((z_low, z_high)):
        total = None
        for i in range(ci):
            first = (z * ci + i) * 8
            part = got[first : first + 8] * xt[i : i + 1]
            total = part if total is None else total + part
        sampled[...] += total * rim

    arrive(y_in + xy_in)
    for x in range(2):

        @pl.when(exists(faces[x][0].move, -1))
        def _():
            i = face(x, ci)
            for part in range(PARTS):
                span = range(part * CHUNK, (part + 1) * CHUNK)
                faces[x][part].copy.wait_recv()
                if part < PARTS - 1:
                    more(jnp.concatenate([turn(x, f) for f in span], axis=0), wx[x], span)
                    continue
                arrive(rim_in[x])
                ends = []
                for z in range(2):
                    block = half(xzh[2 * x + z], i * cj % 128 != 0)
                    high = block.astype(BF16).astype(F32)
                    beside = jnp.where(body, high, pltpu.roll(block - high, cj, 1))
                    beyond = jnp.where(body, high, 0.0)
                    ends.append(jnp.concatenate([beside, beyond], axis=1))
                ends = jnp.concatenate(ends, axis=0).astype(BF16)
                left = jnp.concatenate([turn(x, f) for f in span] + [ends], axis=0)
                rest = more(left, wx[x], span)
                for z, rim in enumerate((z_low, z_high)):
                    total = rest[z * 8 : z * 8 + 8]
                    for y in range(2):
                        lane = cj + 8 * y + i
                        tile = xyzh[4 * x + 2 * y + z]
                        total += tile[:, lane : lane + 1] * cw[2 * x + y : 2 * x + y + 1]
                    sampled[...] += total * rim

    gas = sampled[...]
    live = lanes_of((1, slots)) // TILE < tally[0]
    q = size[...]
    tp = heat[...]
    v = mot[...]
    drag = step_time / (0.5 * q)
    v_new = (v + drag * gas[0:3]) / (1.0 + drag)
    mass = q * jnp.sqrt(q)
    share = jnp.exp(4.0 * (tp - 1.0))
    decay = step_time * evap_rate * gas[5:6] * (share - gas[4:5])
    q_new = q - decay
    mass_new = q_new * jnp.sqrt(q_new)
    conduct = step_time * heat_rate * gas[5:6] / q
    tp_new = (tp + conduct * gas[3:4]) / (1.0 + conduct) - boiling_energy_drain * decay / q
    state[0:3] = jnp.where(live, v_new, v)
    state[3:4] = jnp.where(live, tp_new, tp)
    state[4:5] = jnp.where(live, q_new, q)
    terms[0:3] = jnp.where(live, mass * (v - v_new), 0.0)
    terms[3:4] = jnp.where(live, mass * (tp - tp_new), 0.0)
    terms[4:5] = jnp.where(live, mass - mass_new, 0.0)
    for message in x_out:
        message.start()

    part_rows = 2 * ci
    pieces = [xt[...] * terms[c : c + 1] for c in range(NUM_TERMS)]

    def fan(rims):
        return split(jnp.concatenate([piece * rim for rim in rims for piece in pieces], axis=0))

    def both(high, low, right):
        wide = nt(high, right)
        return wide[:, 0:128] + wide[:, 128:256] + nt(low, right[0:128])

    shape = (2, NUM_TERMS, part_rows, 128)
    fan_hi[0], fan_lo[0] = fan((z_high, z_low))
    fan_hi[1], fan_lo[1] = fan((y_high, y_low))
    dzs[...] = both(fan_hi[0], fan_lo[0], yt[...]).reshape(shape)
    for z in range(2):
        for x in range(2):
            row = ci + 1 - x
            for c in range(NUM_TERMS):
                dxzs[2 * x + z, c : c + 1] = dzs[z, c, row : row + 1]
        tile = jnp.zeros((8, 128), F32)
        for c in range(NUM_TERMS):
            keep = (lanes == cj + c) | (lanes == cj + 8 + c)
            tile = jnp.where(keep, dzs[z, c, 0:ci], tile)
        dyzs[z] = tile
    for message in out:
        if message.move[2] != 0:
            message.start()
    dys[...] = both(fan_hi[1], fan_lo[1], lines[...]).reshape(shape)
    for x in range(2):
        row = ci + 1 - x
        for y in range(2):
            for c in range(NUM_TERMS):
                dxys[2 * x + y, c : c + 1] = dys[y, c, row : row + 1]
    for message in out:
        if message.move[2] == 0:
            message.start()

    for a in range(0, NUM_TERMS, 2):
        b = min(a + 2, NUM_TERMS)
        for c in range(a, b):
            high, low = split(line[...] * terms[c : c + 1])
            src_hi[c * ck : (c + 1) * ck] = high
            src_lo[c * ck : (c + 1) * ck] = low
        span = slice(a * ck, b * ck)
        if b - a == 2:
            got = nt(w_hi[...], src_hi[span])
            got += nt(w_hi[...], src_lo[span])
            got += nt(w_lo[...], src_hi[span])
        else:
            got = nt(w_hi[...], jnp.concatenate([src_hi[span], src_lo[span]], axis=0))
            got = got[:, 0:ck] + got[:, ck:] + nt(w_lo[...], src_hi[span])
        for c in range(a, b):
            dep[c] = got[:, (c - a) * ck : (c - a + 1) * ck].reshape(ci, cj, ck)

    for x, (places, deposits) in enumerate(zip(geo_in, x_out)):
        plane = 0 if x == 0 else ci - 1

        @pl.when(exists(places.move, -1))
        def _():
            places.copy.wait_recv()
            rows = [geor[x, n : n + 1] for n in range(8)]
            there = spots(0, cj, rows[2], rows[4], rows[5]) * rows[x]
            along = jnp.concatenate(split(spots(0, ck, rows[3], rows[6], rows[7])), axis=0)
            deposits.copy.wait_recv()
            high, low = split(
                jnp.concatenate([there * termr[x, c : c + 1] for c in range(NUM_TERMS)], axis=0)
            )
            got = both(high, low, along)
            for c in range(NUM_TERMS):
                dep[c, plane] += got[c * cj : (c + 1) * cj]

    arrive(out)
    drain(send_sem.at[0], made, 1)
    for message in x_out:
        message.leave()


def finish(
    part, old, dyr, dxyr, dzr, dxzr, dyzr, dxyzr, dep_out, state_out, dep, sem
):
    ci, cj, ck = dep.shape[1:]
    terms = dep.shape[0]
    side = pltpu.make_async_copy(old, state_out, sem.at[terms])
    side.start()
    lanes = lanes_of((8, 128))
    rows = lax.broadcasted_iota(jnp.int32, (8, 128), 0)
    ends = (0, ck - 1)

    def at_ends(first, second, where):
        return jnp.where(where == ends[0], first, jnp.where(where == ends[1], second, 0.0))

    corner = []
    for x in range(2):
        for y in range(2):
            lane = cj + 8 if y == 0 else cj
            first, second = (dxyzr[4 * x + 2 * y + z, :, lane : lane + 1] for z in range(2))
            corner.append(dxyr[2 * x + y] + at_ends(first, second, lanes))
    row = lax.broadcasted_iota(jnp.int32, (32, ci * ck), 0)
    row = jnp.where(row < 16, row, row - 16)
    lane = jnp.where(row < 8, row * ck, (row - 8) * ck + ck - 1)
    spot = jnp.where(lanes_of((32, ci * ck)) == lane, 1.0, 0.0).astype(BF16)
    outs = []
    for c in range(terms):
        block = []
        for z in range(2):
            total = dzr[z, c]
            for x in range(2):
                plane = 0 if x == 0 else ci - 1
                total += jnp.where(rows == plane, dxzr[2 * x + z, c : c + 1], 0.0)
            block.append(total)
        block = jnp.concatenate(block, axis=0)
        high = block.astype(BF16).astype(F32)
        turned = jnp.concatenate([high, block - high], axis=0).T[0:cj].astype(BF16)
        ends_of = nn(turned, spot)
        for i in range(ci):
            dep[c, i] = part[c, i] + ends_of[:, i * ck : (i + 1) * ck]
        for y in range(2):
            row = 0 if y == 0 else cj - 1
            lane = cj + 8 + c if y == 0 else cj + c
            first, second = (dyzr[2 * y + z, :, lane : lane + 1] for z in range(2))
            dep[c, :, row, :] += dyr[y, c] + at_ends(first, second, lanes)
            for x in range(2):
                plane = 0 if x == 0 else ci - 1
                dep[c, plane, row : row + 1, :] += corner[2 * x + y][c : c + 1]
        out = pltpu.make_async_copy(dep.at[c], dep_out.at[c], sem.at[c])
        out.start()
        outs.append(out)
    for out in outs:
        out.wait()
    side.wait()


def local(counts, vel, sca, pos, mot, heat, size, li, lj, lk, tally):
    ci, cj, ck = vel.shape[1:]
    slots = heat.shape[0]
    inner = ci * cj
    vmem = pl.BlockSpec(memory_space=pltpu.VMEM)
    hbm = pl.BlockSpec(memory_space=pltpu.HBM)
    row = lambda value: value.reshape(1, slots)
    pin = lambda value: pltpu.with_memory_space_constraint(value, pltpu.HBM)
    tile = (8, 128)
    y_rows = -(-3 * (2 * ci + 4) // 64) * 64
    f32 = lambda *shape: pltpu.VMEM(shape, F32)
    i32 = lambda *shape: pltpu.VMEM(shape, jnp.int32)
    b16 = lambda *shape: pltpu.VMEM(shape, BF16)
    struct = lambda *shape: jax.ShapeDtypeStruct(shape, F32)
    scratch = [
        f32(NUM_FIELDS, ci, cj, ck),
        f32(3, slots),
        f32(3, slots),
        f32(1, slots),
        f32(1, slots),
        i32(1, slots),
        i32(1, slots),
        i32(1, slots),
        b16(NUM_FIELDS * ck, inner),
        b16(NUM_FIELDS * ck, inner),
        b16(inner, slots),
        b16(inner, slots),
        b16(2, 3 * cj + y_rows, slots),
        f32(2 * ci, slots),
        f32(4, slots),
        b16(256, slots),
        f32(ck, slots),
        b16(2 * ck, slots),
        f32(2, ci, *tile),
        b16(NUM_TERMS * ck, slots),
        b16(NUM_TERMS * ck, slots),
        f32(8, slots),
        f32(8, slots),
        f32(NUM_TERMS, slots),
        f32(2, NUM_FIELDS, cj, ck),
        f32(2, NUM_FIELDS, ci, ck),
        f32(4, *tile),
        f32(2, 8, inner),
        f32(4, *tile),
        f32(4, *tile),
        f32(8, *tile),
        f32(2, 8, slots),
        f32(2, NUM_TERMS, slots),
        f32(2, NUM_FIELDS, ci, ck),
        f32(4, *tile),
        f32(2, 8, inner),
        f32(2, *tile),
        f32(2, NUM_TERMS, 2 * ci, ck),
        f32(4, *tile),
        f32(2, NUM_TERMS, 2 * ci, ck),
        f32(4, *tile),
        f32(2, *tile),
        f32(2, NUM_FIELDS, cj, ck),
        b16(inner, 128),
        b16(2, 4 * NUM_TERMS * ci, slots),
        b16(2, 4 * NUM_TERMS * ci, slots),
        f32(256, *tile),
        pltpu.SemaphoreType.DMA((10,)),
        pltpu.SemaphoreType.DMA((3,)),
        pltpu.SemaphoreType.DMA((9 + 2 * PARTS,)),
        pltpu.SemaphoreType.REGULAR,
        pltpu.SemaphoreType.REGULAR,
    ]
    results = (
        struct(NUM_TERMS, ci, cj, ck),
        struct(NUM_TERMS, slots),
        struct(2, NUM_TERMS, ci, ck),
        struct(4, *tile),
        struct(2, NUM_TERMS, ci, ck),
        struct(4, *tile),
        struct(4, *tile),
        struct(8, *tile),
    )
    arrays = (vel, sca, pos, mot, row(heat), row(size), row(li), row(lj), row(lk))
    parts = pl.pallas_call(
        functools.partial(kernel, counts),
        out_shape=results,
        in_specs=[hbm] * len(arrays) + [pl.BlockSpec(memory_space=pltpu.SMEM)],
        out_specs=(vmem,) * len(results),
        scratch_shapes=scratch,
        compiler_params=pltpu.CompilerParams(
            collective_id=0, has_side_effects=True, vmem_limit_bytes=32 * 2**20
        ),
    )(*[pin(value) for value in arrays], tally)
    return pl.pallas_call(
        finish,
        out_shape=results[0:2],
        in_specs=[vmem] * len(results),
        out_specs=(pl.BlockSpec(memory_space=pl.ANY),) * 2,
        scratch_shapes=[
            f32(NUM_TERMS, ci, cj, ck),
            pltpu.SemaphoreType.DMA((NUM_TERMS + 1,)),
        ],
        compiler_params=pltpu.CompilerParams(vmem_limit_bytes=12 * 2**20),
    )(*parts)


def solution(mesh):
    bricks = P(None, AXES[0], AXES[1], AXES[2])
    rows = P(None, AXES)
    flat = P(AXES)
    counts = tuple(mesh.shape[axis] for axis in AXES)
    return jax.shard_map(
        functools.partial(local, counts),
        mesh=mesh,
        in_specs=(bricks, bricks, rows, rows) + (flat,) * 6,
        out_specs=(bricks, rows),
        check_vma=False,
    )
```

```python
import functools
import itertools

import jax
import jax.numpy as jnp
from jax import lax
from jax.experimental import pallas as pl
from jax.experimental.pallas import tpu as pltpu
from jax.sharding import PartitionSpec as P

TILE = 128
AXES = ("gx", "gy", "gz")
MESH = pl.DeviceIdType.MESH
F32 = jnp.float32
BF16 = jnp.bfloat16

step_time = 0.25
evap_rate = 1.0
heat_rate = 2.0
boiling_energy_drain = 0.3

STEPS = ((1, 0), (-1, 1))
NUM_TERMS = 5
NUM_FIELDS = 6


def split(value):
    high = value.astype(BF16)
    return high, (value - high.astype(F32)).astype(BF16)


def nn(a, b):
    return lax.dot_general(a, b, (((1,), (0,)), ((), ())), preferred_element_type=F32)


def nt(a, b):
    return lax.dot_general(a, b, (((1,), (1,)), ((), ())), preferred_element_type=F32)


def pair_weights(offset):
    lower = jnp.where(offset < 0.0, -1.0, 0.0)
    first = jnp.maximum(0.0, 1.0 - jnp.abs(offset - lower))
    second = jnp.maximum(0.0, 1.0 - jnp.abs(offset - (lower + 1.0)))
    return first, second, lower


def lanes_of(shape):
    return lax.broadcasted_iota(jnp.int32, shape, len(shape) - 1)


def tent(count, place):
    rows = lax.broadcasted_iota(jnp.int32, (count, place.shape[1]), 0).astype(F32)
    return jnp.maximum(0.0, 1.0 - jnp.abs(rows - place))


def spots(first, count, base, wa, wb):
    rows = (lax.broadcasted_iota(jnp.int32, (count, base.shape[1]), 0) + first).astype(F32)
    return jnp.where(rows == base, wa, jnp.where(rows == base + 1.0, wb, 0.0))


def kernel(
    counts,
    vel,
    sca,
    pos_in,
    mot_in,
    heat_in,
    size_in,
    li_in,
    lj_in,
    lk_in,
    tally,
    dep,
    state,
    dyr,
    dxyr,
    dzr,
    dxzr,
    dyzr,
    dxyzr,
    fields,
    pos,
    mot,
    heat,
    size,
    li,
    lj,
    lk,
    ft_hi,
    ft_lo,
    w_hi,
    w_lo,
    corner,
    xt,
    yt,
    line,
    lines,
    src_hi,
    src_lo,
    sampled,
    geo,
    back,
    terms,
    there,
    along,
    alongs,
    w_there,
    face_f,
    yh,
    xyh,
    zh,
    xzh,
    yzh,
    xyzh,
    geor,
    backr,
    termr,
    ys,
    xys,
    zs,
    ez,
    dys,
    dzs,
    dyzs,
    dxyzs,
    edges,
    fan_hi,
    fan_lo,
    gauge,
    load_sem,
    send_sem,
    recv_sem,
    far,
):
    ci, cj, ck = vel.shape[1:]
    slots = heat.shape[1]
    inner = ci * cj
    me = [lax.axis_index(axis) for axis in AXES]

    def exists(move, sign):
        good = None
        for d in range(3):
            step = sign * move[d]
            if step == 1:
                test = me[d] < counts[d] - 1
            elif step == -1:
                test = me[d] > 0
            else:
                continue
            good = test if good is None else jnp.logical_and(good, test)
        return good

    def peer(move):
        return tuple(lax.rem(me[d] + move[d] + counts[d], counts[d]) for d in range(3))

    class Message:
        def __init__(self, number, move, src, dst, tiles, post):
            self.move = move
            self.dst = dst
            self.tiles = tiles
            self.number = number
            self.copy = pltpu.make_async_remote_copy(
                src_ref=src,
                dst_ref=dst,
                send_sem=send_sem.at[post],
                recv_sem=recv_sem.at[number],
                device_id=peer(move),
                device_id_type=MESH,
            )

        def start(self):
            @pl.when(exists(self.move, 1))
            def _():
                self.copy.start()

        def blank(self):
            @pl.when(jnp.logical_not(exists(self.move, -1)))
            def _():
                self.dst[...] = jnp.zeros(self.dst.shape, F32)

        def leave(self):
            @pl.when(exists(self.move, 1))
            def _():
                self.copy.wait_send()

    def totals(messages, sign):
        sides = []
        for extent in counts:
            low, high = (-1,), (1,)
            sides.append([()] if extent == 1 else [low, high] + [low + high] * (extent > 2))
        found = set()
        for place in itertools.product(*sides):
            there = [
                message.tiles
                for message in messages
                if all(
                    step == 0 or sign * step in side for step, side in zip(message.move, place)
                )
            ]
            found.add(sum(there))
        return sorted(found - {0})

    def drain(sem, messages, sign):
        count = sum(
            jnp.where(exists(message.move, sign), message.tiles, 0) for message in messages
        )
        for total in totals(messages, sign):

            @pl.when(count == total)
            def _():
                some = gauge.at[0:total]
                pltpu.make_async_copy(some, some, sem).wait()

    def arrive(messages):
        drain(recv_sem.at[messages[0].number], messages, -1)

    made = []

    def add(group, number, move, src, dst, tiles=1, post=0):
        message = Message(number, move, src, dst, tiles, post)
        made.append(message)
        group.append(message)

    Y_IN, Z_IN, RIM, OUT, GEO, TERMS, BACK = 0, 1, 2, 3, 4, 6, 8
    face = lambda n, extent: extent - 1 if n == 0 else 0
    edge_tile = lambda n: pl.ds(face(n, ci) * cj // 128 * 128, 128)
    y_in, xy_in, z_in, yz_in, geo_in, x_out, out = [], [], [], [], [], [], []
    rim_in, corner_in, back_in = [], [], []
    for mx, x in STEPS:
        for my, y in STEPS:
            add(xy_in, Y_IN, (mx, my, 0), xys.at[2 * x + y], xyh.at[2 * x + y])
            add(out, OUT, (mx, my, 0), dys.at[y, NUM_TERMS + x], dxyr.at[2 * x + y])
            for mz, z in STEPS:
                n = 4 * x + 2 * y + z
                add(corner_in, RIM, (mx, my, mz), ez.at[z], xyzh.at[n])
                add(out, OUT, (mx, my, mz), dxyzs.at[n], dxyzr.at[n])
        add(geo_in, GEO + x, (mx, 0, 0), geo, geor.at[x], 0, 1 + x)
        add(back_in, BACK + x, (mx, 0, 0), back.at[1 - x], backr.at[x], 0, 3 + x)
        add(x_out, TERMS + x, (mx, 0, 0), terms, termr.at[x], 0, 5 + x)
        for mz, z in STEPS:
            n = 2 * x + z
            add(rim_in, RIM, (mx, 0, mz), zs.at[z, :, edge_tile(x)], xzh.at[n])
            add(out, OUT, (mx, 0, mz), dzs.at[z, NUM_TERMS + x], dxzr.at[n])
    for my, y in STEPS:
        add(y_in, Y_IN, (0, my, 0), ys.at[y], yh.at[y], NUM_FIELDS)
        add(out, OUT, (0, my, 0), dys.at[y, 0:NUM_TERMS], dyr.at[y], NUM_TERMS)
        for mz, z in STEPS:
            add(yz_in, Z_IN, (0, my, mz), ez.at[z], yzh.at[2 * y + z])
            add(out, OUT, (0, my, mz), dyzs.at[z], dyzr.at[2 * y + z])
    for mz, z in STEPS:
        add(z_in, Z_IN, (0, 0, mz), zs.at[z], zh.at[z], inner // 128)
        add(out, OUT, (0, 0, mz), dzs.at[z, 0:NUM_TERMS], dzr.at[z], NUM_TERMS)

    def signal(sem, move):
        @pl.when(exists(move, 1))
        def _():
            pl.semaphore_signal(sem, inc=1, device_id=peer(move), device_id_type=MESH)

    def heard(sem, moves):
        pl.semaphore_wait(sem, sum(exists(move, -1).astype(jnp.int32) for move in moves))


    def turned_rows(flats, total):
        parts = []
        for flat in flats:
            high = flat.astype(BF16).astype(F32)
            parts += [high, flat - high, high]
        spare = total - sum(part.shape[0] for part in parts)
        if spare > 0:
            parts.append(jnp.zeros((spare, ck), F32))
        return jnp.concatenate(parts, axis=0).T.astype(BF16)

    x_moves = [(step, 0, 0) for step, _ in STEPS]
    y_moves = [(0, step, 0) for step, _ in STEPS]
    z_moves = [(0, 0, step) for step, _ in STEPS]
    xy_moves = [(mx, my, 0) for mx, _ in STEPS for my, _ in STEPS]
    met = xy_moves + z_moves + x_moves + y_moves
    barrier = pltpu.get_barrier_semaphore()
    for move in met:
        signal(barrier, move)

    def load(src, dst, number):
        pltpu.make_async_copy(src, dst, load_sem.at[number]).start()

    def loaded(whole, number):
        pltpu.make_async_copy(whole, whole, load_sem.at[number]).wait()

    pairs = [(pos_in, pos), (li_in, li), (lj_in, lj), (lk_in, lk)]
    pairs += [(mot_in, mot), (heat_in, heat), (size_in, size)]
    for (src, dst), number in zip(pairs, (1, 2, 2, 2, 3, 4, 4)):
        load(src, dst, number)
    load(vel, fields.at[0:3], 0)
    load(sca, fields.at[3:6], 0)

    xys[...] = jnp.zeros_like(xys)
    zs[...] = jnp.zeros_like(zs)
    for message in y_in + xy_in + z_in + yz_in + rim_in + corner_in + out:
        message.blank()
    rows = lax.broadcasted_iota(jnp.int32, (inner, 128), 0)
    cols = lanes_of((inner, 128))
    target = jnp.where(cols < cj + 8, (cols - cj) * cj + cj - 1, (cols - cj - 8) * cj)
    chosen = (rows == target) & (cols >= cj) & (cols < cj + 16)
    edges[...] = jnp.where(chosen, 1.0, 0.0).astype(BF16)

    loaded(pos, 1)
    loaded(gauge.at[0 : 3 * slots // 1024], 2)
    xa, xb, lx = pair_weights(pos[0:1])
    ya, yb, ly = pair_weights(pos[1:2])
    za, zb, lz = pair_weights(pos[2:3])
    i0 = li[...].astype(F32) + lx
    j0 = lj[...].astype(F32) + ly
    k0 = lk[...].astype(F32) + lz

    def at(index, base, wa, wb):
        return jnp.where(base == index, wa, jnp.where(base + 1.0 == index, wb, 0.0))

    x_low, x_high = at(-1.0, i0, xa, xb), at(float(ci), i0, xa, xb)
    y_low, y_high = at(-1.0, j0, ya, yb), at(float(cj), j0, ya, yb)
    z_low, z_high = at(-1.0, k0, za, zb), at(float(ck), k0, za, zb)
    y_place = lj[...].astype(F32) + pos[1:2]
    z_place = lk[...].astype(F32) + pos[2:3]
    for n, row in enumerate((x_high, x_low, y_place, z_place)):
        geo[n : n + 1] = row
    heard(barrier, met)
    for move in z_moves:
        signal(far, move)
    for message in geo_in:
        message.start()
    loaded(fields, 0)
    for y in range(2):
        row = face(y, cj)
        ys[y] = fields[:, :, row, :]
        for x in range(2):
            xys[2 * x + y, 0:NUM_FIELDS] = fields[:, face(x, ci), row, :]
    for message in xy_in + y_in:
        message.start()
    for f in range(NUM_FIELDS):
        turned = fields[f].reshape(inner, ck).T
        high, low = split(turned)
        ft_hi[f * ck : (f + 1) * ck] = high
        ft_lo[f * ck : (f + 1) * ck] = low
        zs[0, f : f + 1] = turned[ck - 1 : ck]
        zs[1, f : f + 1] = turned[0:1]
    for message in z_in:
        message.start()
    high, low = split(zs[...].reshape(16, inner))
    ez[...] = (nn(high, edges[...]) + nn(low, edges[...])).reshape(2, 8, 128)
    for x in range(2):
        plane = 0 if x == 0 else ci - 1

        @pl.when(exists(x_moves[x], -1))
        def _():
            for f in range(NUM_FIELDS):
                face_f[x, f * ck : (f + 1) * ck] = turned_rows([fields[f, plane]], 0)

    xt[0:ci] = spots(0, ci, i0, xa, xb)
    xt[ci : 2 * ci] = jnp.concatenate([x_low, x_high, jnp.zeros((ci - 2, slots), F32)], axis=0)
    across = spots(0, cj, j0, ya, yb)
    rims = [
        jnp.broadcast_to(y_low, (8, slots)),
        jnp.broadcast_to(y_high, (8, slots)),
        jnp.zeros((128 - cj - 16, slots), F32),
    ]
    high, low = split(jnp.concatenate([across] + rims, axis=0))
    yt[0:128] = high
    yt[128:256] = low
    corners = [a * b for a in (x_low, x_high) for b in (y_low, y_high)]
    for n, row in enumerate(corners):
        corner[n : n + 1] = row
    line[...] = spots(0, ck, k0, za, zb)
    high, low = split(line[...])
    lines[0:ck] = high
    lines[ck : 2 * ck] = low

    for i in range(ci):
        high, low = split(xt[i : i + 1] * across)
        w_hi[i * cj : (i + 1) * cj] = high
        w_lo[i * cj : (i + 1) * cj] = low

    heard(far, z_moves)
    for message in corner_in + rim_in + yz_in:
        message.start()

    width = 256

    def collect(got, table, here, target, start=0):
        parts = [
            jnp.sum(got[n * ck : (n + 1) * ck] * table[:, here], axis=0, keepdims=True)
            for n in range(got.shape[0] // ck)
        ]
        for n, part in enumerate(parts):
            target(start + n, here, part)

    def put(f, here, value):
        sampled[f : f + 1, here] = value

    def sample(blocks):
        for s in blocks:
            here = slice(s * width, (s + 1) * width)
            for start in range(0, NUM_FIELDS, NUM_FIELDS // 2):
                part = slice(start * ck, (start + NUM_FIELDS // 2) * ck)
                got = nn(ft_hi[part], w_hi[:, here])
                got += nn(ft_hi[part], w_lo[:, here])
                got += nn(ft_lo[part], w_hi[:, here])
                collect(got, line, here, put, start)

    sample(range(1))
    for x, places in enumerate(geo_in):

        @pl.when(exists(places.move, -1))
        def _():
            places.copy.wait_recv()
            there[x] = tent(cj, geor[x, 2:3]) * geor[x, x : x + 1]
            along[...] = tent(ck, geor[x, 3:4])
            high, low = split(along[...])
            alongs[x, 0:ck] = high
            alongs[x, ck : 2 * ck] = low
            high, low = split(there[x])
            w_there[0:cj] = high
            w_there[cj : 2 * cj] = high
            w_there[2 * cj : 3 * cj] = low

            def keep(f, here, value):
                back[x, f : f + 1, here] = value

            for s in range(0, slots, width):
                here = slice(s, s + width)
                collect(nn(face_f[x], w_there[:, here]), along, here, keep)
            back_in[1 - x].copy.start()

    sample(range(1, slots // width))
    arrive(y_in + xy_in)
    flat = NUM_FIELDS * ci
    ends = jnp.concatenate(
        [yh[y].reshape(flat, ck) for y in range(2)] + [xyh[q] for q in range(4)], axis=0
    )
    count = ends.shape[0]
    high, low = split(ends)
    got = nn(jnp.concatenate([high, low], axis=0), lines[0:ck])
    got = got[0:count] + got[count:] + nn(high, lines[ck : 2 * ck])
    rest = None
    for q in range(4):
        first = 2 * flat + q * 8
        part = got[first : first + 8] * corner[q : q + 1]
        rest = part if rest is None else rest + part
    for f in range(NUM_FIELDS):
        total = sampled[f : f + 1] + rest[f : f + 1]
        for y, rim in enumerate((y_low, y_high)):
            first = y * flat + f * ci
            part = got[first : first + ci] * xt[0:ci]
            total += jnp.sum(part, axis=0, keepdims=True) * rim
        sampled[f : f + 1] = total

    arrive(z_in + yz_in)
    lanes = lanes_of((8, 128))
    body = lanes < cj

    def half(tile, odd):
        return jnp.where(body, pltpu.roll(tile, 128 - cj, 1) if odd else tile, 0.0)

    def pick(tile, lane):
        return jnp.where(lanes == lane, tile, 0.0)

    def beyond(blocks, planes):
        count = 2 * planes.shape[0] * 8
        high, low = split(jnp.concatenate(blocks, axis=0))
        got = nn(jnp.concatenate([high, low], axis=0), yt[0:128])
        got = got[0:count] + got[count:] + nn(high, yt[128:256])
        for z, rim in enumerate((z_low, z_high)):
            total = None
            for b in range(planes.shape[0]):
                first = (z * planes.shape[0] + b) * 8
                part = got[first : first + 8] * planes[b : b + 1]
                total = part if total is None else total + part
            sampled[...] += total * rim

    blocks = []
    for z in range(2):
        for i in range(ci):
            first = i * cj // 128 * 128
            block = half(zh[z, :, first : first + 128], i * cj % 128 != 0)
            blocks.append(block + pick(yzh[z], cj + i) + pick(yzh[2 + z], cj + 8 + i))
    beyond(blocks, xt[0:ci])
    loaded(mot, 3)
    loaded(gauge.at[0 : 2 * slots // 1024], 4)
    for x, message in enumerate(back_in):

        @pl.when(exists(message.move, -1))
        def _():
            message.copy.wait_recv()
            sampled[0:NUM_FIELDS] += backr[x]

    arrive(rim_in + corner_in)
    blocks = []
    for z in range(2):
        for x in range(2):
            i = face(x, ci)
            block = half(xzh[2 * x + z], i * cj % 128 != 0)
            block += pick(xyzh[4 * x + z], cj + i) + pick(xyzh[4 * x + 2 + z], cj + 8 + i)
            blocks.append(block)
    beyond(blocks, xt[ci : ci + 2])

    gas = sampled[...]
    live = lanes_of((1, slots)) // TILE < tally[0]
    q = size[...]
    tp = heat[...]
    v = mot[...]
    drag = step_time / (0.5 * q)
    v_new = (v + drag * gas[0:3]) / (1.0 + drag)
    mass = q * jnp.sqrt(q)
    share = jnp.exp(4.0 * (tp - 1.0))
    decay = step_time * evap_rate * gas[5:6] * (share - gas[4:5])
    q_new = q - decay
    mass_new = q_new * jnp.sqrt(q_new)
    conduct = step_time * heat_rate * gas[5:6] / q
    tp_new = (tp + conduct * gas[3:4]) / (1.0 + conduct) - boiling_energy_drain * decay / q
    state[0:3] = jnp.where(live, v_new, v)
    state[3:4] = jnp.where(live, tp_new, tp)
    state[4:5] = jnp.where(live, q_new, q)
    terms[0:3] = jnp.where(live, mass * (v - v_new), 0.0)
    terms[3:4] = jnp.where(live, mass * (tp - tp_new), 0.0)
    terms[4:5] = jnp.where(live, mass - mass_new, 0.0)
    for message in x_out:
        message.start()

    stack = jnp.concatenate(
        [terms[...], jnp.zeros((8 - NUM_TERMS, slots), F32)], axis=0
    )
    for x in range(2):
        for y in range(2):
            row = 2 * (1 - x) + 1 - y
            for z, rim in enumerate((z_high, z_low)):
                part = stack * (corner[row : row + 1] * rim)
                part = jnp.sum(part, axis=1, keepdims=True)
                dxyzs[4 * x + 2 * y + z] = jnp.broadcast_to(part, (8, 128))
    for message in out:
        if 0 not in message.move:
            message.start()

    pieces = [xt[0:ci] * terms[c : c + 1] for c in range(NUM_TERMS)]
    pieces += [stack * xt[ci + 1 - x : ci + 2 - x] for x in range(2)]

    def fan(rims):
        return split(jnp.concatenate([piece * rim for rim in rims for piece in pieces], axis=0))

    def both(high, low, right):
        wide = nt(high, right)
        return wide[:, 0:128] + wide[:, 128:256] + nt(low, right[0:128])

    shape = (2, NUM_TERMS + 2, ci, 128)
    fan_hi[0], fan_lo[0] = fan((z_high, z_low))
    dzs[...] = both(fan_hi[0], fan_lo[0], yt[...]).reshape(shape)
    for z in range(2):
        tile = jnp.zeros((8, 128), F32)
        for c in range(NUM_TERMS):
            keep = (lanes == cj + c) | (lanes == cj + 8 + c)
            tile = jnp.where(keep, dzs[z, c], tile)
        dyzs[z] = tile
    for message in out:
        if message.move[2] != 0 and 0 in message.move:
            message.start()
    fan_hi[1], fan_lo[1] = fan((y_high, y_low))
    dys[...] = both(fan_hi[1], fan_lo[1], lines[...]).reshape(shape)
    for message in out:
        if message.move[2] == 0:
            message.start()

    for a in range(0, NUM_TERMS, 2):
        b = min(a + 2, NUM_TERMS)
        for c in range(a, b):
            high, low = split(line[...] * terms[c : c + 1])
            src_hi[c * ck : (c + 1) * ck] = high
            src_lo[c * ck : (c + 1) * ck] = low
        span = slice(a * ck, b * ck)
        if b - a == 2:
            got = nt(w_hi[...], src_hi[span])
            got += nt(w_hi[...], src_lo[span])
            got += nt(w_lo[...], src_hi[span])
        else:
            got = nt(w_hi[...], jnp.concatenate([src_hi[span], src_lo[span]], axis=0))
            got = got[:, 0:ck] + got[:, ck:] + nt(w_lo[...], src_hi[span])
        for c in range(a, b):
            dep[c] = got[:, (c - a) * ck : (c - a + 1) * ck].reshape(ci, cj, ck)

    for x, deposits in enumerate(x_out):
        plane = 0 if x == 0 else ci - 1

        @pl.when(exists(deposits.move, -1))
        def _():
            deposits.copy.wait_recv()
            high, low = split(
                jnp.concatenate([there[x] * termr[x, c : c + 1] for c in range(NUM_TERMS)], axis=0)
            )
            got = both(high, low, alongs[x])
            for c in range(NUM_TERMS):
                dep[c, plane] += got[c * cj : (c + 1) * cj]

    arrive(out)
    drain(send_sem.at[0], made, 1)
    for message in geo_in + back_in + x_out:
        message.leave()


def finish(
    part, old, dyr, dxyr, dzr, dxzr, dyzr, dxyzr, dep_out, state_out, dep, sem
):
    ci, cj, ck = dep.shape[1:]
    terms = dep.shape[0]
    side = pltpu.make_async_copy(old, state_out, sem.at[terms])
    side.start()
    lanes = lanes_of((8, 128))
    rows = lax.broadcasted_iota(jnp.int32, (8, 128), 0)
    ends = (0, ck - 1)

    def at_ends(first, second, where):
        return jnp.where(where == ends[0], first, jnp.where(where == ends[1], second, 0.0))

    corner = []
    for x in range(2):
        for y in range(2):
            lane = cj + 8 if y == 0 else cj
            first, second = (dxyzr[4 * x + 2 * y + z, :, lane : lane + 1] for z in range(2))
            corner.append(dxyr[2 * x + y] + at_ends(first, second, lanes))
    row = lax.broadcasted_iota(jnp.int32, (32, ci * ck), 0)
    row = jnp.where(row < 16, row, row - 16)
    lane = jnp.where(row < 8, row * ck, (row - 8) * ck + ck - 1)
    spot = jnp.where(lanes_of((32, ci * ck)) == lane, 1.0, 0.0).astype(BF16)
    outs = []
    for c in range(terms):
        block = []
        for z in range(2):
            total = dzr[z, c]
            for x in range(2):
                plane = 0 if x == 0 else ci - 1
                total += jnp.where(rows == plane, dxzr[2 * x + z, c : c + 1], 0.0)
            block.append(total)
        block = jnp.concatenate(block, axis=0)
        high = block.astype(BF16).astype(F32)
        turned = jnp.concatenate([high, block - high], axis=0).T[0:cj].astype(BF16)
        ends_of = nn(turned, spot)
        for i in range(ci):
            dep[c, i] = part[c, i] + ends_of[:, i * ck : (i + 1) * ck]
        for y in range(2):
            row = 0 if y == 0 else cj - 1
            lane = cj + 8 + c if y == 0 else cj + c
            first, second = (dyzr[2 * y + z, :, lane : lane + 1] for z in range(2))
            dep[c, :, row, :] += dyr[y, c] + at_ends(first, second, lanes)
            for x in range(2):
                plane = 0 if x == 0 else ci - 1
                dep[c, plane, row : row + 1, :] += corner[2 * x + y][c : c + 1]
        out = pltpu.make_async_copy(dep.at[c], dep_out.at[c], sem.at[c])
        out.start()
        outs.append(out)
    for out in outs:
        out.wait()
    side.wait()


def local(counts, vel, sca, pos, mot, heat, size, li, lj, lk, tally):
    ci, cj, ck = vel.shape[1:]
    slots = heat.shape[0]
    inner = ci * cj
    vmem = pl.BlockSpec(memory_space=pltpu.VMEM)
    hbm = pl.BlockSpec(memory_space=pltpu.HBM)
    row = lambda value: value.reshape(1, slots)
    pin = lambda value: pltpu.with_memory_space_constraint(value, pltpu.HBM)
    tile = (8, 128)
    f32 = lambda *shape: pltpu.VMEM(shape, F32)
    i32 = lambda *shape: pltpu.VMEM(shape, jnp.int32)
    b16 = lambda *shape: pltpu.VMEM(shape, BF16)
    struct = lambda *shape: jax.ShapeDtypeStruct(shape, F32)
    scratch = [
        f32(NUM_FIELDS, ci, cj, ck),
        f32(3, slots),
        f32(3, slots),
        f32(1, slots),
        f32(1, slots),
        i32(1, slots),
        i32(1, slots),
        i32(1, slots),
        b16(NUM_FIELDS * ck, inner),
        b16(NUM_FIELDS * ck, inner),
        b16(inner, slots),
        b16(inner, slots),
        f32(4, slots),
        f32(2 * ci, slots),
        b16(256, slots),
        f32(ck, slots),
        b16(2 * ck, slots),
        b16(NUM_TERMS * ck, slots),
        b16(NUM_TERMS * ck, slots),
        f32(8, slots),
        f32(4, slots),
        f32(2, NUM_FIELDS, slots),
        f32(NUM_TERMS, slots),
        f32(2, cj, slots),
        f32(ck, slots),
        b16(2, 2 * ck, slots),
        b16(3 * cj, slots),
        b16(2, NUM_FIELDS * ck, 3 * cj),
        f32(2, NUM_FIELDS, ci, ck),
        f32(4, *tile),
        f32(2, 8, inner),
        f32(4, *tile),
        f32(4, *tile),
        f32(8, *tile),
        f32(2, 4, slots),
        f32(2, NUM_FIELDS, slots),
        f32(2, NUM_TERMS, slots),
        f32(2, NUM_FIELDS, ci, ck),
        f32(4, *tile),
        f32(2, 8, inner),
        f32(2, *tile),
        f32(2, NUM_TERMS + 2, ci, ck),
        f32(2, NUM_TERMS + 2, ci, ck),
        f32(2, *tile),
        f32(8, *tile),
        b16(inner, 128),
        b16(2, 2 * (NUM_TERMS + 2) * ci, slots),
        b16(2, 2 * (NUM_TERMS + 2) * ci, slots),
        f32(256, *tile),
        pltpu.SemaphoreType.DMA((5,)),
        pltpu.SemaphoreType.DMA((7,)),
        pltpu.SemaphoreType.DMA((10,)),
        pltpu.SemaphoreType.REGULAR,
    ]
    results = (
        struct(NUM_TERMS, ci, cj, ck),
        struct(NUM_TERMS, slots),
        struct(2, NUM_TERMS, ci, ck),
        struct(4, *tile),
        struct(2, NUM_TERMS, ci, ck),
        struct(4, *tile),
        struct(4, *tile),
        struct(8, *tile),
    )
    arrays = (vel, sca, pos, mot, row(heat), row(size), row(li), row(lj), row(lk))
    parts = pl.pallas_call(
        functools.partial(kernel, counts),
        out_shape=results,
        in_specs=[hbm] * len(arrays) + [pl.BlockSpec(memory_space=pltpu.SMEM)],
        out_specs=(vmem,) * len(results),
        scratch_shapes=scratch,
        compiler_params=pltpu.CompilerParams(
            collective_id=0, has_side_effects=True, vmem_limit_bytes=32 * 2**20
        ),
    )(*[pin(value) for value in arrays], tally)
    return pl.pallas_call(
        finish,
        out_shape=results[0:2],
        in_specs=[vmem] * len(results),
        out_specs=(pl.BlockSpec(memory_space=pl.ANY),) * 2,
        scratch_shapes=[
            f32(NUM_TERMS, ci, cj, ck),
            pltpu.SemaphoreType.DMA((NUM_TERMS + 1,)),
        ],
        compiler_params=pltpu.CompilerParams(vmem_limit_bytes=12 * 2**20),
    )(*parts)


def solution(mesh):
    bricks = P(None, AXES[0], AXES[1], AXES[2])
    rows = P(None, AXES)
    flat = P(AXES)
    counts = tuple(mesh.shape[axis] for axis in AXES)
    return jax.shard_map(
        functools.partial(local, counts),
        mesh=mesh,
        in_specs=(bricks, bricks, rows, rows) + (flat,) * 6,
        out_specs=(bricks, rows),
        check_vma=False,
    )
```

```python
import functools
import itertools

import jax
import jax.numpy as jnp
from jax import lax
from jax.experimental import pallas as pl
from jax.experimental.pallas import tpu as pltpu
from jax.sharding import PartitionSpec as P

TILE = 128
AXES = ("gx", "gy", "gz")
MESH = pl.DeviceIdType.MESH
F32 = jnp.float32
BF16 = jnp.bfloat16

step_time = 0.25
evap_rate = 1.0
heat_rate = 2.0
boiling_energy_drain = 0.3

STEPS = ((1, 0), (-1, 1))
NUM_TERMS = 5
NUM_FIELDS = 6


def split(value):
    high = value.astype(BF16)
    return high, (value - high.astype(F32)).astype(BF16)


def nn(a, b):
    return lax.dot_general(a, b, (((1,), (0,)), ((), ())), preferred_element_type=F32)


def nt(a, b):
    return lax.dot_general(a, b, (((1,), (1,)), ((), ())), preferred_element_type=F32)


def pair_weights(offset):
    lower = jnp.where(offset < 0.0, -1.0, 0.0)
    first = jnp.maximum(0.0, 1.0 - jnp.abs(offset - lower))
    second = jnp.maximum(0.0, 1.0 - jnp.abs(offset - (lower + 1.0)))
    return first, second, lower


def lanes_of(shape):
    return lax.broadcasted_iota(jnp.int32, shape, len(shape) - 1)


def tent(count, place):
    rows = lax.broadcasted_iota(jnp.int32, (count, place.shape[1]), 0).astype(F32)
    return jnp.maximum(0.0, 1.0 - jnp.abs(rows - place))


def spots(first, count, base, wa, wb):
    rows = (lax.broadcasted_iota(jnp.int32, (count, base.shape[1]), 0) + first).astype(F32)
    return jnp.where(rows == base, wa, jnp.where(rows == base + 1.0, wb, 0.0))


def kernel(
    counts,
    vel,
    sca,
    pos_in,
    mot_in,
    heat_in,
    size_in,
    li_in,
    lj_in,
    lk_in,
    tally,
    dep,
    state,
    dyr,
    dxyr,
    dzr,
    dxzr,
    dyzr,
    dxyzr,
    fields,
    pos,
    mot,
    heat,
    size,
    li,
    lj,
    lk,
    ft_hi,
    ft_lo,
    w_hi,
    w_lo,
    corner,
    xt,
    yt,
    line,
    lines,
    src_hi,
    src_lo,
    sampled,
    geo,
    back,
    terms,
    there,
    along,
    alongs,
    w_there,
    face_f,
    yh,
    xyh,
    zh,
    xzh,
    yzh,
    xyzh,
    geor,
    backr,
    termr,
    ys,
    xys,
    zs,
    ez,
    dys,
    dzs,
    dyzs,
    dxyzs,
    edges,
    fan_hi,
    fan_lo,
    gauge,
    load_sem,
    send_sem,
    recv_sem,
    far,
):
    ci, cj, ck = vel.shape[1:]
    slots = heat.shape[1]
    inner = ci * cj
    me = [lax.axis_index(axis) for axis in AXES]

    def exists(move, sign):
        good = None
        for d in range(3):
            step = sign * move[d]
            if step == 1:
                test = me[d] < counts[d] - 1
            elif step == -1:
                test = me[d] > 0
            else:
                continue
            good = test if good is None else jnp.logical_and(good, test)
        return good

    def peer(move):
        return tuple(lax.rem(me[d] + move[d] + counts[d], counts[d]) for d in range(3))

    class Message:
        def __init__(self, number, move, src, dst, tiles, post):
            self.move = move
            self.dst = dst
            self.tiles = tiles
            self.number = number
            self.copy = pltpu.make_async_remote_copy(
                src_ref=src,
                dst_ref=dst,
                send_sem=send_sem.at[post],
                recv_sem=recv_sem.at[number],
                device_id=peer(move),
                device_id_type=MESH,
            )

        def start(self):
            @pl.when(exists(self.move, 1))
            def _():
                self.copy.start()

        def blank(self):
            @pl.when(jnp.logical_not(exists(self.move, -1)))
            def _():
                self.dst[...] = jnp.zeros(self.dst.shape, F32)

        def leave(self):
            @pl.when(exists(self.move, 1))
            def _():
                self.copy.wait_send()

    def totals(messages, sign):
        sides = []
        for extent in counts:
            low, high = (-1,), (1,)
            sides.append([()] if extent == 1 else [low, high] + [low + high] * (extent > 2))
        found = set()
        for place in itertools.product(*sides):
            there = [
                message.tiles
                for message in messages
                if all(
                    step == 0 or sign * step in side for step, side in zip(message.move, place)
                )
            ]
            found.add(sum(there))
        return sorted(found - {0})

    def drain(sem, messages, sign):
        count = sum(
            jnp.where(exists(message.move, sign), message.tiles, 0) for message in messages
        )
        for total in totals(messages, sign):

            @pl.when(count == total)
            def _():
                some = gauge.at[0:total]
                pltpu.make_async_copy(some, some, sem).wait()

    def arrive(messages):
        drain(recv_sem.at[messages[0].number], messages, -1)

    made = []

    def add(group, number, move, src, dst, tiles=1, post=0):
        message = Message(number, move, src, dst, tiles, post)
        made.append(message)
        group.append(message)

    Y_IN, Z_IN, RIM, OUT, GEO, TERMS, BACK = 0, 1, 2, 3, 4, 6, 8
    face = lambda n, extent: extent - 1 if n == 0 else 0
    edge_tile = lambda n: pl.ds(face(n, ci) * cj // 128 * 128, 128)
    y_in, xy_in, z_in, yz_in, geo_in, x_out, out = [], [], [], [], [], [], []
    rim_in, corner_in, back_in = [], [], []
    for mx, x in STEPS:
        for my, y in STEPS:
            add(xy_in, Y_IN, (mx, my, 0), xys.at[2 * x + y], xyh.at[2 * x + y])
            add(out, OUT, (mx, my, 0), dys.at[y, NUM_TERMS + x], dxyr.at[2 * x + y])
            for mz, z in STEPS:
                n = 4 * x + 2 * y + z
                add(corner_in, RIM, (mx, my, mz), ez.at[z], xyzh.at[n])
                add(out, OUT, (mx, my, mz), dxyzs.at[n], dxyzr.at[n])
        add(geo_in, GEO + x, (mx, 0, 0), geo, geor.at[x], 0, 1 + x)
        add(back_in, BACK + x, (mx, 0, 0), back.at[1 - x], backr.at[x], 0, 3 + x)
        add(x_out, TERMS + x, (mx, 0, 0), terms, termr.at[x], 0, 5 + x)
        for mz, z in STEPS:
            n = 2 * x + z
            add(rim_in, RIM, (mx, 0, mz), zs.at[z, :, edge_tile(x)], xzh.at[n])
            add(out, OUT, (mx, 0, mz), dzs.at[z, NUM_TERMS + x], dxzr.at[n])
    for my, y in STEPS:
        add(y_in, Y_IN, (0, my, 0), ys.at[y], yh.at[y], NUM_FIELDS)
        add(out, OUT, (0, my, 0), dys.at[y, 0:NUM_TERMS], dyr.at[y], NUM_TERMS)
        for mz, z in STEPS:
            add(yz_in, Z_IN, (0, my, mz), ez.at[z], yzh.at[2 * y + z])
            add(out, OUT, (0, my, mz), dyzs.at[z], dyzr.at[2 * y + z])
    for mz, z in STEPS:
        add(z_in, Z_IN, (0, 0, mz), zs.at[z], zh.at[z], inner // 128)
        add(out, OUT, (0, 0, mz), dzs.at[z, 0:NUM_TERMS], dzr.at[z], NUM_TERMS)

    def signal(sem, move):
        @pl.when(exists(move, 1))
        def _():
            pl.semaphore_signal(sem, inc=1, device_id=peer(move), device_id_type=MESH)

    def heard(sem, moves):
        pl.semaphore_wait(sem, sum(exists(move, -1).astype(jnp.int32) for move in moves))


    def turned_rows(flats, total):
        parts = []
        for flat in flats:
            high = flat.astype(BF16).astype(F32)
            parts += [high, flat - high, high]
        spare = total - sum(part.shape[0] for part in parts)
        if spare > 0:
            parts.append(jnp.zeros((spare, ck), F32))
        return jnp.concatenate(parts, axis=0).T.astype(BF16)

    x_moves = [(step, 0, 0) for step, _ in STEPS]
    y_moves = [(0, step, 0) for step, _ in STEPS]
    z_moves = [(0, 0, step) for step, _ in STEPS]
    xy_moves = [(mx, my, 0) for mx, _ in STEPS for my, _ in STEPS]
    met = xy_moves + z_moves + x_moves + y_moves
    barrier = pltpu.get_barrier_semaphore()
    for move in met:
        signal(barrier, move)

    def load(src, dst, number):
        pltpu.make_async_copy(src, dst, load_sem.at[number]).start()

    def loaded(whole, number):
        pltpu.make_async_copy(whole, whole, load_sem.at[number]).wait()

    pairs = [(pos_in, pos), (li_in, li), (lj_in, lj), (lk_in, lk)]
    pairs += [(mot_in, mot), (heat_in, heat), (size_in, size)]
    for (src, dst), number in zip(pairs, (1, 2, 2, 2, 3, 4, 4)):
        load(src, dst, number)
    load(vel, fields.at[0:3], 0)
    load(sca, fields.at[3:6], 0)

    xys[...] = jnp.zeros_like(xys)
    zs[...] = jnp.zeros_like(zs)
    for message in y_in + xy_in + z_in + yz_in + rim_in + corner_in + out:
        message.blank()
    rows = lax.broadcasted_iota(jnp.int32, (inner, 128), 0)
    cols = lanes_of((inner, 128))
    target = jnp.where(cols < cj + 8, (cols - cj) * cj + cj - 1, (cols - cj - 8) * cj)
    chosen = (rows == target) & (cols >= cj) & (cols < cj + 16)
    edges[...] = jnp.where(chosen, 1.0, 0.0).astype(BF16)

    loaded(pos, 1)
    loaded(gauge.at[0 : 3 * slots // 1024], 2)
    xa, xb, lx = pair_weights(pos[0:1])
    ya, yb, ly = pair_weights(pos[1:2])
    za, zb, lz = pair_weights(pos[2:3])
    i0 = li[...].astype(F32) + lx
    j0 = lj[...].astype(F32) + ly
    k0 = lk[...].astype(F32) + lz

    def at(index, base, wa, wb):
        return jnp.where(base == index, wa, jnp.where(base + 1.0 == index, wb, 0.0))

    x_low, x_high = at(-1.0, i0, xa, xb), at(float(ci), i0, xa, xb)
    y_low, y_high = at(-1.0, j0, ya, yb), at(float(cj), j0, ya, yb)
    z_low, z_high = at(-1.0, k0, za, zb), at(float(ck), k0, za, zb)
    y_place = lj[...].astype(F32) + pos[1:2]
    z_place = lk[...].astype(F32) + pos[2:3]
    for n, row in enumerate((x_high, x_low, y_place, z_place)):
        geo[n : n + 1] = row
    xt[0:ci] = spots(0, ci, i0, xa, xb)
    xt[ci : 2 * ci] = jnp.concatenate([x_low, x_high, jnp.zeros((ci - 2, slots), F32)], axis=0)
    across = spots(0, cj, j0, ya, yb)
    rims = [
        jnp.broadcast_to(y_low, (8, slots)),
        jnp.broadcast_to(y_high, (8, slots)),
        jnp.zeros((128 - cj - 16, slots), F32),
    ]
    high, low = split(jnp.concatenate([across] + rims, axis=0))
    yt[0:128] = high
    yt[128:256] = low
    corners = [a * b for a in (x_low, x_high) for b in (y_low, y_high)]
    for n, row in enumerate(corners):
        corner[n : n + 1] = row
    line[...] = spots(0, ck, k0, za, zb)
    high, low = split(line[...])
    lines[0:ck] = high
    lines[ck : 2 * ck] = low

    for i in range(ci):
        high, low = split(xt[i : i + 1] * across)
        w_hi[i * cj : (i + 1) * cj] = high
        w_lo[i * cj : (i + 1) * cj] = low
    heard(barrier, met)
    for move in z_moves:
        signal(far, move)
    for message in geo_in:
        message.start()
    loaded(fields, 0)
    for y in range(2):
        row = face(y, cj)
        ys[y] = fields[:, :, row, :]
        for x in range(2):
            xys[2 * x + y, 0:NUM_FIELDS] = fields[:, face(x, ci), row, :]
    for message in xy_in + y_in:
        message.start()
    for f in range(NUM_FIELDS):
        turned = fields[f].reshape(inner, ck).T
        high, low = split(turned)
        ft_hi[f * ck : (f + 1) * ck] = high
        ft_lo[f * ck : (f + 1) * ck] = low
        zs[0, f : f + 1] = turned[ck - 1 : ck]
        zs[1, f : f + 1] = turned[0:1]
    for message in z_in:
        message.start()
    high, low = split(zs[...].reshape(16, inner))
    ez[...] = (nn(high, edges[...]) + nn(low, edges[...])).reshape(2, 8, 128)
    for x in range(2):
        plane = 0 if x == 0 else ci - 1

        @pl.when(exists(x_moves[x], -1))
        def _():
            for f in range(NUM_FIELDS):
                face_f[x, f * ck : (f + 1) * ck] = turned_rows([fields[f, plane]], 0)

    width = 256

    def collect(got, table, here, target, start=0):
        parts = [
            jnp.sum(got[n * ck : (n + 1) * ck] * table[:, here], axis=0, keepdims=True)
            for n in range(got.shape[0] // ck)
        ]
        for n, part in enumerate(parts):
            target(start + n, here, part)

    def put(f, here, value):
        sampled[f : f + 1, here] = value

    def sample(blocks):
        for s in blocks:
            here = slice(s * width, (s + 1) * width)
            for start in range(0, NUM_FIELDS, NUM_FIELDS // 2):
                part = slice(start * ck, (start + NUM_FIELDS // 2) * ck)
                got = nn(ft_hi[part], w_hi[:, here])
                got += nn(ft_hi[part], w_lo[:, here])
                got += nn(ft_lo[part], w_hi[:, here])
                collect(got, line, here, put, start)

    def ghosts():
        for x, places in enumerate(geo_in):

            @pl.when(exists(places.move, -1))
            def _():
                places.copy.wait_recv()
                there[x] = tent(cj, geor[x, 2:3]) * geor[x, x : x + 1]
                along[...] = tent(ck, geor[x, 3:4])
                high, low = split(along[...])
                alongs[x, 0:ck] = high
                alongs[x, ck : 2 * ck] = low
                high, low = split(there[x])
                w_there[0:cj] = high
                w_there[cj : 2 * cj] = high
                w_there[2 * cj : 3 * cj] = low

                def keep(f, here, value):
                    back[x, f : f + 1, here] = value

                for s in range(0, slots, width):
                    here = slice(s, s + width)
                    collect(nn(face_f[x], w_there[:, here]), along, here, keep)
                back_in[1 - x].copy.start()

    sample(range(1))
    heard(far, z_moves)
    for message in corner_in + rim_in + yz_in:
        message.start()

    early = lax.rem(me[0], 2) == 1
    blocks = slots // width

    @pl.when(early)
    def _():
        ghosts()
        sample(range(1, blocks))

    @pl.when(jnp.logical_not(early))
    def _():
        sample(range(1, blocks // 2))
        ghosts()
        sample(range(blocks // 2, blocks))

    arrive(y_in + xy_in)
    flat = NUM_FIELDS * ci
    ends = jnp.concatenate(
        [yh[y].reshape(flat, ck) for y in range(2)] + [xyh[q] for q in range(4)], axis=0
    )
    count = ends.shape[0]
    high, low = split(ends)
    got = nn(jnp.concatenate([high, low], axis=0), lines[0:ck])
    got = got[0:count] + got[count:] + nn(high, lines[ck : 2 * ck])
    rest = None
    for q in range(4):
        first = 2 * flat + q * 8
        part = got[first : first + 8] * corner[q : q + 1]
        rest = part if rest is None else rest + part
    for f in range(NUM_FIELDS):
        total = sampled[f : f + 1] + rest[f : f + 1]
        for y, rim in enumerate((y_low, y_high)):
            first = y * flat + f * ci
            part = got[first : first + ci] * xt[0:ci]
            total += jnp.sum(part, axis=0, keepdims=True) * rim
        sampled[f : f + 1] = total

    arrive(z_in + yz_in)
    lanes = lanes_of((8, 128))
    body = lanes < cj

    def half(tile, odd):
        return jnp.where(body, pltpu.roll(tile, 128 - cj, 1) if odd else tile, 0.0)

    def pick(tile, lane):
        return jnp.where(lanes == lane, tile, 0.0)

    def beyond(blocks, planes):
        count = 2 * planes.shape[0] * 8
        high, low = split(jnp.concatenate(blocks, axis=0))
        got = nn(jnp.concatenate([high, low], axis=0), yt[0:128])
        got = got[0:count] + got[count:] + nn(high, yt[128:256])
        for z, rim in enumerate((z_low, z_high)):
            total = None
            for b in range(planes.shape[0]):
                first = (z * planes.shape[0] + b) * 8
                part = got[first : first + 8] * planes[b : b + 1]
                total = part if total is None else total + part
            sampled[...] += total * rim

    blocks = []
    for z in range(2):
        for i in range(ci):
            first = i * cj // 128 * 128
            block = half(zh[z, :, first : first + 128], i * cj % 128 != 0)
            blocks.append(block + pick(yzh[z], cj + i) + pick(yzh[2 + z], cj + 8 + i))
    beyond(blocks, xt[0:ci])
    loaded(mot, 3)
    loaded(gauge.at[0 : 2 * slots // 1024], 4)
    for x, message in enumerate(back_in):

        @pl.when(exists(message.move, -1))
        def _():
            message.copy.wait_recv()
            sampled[0:NUM_FIELDS] += backr[x]

    arrive(rim_in + corner_in)
    blocks = []
    for z in range(2):
        for x in range(2):
            i = face(x, ci)
            block = half(xzh[2 * x + z], i * cj % 128 != 0)
            block += pick(xyzh[4 * x + z], cj + i) + pick(xyzh[4 * x + 2 + z], cj + 8 + i)
            blocks.append(block)
    beyond(blocks, xt[ci : ci + 2])

    gas = sampled[...]
    live = lanes_of((1, slots)) // TILE < tally[0]
    q = size[...]
    tp = heat[...]
    v = mot[...]
    drag = step_time / (0.5 * q)
    v_new = (v + drag * gas[0:3]) / (1.0 + drag)
    mass = q * jnp.sqrt(q)
    share = jnp.exp(4.0 * (tp - 1.0))
    decay = step_time * evap_rate * gas[5:6] * (share - gas[4:5])
    q_new = q - decay
    mass_new = q_new * jnp.sqrt(q_new)
    conduct = step_time * heat_rate * gas[5:6] / q
    tp_new = (tp + conduct * gas[3:4]) / (1.0 + conduct) - boiling_energy_drain * decay / q
    state[0:3] = jnp.where(live, v_new, v)
    state[3:4] = jnp.where(live, tp_new, tp)
    state[4:5] = jnp.where(live, q_new, q)
    terms[0:3] = jnp.where(live, mass * (v - v_new), 0.0)
    terms[3:4] = jnp.where(live, mass * (tp - tp_new), 0.0)
    terms[4:5] = jnp.where(live, mass - mass_new, 0.0)
    for message in x_out:
        message.start()

    stack = jnp.concatenate(
        [terms[...], jnp.zeros((8 - NUM_TERMS, slots), F32)], axis=0
    )
    for x in range(2):
        for y in range(2):
            row = 2 * (1 - x) + 1 - y
            for z, rim in enumerate((z_high, z_low)):
                part = stack * (corner[row : row + 1] * rim)
                part = jnp.sum(part, axis=1, keepdims=True)
                dxyzs[4 * x + 2 * y + z] = jnp.broadcast_to(part, (8, 128))
    for message in out:
        if 0 not in message.move:
            message.start()

    pieces = [xt[0:ci] * terms[c : c + 1] for c in range(NUM_TERMS)]
    pieces += [stack * xt[ci + 1 - x : ci + 2 - x] for x in range(2)]

    def fan(rims):
        return split(jnp.concatenate([piece * rim for rim in rims for piece in pieces], axis=0))

    def both(high, low, right):
        wide = nt(high, right)
        return wide[:, 0:128] + wide[:, 128:256] + nt(low, right[0:128])

    shape = (2, NUM_TERMS + 2, ci, 128)
    fan_hi[0], fan_lo[0] = fan((z_high, z_low))
    dzs[...] = both(fan_hi[0], fan_lo[0], yt[...]).reshape(shape)
    for z in range(2):
        tile = jnp.zeros((8, 128), F32)
        for c in range(NUM_TERMS):
            keep = (lanes == cj + c) | (lanes == cj + 8 + c)
            tile = jnp.where(keep, dzs[z, c], tile)
        dyzs[z] = tile
    for message in out:
        if message.move[2] != 0 and 0 in message.move:
            message.start()
    fan_hi[1], fan_lo[1] = fan((y_high, y_low))
    dys[...] = both(fan_hi[1], fan_lo[1], lines[...]).reshape(shape)
    for message in out:
        if message.move[2] == 0:
            message.start()

    for a in range(0, NUM_TERMS, 2):
        b = min(a + 2, NUM_TERMS)
        for c in range(a, b):
            high, low = split(line[...] * terms[c : c + 1])
            src_hi[c * ck : (c + 1) * ck] = high
            src_lo[c * ck : (c + 1) * ck] = low
        span = slice(a * ck, b * ck)
        if b - a == 2:
            got = nt(w_hi[...], src_hi[span])
            got += nt(w_hi[...], src_lo[span])
            got += nt(w_lo[...], src_hi[span])
        else:
            got = nt(w_hi[...], jnp.concatenate([src_hi[span], src_lo[span]], axis=0))
            got = got[:, 0:ck] + got[:, ck:] + nt(w_lo[...], src_hi[span])
        for c in range(a, b):
            dep[c] = got[:, (c - a) * ck : (c - a + 1) * ck].reshape(ci, cj, ck)

    for x, deposits in enumerate(x_out):
        plane = 0 if x == 0 else ci - 1

        @pl.when(exists(deposits.move, -1))
        def _():
            deposits.copy.wait_recv()
            high, low = split(
                jnp.concatenate([there[x] * termr[x, c : c + 1] for c in range(NUM_TERMS)], axis=0)
            )
            got = both(high, low, alongs[x])
            for c in range(NUM_TERMS):
                dep[c, plane] += got[c * cj : (c + 1) * cj]

    arrive(out)
    drain(send_sem.at[0], made, 1)
    for message in geo_in + back_in + x_out:
        message.leave()


def finish(
    part, old, dyr, dxyr, dzr, dxzr, dyzr, dxyzr, dep_out, state_out, dep, sem
):
    ci, cj, ck = dep.shape[1:]
    terms = dep.shape[0]
    side = pltpu.make_async_copy(old, state_out, sem.at[terms])
    side.start()
    lanes = lanes_of((8, 128))
    rows = lax.broadcasted_iota(jnp.int32, (8, 128), 0)
    ends = (0, ck - 1)

    def at_ends(first, second, where):
        return jnp.where(where == ends[0], first, jnp.where(where == ends[1], second, 0.0))

    corner = []
    for x in range(2):
        for y in range(2):
            lane = cj + 8 if y == 0 else cj
            first, second = (dxyzr[4 * x + 2 * y + z, :, lane : lane + 1] for z in range(2))
            corner.append(dxyr[2 * x + y] + at_ends(first, second, lanes))
    row = lax.broadcasted_iota(jnp.int32, (32, ci * ck), 0)
    row = jnp.where(row < 16, row, row - 16)
    lane = jnp.where(row < 8, row * ck, (row - 8) * ck + ck - 1)
    spot = jnp.where(lanes_of((32, ci * ck)) == lane, 1.0, 0.0).astype(BF16)
    outs = []
    for c in range(terms):
        block = []
        for z in range(2):
            total = dzr[z, c]
            for x in range(2):
                plane = 0 if x == 0 else ci - 1
                total += jnp.where(rows == plane, dxzr[2 * x + z, c : c + 1], 0.0)
            block.append(total)
        block = jnp.concatenate(block, axis=0)
        high = block.astype(BF16).astype(F32)
        turned = jnp.concatenate([high, block - high], axis=0).T[0:cj].astype(BF16)
        ends_of = nn(turned, spot)
        for i in range(ci):
            dep[c, i] = part[c, i] + ends_of[:, i * ck : (i + 1) * ck]
        for y in range(2):
            row = 0 if y == 0 else cj - 1
            lane = cj + 8 + c if y == 0 else cj + c
            first, second = (dyzr[2 * y + z, :, lane : lane + 1] for z in range(2))
            dep[c, :, row, :] += dyr[y, c] + at_ends(first, second, lanes)
            for x in range(2):
                plane = 0 if x == 0 else ci - 1
                dep[c, plane, row : row + 1, :] += corner[2 * x + y][c : c + 1]
        out = pltpu.make_async_copy(dep.at[c], dep_out.at[c], sem.at[c])
        out.start()
        outs.append(out)
    for out in outs:
        out.wait()
    side.wait()


def local(counts, vel, sca, pos, mot, heat, size, li, lj, lk, tally):
    ci, cj, ck = vel.shape[1:]
    slots = heat.shape[0]
    inner = ci * cj
    vmem = pl.BlockSpec(memory_space=pltpu.VMEM)
    hbm = pl.BlockSpec(memory_space=pltpu.HBM)
    row = lambda value: value.reshape(1, slots)
    pin = lambda value: pltpu.with_memory_space_constraint(value, pltpu.HBM)
    tile = (8, 128)
    f32 = lambda *shape: pltpu.VMEM(shape, F32)
    i32 = lambda *shape: pltpu.VMEM(shape, jnp.int32)
    b16 = lambda *shape: pltpu.VMEM(shape, BF16)
    struct = lambda *shape: jax.ShapeDtypeStruct(shape, F32)
    scratch = [
        f32(NUM_FIELDS, ci, cj, ck),
        f32(3, slots),
        f32(3, slots),
        f32(1, slots),
        f32(1, slots),
        i32(1, slots),
        i32(1, slots),
        i32(1, slots),
        b16(NUM_FIELDS * ck, inner),
        b16(NUM_FIELDS * ck, inner),
        b16(inner, slots),
        b16(inner, slots),
        f32(4, slots),
        f32(2 * ci, slots),
        b16(256, slots),
        f32(ck, slots),
        b16(2 * ck, slots),
        b16(NUM_TERMS * ck, slots),
        b16(NUM_TERMS * ck, slots),
        f32(8, slots),
        f32(4, slots),
        f32(2, NUM_FIELDS, slots),
        f32(NUM_TERMS, slots),
        f32(2, cj, slots),
        f32(ck, slots),
        b16(2, 2 * ck, slots),
        b16(3 * cj, slots),
        b16(2, NUM_FIELDS * ck, 3 * cj),
        f32(2, NUM_FIELDS, ci, ck),
        f32(4, *tile),
        f32(2, 8, inner),
        f32(4, *tile),
        f32(4, *tile),
        f32(8, *tile),
        f32(2, 4, slots),
        f32(2, NUM_FIELDS, slots),
        f32(2, NUM_TERMS, slots),
        f32(2, NUM_FIELDS, ci, ck),
        f32(4, *tile),
        f32(2, 8, inner),
        f32(2, *tile),
        f32(2, NUM_TERMS + 2, ci, ck),
        f32(2, NUM_TERMS + 2, ci, ck),
        f32(2, *tile),
        f32(8, *tile),
        b16(inner, 128),
        b16(2, 2 * (NUM_TERMS + 2) * ci, slots),
        b16(2, 2 * (NUM_TERMS + 2) * ci, slots),
        f32(256, *tile),
        pltpu.SemaphoreType.DMA((5,)),
        pltpu.SemaphoreType.DMA((7,)),
        pltpu.SemaphoreType.DMA((10,)),
        pltpu.SemaphoreType.REGULAR,
    ]
    results = (
        struct(NUM_TERMS, ci, cj, ck),
        struct(NUM_TERMS, slots),
        struct(2, NUM_TERMS, ci, ck),
        struct(4, *tile),
        struct(2, NUM_TERMS, ci, ck),
        struct(4, *tile),
        struct(4, *tile),
        struct(8, *tile),
    )
    arrays = (vel, sca, pos, mot, row(heat), row(size), row(li), row(lj), row(lk))
    parts = pl.pallas_call(
        functools.partial(kernel, counts),
        out_shape=results,
        in_specs=[hbm] * len(arrays) + [pl.BlockSpec(memory_space=pltpu.SMEM)],
        out_specs=(vmem,) * len(results),
        scratch_shapes=scratch,
        compiler_params=pltpu.CompilerParams(
            collective_id=0, has_side_effects=True, vmem_limit_bytes=32 * 2**20
        ),
    )(*[pin(value) for value in arrays], tally)
    return pl.pallas_call(
        finish,
        out_shape=results[0:2],
        in_specs=[vmem] * len(results),
        out_specs=(pl.BlockSpec(memory_space=pl.ANY),) * 2,
        scratch_shapes=[
            f32(NUM_TERMS, ci, cj, ck),
            pltpu.SemaphoreType.DMA((NUM_TERMS + 1,)),
        ],
        compiler_params=pltpu.CompilerParams(vmem_limit_bytes=12 * 2**20),
    )(*parts)


def solution(mesh):
    bricks = P(None, AXES[0], AXES[1], AXES[2])
    rows = P(None, AXES)
    flat = P(AXES)
    counts = tuple(mesh.shape[axis] for axis in AXES)
    return jax.shard_map(
        functools.partial(local, counts),
        mesh=mesh,
        in_specs=(bricks, bricks, rows, rows) + (flat,) * 6,
        out_specs=(bricks, rows),
        check_vma=False,
    )
```

```python
import functools
import itertools

import jax
import jax.numpy as jnp
from jax import lax
from jax.experimental import pallas as pl
from jax.experimental.pallas import tpu as pltpu
from jax.sharding import PartitionSpec as P

TILE = 128
AXES = ("gx", "gy", "gz")
MESH = pl.DeviceIdType.MESH
F32 = jnp.float32
BF16 = jnp.bfloat16

step_time = 0.25
evap_rate = 1.0
heat_rate = 2.0
boiling_energy_drain = 0.3

STEPS = ((1, 0), (-1, 1))
NUM_TERMS = 5
NUM_FIELDS = 6


def split(value):
    high = value.astype(BF16)
    return high, (value - high.astype(F32)).astype(BF16)


def nn(a, b):
    return lax.dot_general(a, b, (((1,), (0,)), ((), ())), preferred_element_type=F32)


def nt(a, b):
    return lax.dot_general(a, b, (((1,), (1,)), ((), ())), preferred_element_type=F32)


def pair_weights(offset):
    lower = jnp.where(offset < 0.0, -1.0, 0.0)
    first = jnp.maximum(0.0, 1.0 - jnp.abs(offset - lower))
    second = jnp.maximum(0.0, 1.0 - jnp.abs(offset - (lower + 1.0)))
    return first, second, lower


def lanes_of(shape):
    return lax.broadcasted_iota(jnp.int32, shape, len(shape) - 1)


def tent(count, place):
    rows = lax.broadcasted_iota(jnp.int32, (count, place.shape[1]), 0).astype(F32)
    return jnp.maximum(0.0, 1.0 - jnp.abs(rows - place))


def spots(first, count, base, wa, wb):
    rows = (lax.broadcasted_iota(jnp.int32, (count, base.shape[1]), 0) + first).astype(F32)
    return jnp.where(rows == base, wa, jnp.where(rows == base + 1.0, wb, 0.0))


def kernel(
    counts,
    vel,
    sca,
    pos_in,
    mot_in,
    heat_in,
    size_in,
    li_in,
    lj_in,
    lk_in,
    tally,
    dep,
    state,
    dyr,
    dxyr,
    dzr,
    dxzr,
    dyzr,
    dxyzr,
    fields,
    pos,
    mot,
    heat,
    size,
    li,
    lj,
    lk,
    ft_hi,
    ft_lo,
    w_hi,
    w_lo,
    corner,
    xt,
    yt,
    line,
    lines,
    src_hi,
    src_lo,
    sampled,
    geo,
    back,
    terms,
    there,
    along,
    alongs,
    w_there,
    face_f,
    yh,
    xyh,
    zh,
    xzh,
    yzh,
    xyzh,
    geor,
    backr,
    termr,
    ys,
    xys,
    zs,
    ez,
    dys,
    dzs,
    dyzs,
    dxyzs,
    edges,
    fan_hi,
    fan_lo,
    gauge,
    load_sem,
    send_sem,
    recv_sem,
    far,
):
    ci, cj, ck = vel.shape[1:]
    slots = heat.shape[1]
    inner = ci * cj
    me = [lax.axis_index(axis) for axis in AXES]

    def exists(move, sign):
        good = None
        for d in range(3):
            step = sign * move[d]
            if step == 1:
                test = me[d] < counts[d] - 1
            elif step == -1:
                test = me[d] > 0
            else:
                continue
            good = test if good is None else jnp.logical_and(good, test)
        return good

    def peer(move):
        return tuple(lax.rem(me[d] + move[d] + counts[d], counts[d]) for d in range(3))

    class Message:
        def __init__(self, number, move, src, dst, tiles, post):
            self.move = move
            self.dst = dst
            self.tiles = tiles
            self.number = number
            self.copy = pltpu.make_async_remote_copy(
                src_ref=src,
                dst_ref=dst,
                send_sem=send_sem.at[post],
                recv_sem=recv_sem.at[number],
                device_id=peer(move),
                device_id_type=MESH,
            )

        def start(self):
            @pl.when(exists(self.move, 1))
            def _():
                self.copy.start()

        def blank(self):
            @pl.when(jnp.logical_not(exists(self.move, -1)))
            def _():
                self.dst[...] = jnp.zeros(self.dst.shape, F32)

        def leave(self):
            @pl.when(exists(self.move, 1))
            def _():
                self.copy.wait_send()

    def totals(messages, sign):
        sides = []
        for extent in counts:
            low, high = (-1,), (1,)
            sides.append([()] if extent == 1 else [low, high] + [low + high] * (extent > 2))
        found = set()
        for place in itertools.product(*sides):
            there = [
                message.tiles
                for message in messages
                if all(
                    step == 0 or sign * step in side for step, side in zip(message.move, place)
                )
            ]
            found.add(sum(there))
        return sorted(found - {0})

    def drain(sem, messages, sign):
        count = sum(
            jnp.where(exists(message.move, sign), message.tiles, 0) for message in messages
        )
        for total in totals(messages, sign):

            @pl.when(count == total)
            def _():
                some = gauge.at[0:total]
                pltpu.make_async_copy(some, some, sem).wait()

    def arrive(messages):
        drain(recv_sem.at[messages[0].number], messages, -1)

    made = []

    def add(group, number, move, src, dst, tiles=1, post=0):
        message = Message(number, move, src, dst, tiles, post)
        made.append(message)
        group.append(message)

    Y_IN, Z_IN, RIM, OUT, GEO, TERMS, BACK = 0, 1, 2, 3, 4, 6, 8
    face = lambda n, extent: extent - 1 if n == 0 else 0
    edge_tile = lambda n: pl.ds(face(n, ci) * cj // 128 * 128, 128)
    y_in, xy_in, z_in, yz_in, geo_in, x_out, out = [], [], [], [], [], [], []
    rim_in, corner_in, back_in = [], [], []
    for mx, x in STEPS:
        for my, y in STEPS:
            add(xy_in, Y_IN, (mx, my, 0), xys.at[2 * x + y], xyh.at[2 * x + y])
            add(out, OUT, (mx, my, 0), dys.at[y, NUM_TERMS + x], dxyr.at[2 * x + y])
            for mz, z in STEPS:
                n = 4 * x + 2 * y + z
                add(corner_in, RIM, (mx, my, mz), ez.at[z], xyzh.at[n])
                add(out, OUT, (mx, my, mz), dxyzs.at[n], dxyzr.at[n])
        add(geo_in, GEO + x, (mx, 0, 0), geo, geor.at[x], 0, 1 + x)
        add(back_in, BACK + x, (mx, 0, 0), back.at[1 - x], backr.at[x], 0, 3 + x)
        add(x_out, TERMS + x, (mx, 0, 0), terms, termr.at[x], 0, 5 + x)
        for mz, z in STEPS:
            n = 2 * x + z
            add(rim_in, RIM, (mx, 0, mz), zs.at[z, :, edge_tile(x)], xzh.at[n])
            add(out, OUT, (mx, 0, mz), dzs.at[z, NUM_TERMS + x], dxzr.at[n])
    for my, y in STEPS:
        add(y_in, Y_IN, (0, my, 0), ys.at[y], yh.at[y], NUM_FIELDS)
        add(out, OUT, (0, my, 0), dys.at[y, 0:NUM_TERMS], dyr.at[y], NUM_TERMS)
        for mz, z in STEPS:
            add(yz_in, Z_IN, (0, my, mz), ez.at[z], yzh.at[2 * y + z])
            add(out, OUT, (0, my, mz), dyzs.at[z], dyzr.at[2 * y + z])
    for mz, z in STEPS:
        add(z_in, Z_IN, (0, 0, mz), zs.at[z], zh.at[z], inner // 128)
        add(out, OUT, (0, 0, mz), dzs.at[z, 0:NUM_TERMS], dzr.at[z], NUM_TERMS)

    def signal(sem, move):
        @pl.when(exists(move, 1))
        def _():
            pl.semaphore_signal(sem, inc=1, device_id=peer(move), device_id_type=MESH)

    def heard(sem, moves):
        pl.semaphore_wait(sem, sum(exists(move, -1).astype(jnp.int32) for move in moves))


    def turned_rows(flats, total):
        parts = []
        for flat in flats:
            high = flat.astype(BF16).astype(F32)
            parts += [high, flat - high, high]
        spare = total - sum(part.shape[0] for part in parts)
        if spare > 0:
            parts.append(jnp.zeros((spare, ck), F32))
        return jnp.concatenate(parts, axis=0).T.astype(BF16)

    x_moves = [(step, 0, 0) for step, _ in STEPS]
    y_moves = [(0, step, 0) for step, _ in STEPS]
    z_moves = [(0, 0, step) for step, _ in STEPS]
    xy_moves = [(mx, my, 0) for mx, _ in STEPS for my, _ in STEPS]
    met = xy_moves + z_moves + x_moves + y_moves
    barrier = pltpu.get_barrier_semaphore()
    for move in met:
        signal(barrier, move)

    def load(src, dst, number):
        pltpu.make_async_copy(src, dst, load_sem.at[number]).start()

    def loaded(whole, number):
        pltpu.make_async_copy(whole, whole, load_sem.at[number]).wait()

    pairs = [(pos_in, pos), (li_in, li), (lj_in, lj), (lk_in, lk)]
    pairs += [(mot_in, mot), (heat_in, heat), (size_in, size)]
    for (src, dst), number in zip(pairs, (1, 2, 2, 2, 3, 4, 4)):
        load(src, dst, number)
    load(vel, fields.at[0:3], 0)
    load(sca, fields.at[3:6], 0)

    xys[...] = jnp.zeros_like(xys)
    zs[...] = jnp.zeros_like(zs)
    for message in y_in + xy_in + z_in + yz_in + rim_in + corner_in + out:
        message.blank()
    rows = lax.broadcasted_iota(jnp.int32, (inner, 128), 0)
    cols = lanes_of((inner, 128))
    target = jnp.where(cols < cj + 8, (cols - cj) * cj + cj - 1, (cols - cj - 8) * cj)
    chosen = (rows == target) & (cols >= cj) & (cols < cj + 16)
    edges[...] = jnp.where(chosen, 1.0, 0.0).astype(BF16)

    loaded(pos, 1)
    loaded(gauge.at[0 : 3 * slots // 1024], 2)
    xa, xb, lx = pair_weights(pos[0:1])
    ya, yb, ly = pair_weights(pos[1:2])
    za, zb, lz = pair_weights(pos[2:3])
    i0 = li[...].astype(F32) + lx
    j0 = lj[...].astype(F32) + ly
    k0 = lk[...].astype(F32) + lz

    def at(index, base, wa, wb):
        return jnp.where(base == index, wa, jnp.where(base + 1.0 == index, wb, 0.0))

    x_low, x_high = at(-1.0, i0, xa, xb), at(float(ci), i0, xa, xb)
    y_low, y_high = at(-1.0, j0, ya, yb), at(float(cj), j0, ya, yb)
    z_low, z_high = at(-1.0, k0, za, zb), at(float(ck), k0, za, zb)
    y_place = lj[...].astype(F32) + pos[1:2]
    z_place = lk[...].astype(F32) + pos[2:3]
    for n, row in enumerate((x_high, x_low, y_place, z_place)):
        geo[n : n + 1] = row
    xt[0:ci] = spots(0, ci, i0, xa, xb)
    xt[ci : 2 * ci] = jnp.concatenate([x_low, x_high, jnp.zeros((ci - 2, slots), F32)], axis=0)
    across = spots(0, cj, j0, ya, yb)
    rims = [
        jnp.broadcast_to(y_low, (8, slots)),
        jnp.broadcast_to(y_high, (8, slots)),
        jnp.zeros((128 - cj - 16, slots), F32),
    ]
    high, low = split(jnp.concatenate([across] + rims, axis=0))
    yt[0:128] = high
    yt[128:256] = low
    corners = [a * b for a in (x_low, x_high) for b in (y_low, y_high)]
    for n, row in enumerate(corners):
        corner[n : n + 1] = row
    line[...] = spots(0, ck, k0, za, zb)
    high, low = split(line[...])
    lines[0:ck] = high
    lines[ck : 2 * ck] = low

    for i in range(ci):
        high, low = split(xt[i : i + 1] * across)
        w_hi[i * cj : (i + 1) * cj] = high
        w_lo[i * cj : (i + 1) * cj] = low
    heard(barrier, met)
    for move in z_moves:
        signal(far, move)
    for message in geo_in:
        message.start()
    loaded(fields, 0)
    for y in range(2):
        row = face(y, cj)
        ys[y] = fields[:, :, row, :]
        for x in range(2):
            xys[2 * x + y, 0:NUM_FIELDS] = fields[:, face(x, ci), row, :]
    for message in xy_in + y_in:
        message.start()
    for f in range(NUM_FIELDS):
        turned = fields[f].reshape(inner, ck).T
        high, low = split(turned)
        ft_hi[f * ck : (f + 1) * ck] = high
        ft_lo[f * ck : (f + 1) * ck] = low
        zs[0, f : f + 1] = turned[ck - 1 : ck]
        zs[1, f : f + 1] = turned[0:1]
    for message in z_in:
        message.start()
    high, low = split(zs[...].reshape(16, inner))
    ez[...] = (nn(high, edges[...]) + nn(low, edges[...])).reshape(2, 8, 128)
    for x in range(2):
        plane = 0 if x == 0 else ci - 1

        @pl.when(exists(x_moves[x], -1))
        def _():
            for f in range(NUM_FIELDS):
                face_f[x, f * ck : (f + 1) * ck] = turned_rows([fields[f, plane]], 0)

    width = 256

    def collect(got, table, here, target, start=0):
        parts = [
            jnp.sum(got[n * ck : (n + 1) * ck] * table[:, here], axis=0, keepdims=True)
            for n in range(got.shape[0] // ck)
        ]
        for n, part in enumerate(parts):
            target(start + n, here, part)

    def put(f, here, value):
        sampled[f : f + 1, here] = value

    def sample(blocks):
        for s in blocks:
            here = slice(s * width, (s + 1) * width)
            for start in range(0, NUM_FIELDS, NUM_FIELDS // 2):
                part = slice(start * ck, (start + NUM_FIELDS // 2) * ck)
                got = nn(ft_hi[part], w_hi[:, here])
                got += nn(ft_hi[part], w_lo[:, here])
                got += nn(ft_lo[part], w_hi[:, here])
                collect(got, line, here, put, start)

    def ghosts():
        for x, places in enumerate(geo_in):

            @pl.when(exists(places.move, -1))
            def _():
                places.copy.wait_recv()
                there[x] = tent(cj, geor[x, 2:3]) * geor[x, x : x + 1]
                along[...] = tent(ck, geor[x, 3:4])
                high, low = split(along[...])
                alongs[x, 0:ck] = high
                alongs[x, ck : 2 * ck] = low
                high, low = split(there[x])
                w_there[0:cj] = high
                w_there[cj : 2 * cj] = high
                w_there[2 * cj : 3 * cj] = low

                def keep(f, here, value):
                    back[x, f : f + 1, here] = value

                for s in range(0, slots, width):
                    here = slice(s, s + width)
                    collect(nn(face_f[x], w_there[:, here]), along, here, keep)
                back_in[1 - x].copy.start()

    sample(range(1))
    heard(far, z_moves)
    for message in corner_in + rim_in + yz_in:
        message.start()

    early = lax.rem(me[0], 2) == 1
    blocks = slots // width

    @pl.when(early)
    def _():
        ghosts()
        sample(range(1, blocks))

    @pl.when(jnp.logical_not(early))
    def _():
        sample(range(1, blocks // 2))
        ghosts()
        sample(range(blocks // 2, blocks))

    arrive(y_in + xy_in)
    arrive(z_in + yz_in)
    flat = NUM_FIELDS * ci
    ends = jnp.concatenate(
        [yh[y].reshape(flat, ck) for y in range(2)] + [xyh[q] for q in range(4)], axis=0
    )
    count = ends.shape[0]
    high, low = split(ends)
    got = nn(jnp.concatenate([high, low], axis=0), lines[0:ck])
    got = got[0:count] + got[count:] + nn(high, lines[ck : 2 * ck])
    rest = None
    for q in range(4):
        first = 2 * flat + q * 8
        part = got[first : first + 8] * corner[q : q + 1]
        rest = part if rest is None else rest + part
    for f in range(NUM_FIELDS):
        total = sampled[f : f + 1] + rest[f : f + 1]
        for y, rim in enumerate((y_low, y_high)):
            first = y * flat + f * ci
            part = got[first : first + ci] * xt[0:ci]
            total += jnp.sum(part, axis=0, keepdims=True) * rim
        sampled[f : f + 1] = total

    lanes = lanes_of((8, 128))
    body = lanes < cj

    def half(tile, odd):
        return jnp.where(body, pltpu.roll(tile, 128 - cj, 1) if odd else tile, 0.0)

    def pick(tile, lane):
        return jnp.where(lanes == lane, tile, 0.0)

    def beyond(blocks, planes):
        count = 2 * planes.shape[0] * 8
        high, low = split(jnp.concatenate(blocks, axis=0))
        got = nn(jnp.concatenate([high, low], axis=0), yt[0:128])
        got = got[0:count] + got[count:] + nn(high, yt[128:256])
        for z, rim in enumerate((z_low, z_high)):
            total = None
            for b in range(planes.shape[0]):
                first = (z * planes.shape[0] + b) * 8
                part = got[first : first + 8] * planes[b : b + 1]
                total = part if total is None else total + part
            sampled[...] += total * rim

    blocks = []
    for z in range(2):
        for i in range(ci):
            first = i * cj // 128 * 128
            block = half(zh[z, :, first : first + 128], i * cj % 128 != 0)
            blocks.append(block + pick(yzh[z], cj + i) + pick(yzh[2 + z], cj + 8 + i))
    beyond(blocks, xt[0:ci])
    loaded(mot, 3)
    loaded(gauge.at[0 : 2 * slots // 1024], 4)
    for x, message in enumerate(back_in):

        @pl.when(exists(message.move, -1))
        def _():
            message.copy.wait_recv()
            sampled[0:NUM_FIELDS] += backr[x]

    arrive(rim_in + corner_in)
    blocks = []
    for z in range(2):
        for x in range(2):
            i = face(x, ci)
            block = half(xzh[2 * x + z], i * cj % 128 != 0)
            block += pick(xyzh[4 * x + z], cj + i) + pick(xyzh[4 * x + 2 + z], cj + 8 + i)
            blocks.append(block)
    beyond(blocks, xt[ci : ci + 2])

    gas = sampled[...]
    live = lanes_of((1, slots)) // TILE < tally[0]
    q = size[...]
    tp = heat[...]
    v = mot[...]
    drag = step_time / (0.5 * q)
    v_new = (v + drag * gas[0:3]) / (1.0 + drag)
    mass = q * jnp.sqrt(q)
    share = jnp.exp(4.0 * (tp - 1.0))
    decay = step_time * evap_rate * gas[5:6] * (share - gas[4:5])
    q_new = q - decay
    mass_new = q_new * jnp.sqrt(q_new)
    conduct = step_time * heat_rate * gas[5:6] / q
    tp_new = (tp + conduct * gas[3:4]) / (1.0 + conduct) - boiling_energy_drain * decay / q
    state[0:3] = jnp.where(live, v_new, v)
    state[3:4] = jnp.where(live, tp_new, tp)
    state[4:5] = jnp.where(live, q_new, q)
    terms[0:3] = jnp.where(live, mass * (v - v_new), 0.0)
    terms[3:4] = jnp.where(live, mass * (tp - tp_new), 0.0)
    terms[4:5] = jnp.where(live, mass - mass_new, 0.0)
    for message in x_out:
        message.start()

    stack = jnp.concatenate(
        [terms[...], jnp.zeros((8 - NUM_TERMS, slots), F32)], axis=0
    )
    for x in range(2):
        for y in range(2):
            row = 2 * (1 - x) + 1 - y
            for z, rim in enumerate((z_high, z_low)):
                part = stack * (corner[row : row + 1] * rim)
                part = jnp.sum(part, axis=1, keepdims=True)
                dxyzs[4 * x + 2 * y + z] = jnp.broadcast_to(part, (8, 128))
    for message in out:
        if 0 not in message.move:
            message.start()

    pieces = [xt[0:ci] * terms[c : c + 1] for c in range(NUM_TERMS)]
    pieces += [stack * xt[ci + 1 - x : ci + 2 - x] for x in range(2)]

    def fan(rims):
        return split(jnp.concatenate([piece * rim for rim in rims for piece in pieces], axis=0))

    def both(high, low, right):
        wide = nt(high, right)
        return wide[:, 0:128] + wide[:, 128:256] + nt(low, right[0:128])

    shape = (2, NUM_TERMS + 2, ci, 128)
    fan_hi[0], fan_lo[0] = fan((z_high, z_low))
    dzs[...] = both(fan_hi[0], fan_lo[0], yt[...]).reshape(shape)
    for z in range(2):
        tile = jnp.zeros((8, 128), F32)
        for c in range(NUM_TERMS):
            keep = (lanes == cj + c) | (lanes == cj + 8 + c)
            tile = jnp.where(keep, dzs[z, c], tile)
        dyzs[z] = tile
    for message in out:
        if message.move[2] != 0 and 0 in message.move:
            message.start()
    fan_hi[1], fan_lo[1] = fan((y_high, y_low))
    dys[...] = both(fan_hi[1], fan_lo[1], lines[...]).reshape(shape)
    for message in out:
        if message.move[2] == 0:
            message.start()

    for a in range(0, NUM_TERMS, 2):
        b = min(a + 2, NUM_TERMS)
        for c in range(a, b):
            high, low = split(line[...] * terms[c : c + 1])
            src_hi[c * ck : (c + 1) * ck] = high
            src_lo[c * ck : (c + 1) * ck] = low
        span = slice(a * ck, b * ck)
        if b - a == 2:
            got = nt(w_hi[...], src_hi[span])
            got += nt(w_hi[...], src_lo[span])
            got += nt(w_lo[...], src_hi[span])
        else:
            got = nt(w_hi[...], jnp.concatenate([src_hi[span], src_lo[span]], axis=0))
            got = got[:, 0:ck] + got[:, ck:] + nt(w_lo[...], src_hi[span])
        for c in range(a, b):
            dep[c] = got[:, (c - a) * ck : (c - a + 1) * ck].reshape(ci, cj, ck)

    for x, deposits in enumerate(x_out):
        plane = 0 if x == 0 else ci - 1

        @pl.when(exists(deposits.move, -1))
        def _():
            deposits.copy.wait_recv()
            high, low = split(
                jnp.concatenate([there[x] * termr[x, c : c + 1] for c in range(NUM_TERMS)], axis=0)
            )
            got = both(high, low, alongs[x])
            for c in range(NUM_TERMS):
                dep[c, plane] += got[c * cj : (c + 1) * cj]

    arrive(out)
    drain(send_sem.at[0], made, 1)
    for message in geo_in + back_in + x_out:
        message.leave()


def finish(
    part, old, dyr, dxyr, dzr, dxzr, dyzr, dxyzr, dep_out, state_out, dep, sem
):
    ci, cj, ck = dep.shape[1:]
    terms = dep.shape[0]
    side = pltpu.make_async_copy(old, state_out, sem.at[terms])
    side.start()
    lanes = lanes_of((8, 128))
    rows = lax.broadcasted_iota(jnp.int32, (8, 128), 0)
    ends = (0, ck - 1)

    def at_ends(first, second, where):
        return jnp.where(where == ends[0], first, jnp.where(where == ends[1], second, 0.0))

    corner = []
    for x in range(2):
        for y in range(2):
            lane = cj + 8 if y == 0 else cj
            first, second = (dxyzr[4 * x + 2 * y + z, :, lane : lane + 1] for z in range(2))
            corner.append(dxyr[2 * x + y] + at_ends(first, second, lanes))
    row = lax.broadcasted_iota(jnp.int32, (32, ci * ck), 0)
    row = jnp.where(row < 16, row, row - 16)
    lane = jnp.where(row < 8, row * ck, (row - 8) * ck + ck - 1)
    spot = jnp.where(lanes_of((32, ci * ck)) == lane, 1.0, 0.0).astype(BF16)
    outs = []
    for c in range(terms):
        block = []
        for z in range(2):
            total = dzr[z, c]
            for x in range(2):
                plane = 0 if x == 0 else ci - 1
                total += jnp.where(rows == plane, dxzr[2 * x + z, c : c + 1], 0.0)
            block.append(total)
        block = jnp.concatenate(block, axis=0)
        high = block.astype(BF16).astype(F32)
        turned = jnp.concatenate([high, block - high], axis=0).T[0:cj].astype(BF16)
        ends_of = nn(turned, spot)
        for i in range(ci):
            dep[c, i] = part[c, i] + ends_of[:, i * ck : (i + 1) * ck]
        for y in range(2):
            row = 0 if y == 0 else cj - 1
            lane = cj + 8 + c if y == 0 else cj + c
            first, second = (dyzr[2 * y + z, :, lane : lane + 1] for z in range(2))
            dep[c, :, row, :] += dyr[y, c] + at_ends(first, second, lanes)
            for x in range(2):
                plane = 0 if x == 0 else ci - 1
                dep[c, plane, row : row + 1, :] += corner[2 * x + y][c : c + 1]
        out = pltpu.make_async_copy(dep.at[c], dep_out.at[c], sem.at[c])
        out.start()
        outs.append(out)
    for out in outs:
        out.wait()
    side.wait()


def local(counts, vel, sca, pos, mot, heat, size, li, lj, lk, tally):
    ci, cj, ck = vel.shape[1:]
    slots = heat.shape[0]
    inner = ci * cj
    vmem = pl.BlockSpec(memory_space=pltpu.VMEM)
    hbm = pl.BlockSpec(memory_space=pltpu.HBM)
    row = lambda value: value.reshape(1, slots)
    pin = lambda value: pltpu.with_memory_space_constraint(value, pltpu.HBM)
    tile = (8, 128)
    f32 = lambda *shape: pltpu.VMEM(shape, F32)
    i32 = lambda *shape: pltpu.VMEM(shape, jnp.int32)
    b16 = lambda *shape: pltpu.VMEM(shape, BF16)
    struct = lambda *shape: jax.ShapeDtypeStruct(shape, F32)
    scratch = [
        f32(NUM_FIELDS, ci, cj, ck),
        f32(3, slots),
        f32(3, slots),
        f32(1, slots),
        f32(1, slots),
        i32(1, slots),
        i32(1, slots),
        i32(1, slots),
        b16(NUM_FIELDS * ck, inner),
        b16(NUM_FIELDS * ck, inner),
        b16(inner, slots),
        b16(inner, slots),
        f32(4, slots),
        f32(2 * ci, slots),
        b16(256, slots),
        f32(ck, slots),
        b16(2 * ck, slots),
        b16(NUM_TERMS * ck, slots),
        b16(NUM_TERMS * ck, slots),
        f32(8, slots),
        f32(4, slots),
        f32(2, NUM_FIELDS, slots),
        f32(NUM_TERMS, slots),
        f32(2, cj, slots),
        f32(ck, slots),
        b16(2, 2 * ck, slots),
        b16(3 * cj, slots),
        b16(2, NUM_FIELDS * ck, 3 * cj),
        f32(2, NUM_FIELDS, ci, ck),
        f32(4, *tile),
        f32(2, 8, inner),
        f32(4, *tile),
        f32(4, *tile),
        f32(8, *tile),
        f32(2, 4, slots),
        f32(2, NUM_FIELDS, slots),
        f32(2, NUM_TERMS, slots),
        f32(2, NUM_FIELDS, ci, ck),
        f32(4, *tile),
        f32(2, 8, inner),
        f32(2, *tile),
        f32(2, NUM_TERMS + 2, ci, ck),
        f32(2, NUM_TERMS + 2, ci, ck),
        f32(2, *tile),
        f32(8, *tile),
        b16(inner, 128),
        b16(2, 2 * (NUM_TERMS + 2) * ci, slots),
        b16(2, 2 * (NUM_TERMS + 2) * ci, slots),
        f32(256, *tile),
        pltpu.SemaphoreType.DMA((5,)),
        pltpu.SemaphoreType.DMA((7,)),
        pltpu.SemaphoreType.DMA((10,)),
        pltpu.SemaphoreType.REGULAR,
    ]
    results = (
        struct(NUM_TERMS, ci, cj, ck),
        struct(NUM_TERMS, slots),
        struct(2, NUM_TERMS, ci, ck),
        struct(4, *tile),
        struct(2, NUM_TERMS, ci, ck),
        struct(4, *tile),
        struct(4, *tile),
        struct(8, *tile),
    )
    arrays = (vel, sca, pos, mot, row(heat), row(size), row(li), row(lj), row(lk))
    parts = pl.pallas_call(
        functools.partial(kernel, counts),
        out_shape=results,
        in_specs=[hbm] * len(arrays) + [pl.BlockSpec(memory_space=pltpu.SMEM)],
        out_specs=(vmem,) * len(results),
        scratch_shapes=scratch,
        compiler_params=pltpu.CompilerParams(
            collective_id=0, has_side_effects=True, vmem_limit_bytes=32 * 2**20
        ),
    )(*[pin(value) for value in arrays], tally)
    return pl.pallas_call(
        finish,
        out_shape=results[0:2],
        in_specs=[vmem] * len(results),
        out_specs=(pl.BlockSpec(memory_space=pl.ANY),) * 2,
        scratch_shapes=[
            f32(NUM_TERMS, ci, cj, ck),
            pltpu.SemaphoreType.DMA((NUM_TERMS + 1,)),
        ],
        compiler_params=pltpu.CompilerParams(vmem_limit_bytes=12 * 2**20),
    )(*parts)


def solution(mesh):
    bricks = P(None, AXES[0], AXES[1], AXES[2])
    rows = P(None, AXES)
    flat = P(AXES)
    counts = tuple(mesh.shape[axis] for axis in AXES)
    return jax.shard_map(
        functools.partial(local, counts),
        mesh=mesh,
        in_specs=(bricks, bricks, rows, rows) + (flat,) * 6,
        out_specs=(bricks, rows),
        check_vma=False,
    )
```

```python
import functools
import itertools

import jax
import jax.numpy as jnp
from jax import lax
from jax.experimental import pallas as pl
from jax.experimental.pallas import tpu as pltpu
from jax.sharding import PartitionSpec as P

TILE = 128
AXES = ("gx", "gy", "gz")
MESH = pl.DeviceIdType.MESH
F32 = jnp.float32
BF16 = jnp.bfloat16

step_time = 0.25
evap_rate = 1.0
heat_rate = 2.0
boiling_energy_drain = 0.3

STEPS = ((1, 0), (-1, 1))
NUM_TERMS = 5
NUM_FIELDS = 6


def split(value):
    high = value.astype(BF16)
    return high, (value - high.astype(F32)).astype(BF16)


def nn(a, b):
    return lax.dot_general(a, b, (((1,), (0,)), ((), ())), preferred_element_type=F32)


def nt(a, b):
    return lax.dot_general(a, b, (((1,), (1,)), ((), ())), preferred_element_type=F32)


def pair_weights(offset):
    lower = jnp.where(offset < 0.0, -1.0, 0.0)
    first = jnp.maximum(0.0, 1.0 - jnp.abs(offset - lower))
    second = jnp.maximum(0.0, 1.0 - jnp.abs(offset - (lower + 1.0)))
    return first, second, lower


def lanes_of(shape):
    return lax.broadcasted_iota(jnp.int32, shape, len(shape) - 1)


def tent(count, place):
    rows = lax.broadcasted_iota(jnp.int32, (count, place.shape[1]), 0).astype(F32)
    return jnp.maximum(0.0, 1.0 - jnp.abs(rows - place))


def spots(first, count, base, wa, wb):
    rows = (lax.broadcasted_iota(jnp.int32, (count, base.shape[1]), 0) + first).astype(F32)
    return jnp.where(rows == base, wa, jnp.where(rows == base + 1.0, wb, 0.0))


def kernel(
    counts,
    vel,
    sca,
    pos_in,
    mot_in,
    heat_in,
    size_in,
    li_in,
    lj_in,
    lk_in,
    tally,
    dep,
    state,
    dyr,
    dxyr,
    dzr,
    dxzr,
    dyzr,
    dxyzr,
    fields,
    pos,
    mot,
    heat,
    size,
    li,
    lj,
    lk,
    ft_hi,
    ft_lo,
    w_hi,
    w_lo,
    corner,
    xt,
    yt,
    line,
    lines,
    src_hi,
    src_lo,
    sampled,
    geo,
    back,
    terms,
    there,
    along,
    alongs,
    w_there,
    face_f,
    yh,
    xyh,
    zh,
    xzh,
    yzh,
    xyzh,
    geor,
    backr,
    termr,
    ys,
    xys,
    zs,
    ez,
    dys,
    dzs,
    dyzs,
    dxyzs,
    edges,
    fan_hi,
    fan_lo,
    gauge,
    load_sem,
    send_sem,
    recv_sem,
    far,
):
    ci, cj, ck = vel.shape[1:]
    slots = heat.shape[1]
    inner = ci * cj
    me = [lax.axis_index(axis) for axis in AXES]

    def exists(move, sign):
        good = None
        for d in range(3):
            step = sign * move[d]
            if step == 1:
                test = me[d] < counts[d] - 1
            elif step == -1:
                test = me[d] > 0
            else:
                continue
            good = test if good is None else jnp.logical_and(good, test)
        return good

    def peer(move):
        return tuple(lax.rem(me[d] + move[d] + counts[d], counts[d]) for d in range(3))

    class Message:
        def __init__(self, number, move, src, dst, tiles, post):
            self.move = move
            self.dst = dst
            self.tiles = tiles
            self.number = number
            self.copy = pltpu.make_async_remote_copy(
                src_ref=src,
                dst_ref=dst,
                send_sem=send_sem.at[post],
                recv_sem=recv_sem.at[number],
                device_id=peer(move),
                device_id_type=MESH,
            )

        def start(self):
            @pl.when(exists(self.move, 1))
            def _():
                self.copy.start()

        def blank(self):
            @pl.when(jnp.logical_not(exists(self.move, -1)))
            def _():
                self.dst[...] = jnp.zeros(self.dst.shape, F32)

        def leave(self):
            @pl.when(exists(self.move, 1))
            def _():
                self.copy.wait_send()

    def totals(messages, sign):
        sides = []
        for extent in counts:
            low, high = (-1,), (1,)
            sides.append([()] if extent == 1 else [low, high] + [low + high] * (extent > 2))
        found = set()
        for place in itertools.product(*sides):
            there = [
                message.tiles
                for message in messages
                if all(
                    step == 0 or sign * step in side for step, side in zip(message.move, place)
                )
            ]
            found.add(sum(there))
        return sorted(found - {0})

    def drain(sem, messages, sign):
        count = sum(
            jnp.where(exists(message.move, sign), message.tiles, 0) for message in messages
        )
        for total in totals(messages, sign):

            @pl.when(count == total)
            def _():
                some = gauge.at[0:total]
                pltpu.make_async_copy(some, some, sem).wait()

    def arrive(messages):
        drain(recv_sem.at[messages[0].number], messages, -1)

    made = []

    def add(group, number, move, src, dst, tiles=1, post=0):
        message = Message(number, move, src, dst, tiles, post)
        made.append(message)
        group.append(message)

    Y_IN, Z_IN, RIM, OUT, GEO, TERMS, BACK = 0, 1, 2, 3, 4, 6, 8
    face = lambda n, extent: extent - 1 if n == 0 else 0
    edge_tile = lambda n: pl.ds(face(n, ci) * cj // 128 * 128, 128)
    y_in, xy_in, z_in, yz_in, geo_in, x_out, out = [], [], [], [], [], [], []
    rim_in, corner_in, back_in = [], [], []
    for mx, x in STEPS:
        for my, y in STEPS:
            add(xy_in, Y_IN, (mx, my, 0), xys.at[2 * x + y], xyh.at[2 * x + y])
            add(out, OUT, (mx, my, 0), dys.at[y, NUM_TERMS + x], dxyr.at[2 * x + y])
            for mz, z in STEPS:
                n = 4 * x + 2 * y + z
                add(corner_in, RIM, (mx, my, mz), ez.at[z], xyzh.at[n])
                add(out, OUT, (mx, my, mz), dxyzs.at[n], dxyzr.at[n])
        add(geo_in, GEO + x, (mx, 0, 0), geo, geor.at[x], 0, 1 + x)
        add(back_in, BACK + x, (mx, 0, 0), back.at[1 - x], backr.at[x], 0, 3 + x)
        add(x_out, TERMS + x, (mx, 0, 0), terms, termr.at[x], 0, 5 + x)
        for mz, z in STEPS:
            n = 2 * x + z
            add(rim_in, RIM, (mx, 0, mz), zs.at[z, :, edge_tile(x)], xzh.at[n])
            add(out, OUT, (mx, 0, mz), dzs.at[z, NUM_TERMS + x], dxzr.at[n])
    for my, y in STEPS:
        add(y_in, Y_IN, (0, my, 0), ys.at[y], yh.at[y], NUM_FIELDS)
        add(out, OUT, (0, my, 0), dys.at[y, 0:NUM_TERMS], dyr.at[y], NUM_TERMS)
        for mz, z in STEPS:
            add(yz_in, Z_IN, (0, my, mz), ez.at[z], yzh.at[2 * y + z])
            add(out, OUT, (0, my, mz), dyzs.at[z], dyzr.at[2 * y + z])
    for mz, z in STEPS:
        add(z_in, Z_IN, (0, 0, mz), zs.at[z], zh.at[z], inner // 128)
        add(out, OUT, (0, 0, mz), dzs.at[z, 0:NUM_TERMS], dzr.at[z], NUM_TERMS)

    def signal(sem, move):
        @pl.when(exists(move, 1))
        def _():
            pl.semaphore_signal(sem, inc=1, device_id=peer(move), device_id_type=MESH)

    def heard(sem, moves):
        pl.semaphore_wait(sem, sum(exists(move, -1).astype(jnp.int32) for move in moves))


    def turned_rows(flats, total):
        parts = []
        for flat in flats:
            high = flat.astype(BF16).astype(F32)
            parts += [high, flat - high, high]
        spare = total - sum(part.shape[0] for part in parts)
        if spare > 0:
            parts.append(jnp.zeros((spare, ck), F32))
        return jnp.concatenate(parts, axis=0).T.astype(BF16)

    x_moves = [(step, 0, 0) for step, _ in STEPS]
    y_moves = [(0, step, 0) for step, _ in STEPS]
    z_moves = [(0, 0, step) for step, _ in STEPS]
    xy_moves = [(mx, my, 0) for mx, _ in STEPS for my, _ in STEPS]
    met = xy_moves + z_moves + x_moves + y_moves
    barrier = pltpu.get_barrier_semaphore()
    for move in met:
        signal(barrier, move)

    def load(src, dst, number):
        pltpu.make_async_copy(src, dst, load_sem.at[number]).start()

    def loaded(whole, number):
        pltpu.make_async_copy(whole, whole, load_sem.at[number]).wait()

    pairs = [(pos_in, pos), (li_in, li), (lj_in, lj), (lk_in, lk)]
    pairs += [(mot_in, mot), (heat_in, heat), (size_in, size)]
    for (src, dst), number in zip(pairs, (1, 2, 2, 2, 3, 4, 4)):
        load(src, dst, number)
    load(vel, fields.at[0:3], 0)
    load(sca, fields.at[3:6], 0)

    xys[...] = jnp.zeros_like(xys)
    zs[...] = jnp.zeros_like(zs)
    for message in y_in + xy_in + z_in + yz_in + rim_in + corner_in + out:
        message.blank()
    rows = lax.broadcasted_iota(jnp.int32, (inner, 128), 0)
    cols = lanes_of((inner, 128))
    target = jnp.where(cols < cj + 8, (cols - cj) * cj + cj - 1, (cols - cj - 8) * cj)
    chosen = (rows == target) & (cols >= cj) & (cols < cj + 16)
    edges[...] = jnp.where(chosen, 1.0, 0.0).astype(BF16)

    loaded(pos, 1)
    loaded(gauge.at[0 : 3 * slots // 1024], 2)
    xa, xb, lx = pair_weights(pos[0:1])
    ya, yb, ly = pair_weights(pos[1:2])
    za, zb, lz = pair_weights(pos[2:3])
    i0 = li[...].astype(F32) + lx
    j0 = lj[...].astype(F32) + ly
    k0 = lk[...].astype(F32) + lz

    def at(index, base, wa, wb):
        return jnp.where(base == index, wa, jnp.where(base + 1.0 == index, wb, 0.0))

    x_low, x_high = at(-1.0, i0, xa, xb), at(float(ci), i0, xa, xb)
    y_low, y_high = at(-1.0, j0, ya, yb), at(float(cj), j0, ya, yb)
    z_low, z_high = at(-1.0, k0, za, zb), at(float(ck), k0, za, zb)
    y_place = lj[...].astype(F32) + pos[1:2]
    z_place = lk[...].astype(F32) + pos[2:3]
    for n, row in enumerate((x_high, x_low, y_place, z_place)):
        geo[n : n + 1] = row
    xt[0:ci] = spots(0, ci, i0, xa, xb)
    xt[ci : 2 * ci] = jnp.concatenate([x_low, x_high, jnp.zeros((ci - 2, slots), F32)], axis=0)
    across = spots(0, cj, j0, ya, yb)
    rims = [
        jnp.broadcast_to(y_low, (8, slots)),
        jnp.broadcast_to(y_high, (8, slots)),
        jnp.zeros((128 - cj - 16, slots), F32),
    ]
    high, low = split(jnp.concatenate([across] + rims, axis=0))
    yt[0:128] = high
    yt[128:256] = low
    corners = [a * b for a in (x_low, x_high) for b in (y_low, y_high)]
    for n, row in enumerate(corners):
        corner[n : n + 1] = row
    line[...] = spots(0, ck, k0, za, zb)
    high, low = split(line[...])
    lines[0:ck] = high
    lines[ck : 2 * ck] = low

    for i in range(ci):
        high, low = split(xt[i : i + 1] * across)
        w_hi[i * cj : (i + 1) * cj] = high
        w_lo[i * cj : (i + 1) * cj] = low
    heard(barrier, met)
    for move in z_moves:
        signal(far, move)
    for message in geo_in:
        message.start()
    loaded(fields, 0)
    for y in range(2):
        row = face(y, cj)
        ys[y] = fields[:, :, row, :]
        for x in range(2):
            xys[2 * x + y, 0:NUM_FIELDS] = fields[:, face(x, ci), row, :]
    for message in xy_in + y_in:
        message.start()
    for f in range(NUM_FIELDS):
        turned = fields[f].reshape(inner, ck).T
        high, low = split(turned)
        ft_hi[f * ck : (f + 1) * ck] = high
        ft_lo[f * ck : (f + 1) * ck] = low
        zs[0, f : f + 1] = turned[ck - 1 : ck]
        zs[1, f : f + 1] = turned[0:1]
    for message in z_in:
        message.start()
    high, low = split(zs[...].reshape(16, inner))
    ez[...] = (nn(high, edges[...]) + nn(low, edges[...])).reshape(2, 8, 128)
    for x in range(2):
        plane = 0 if x == 0 else ci - 1

        @pl.when(exists(x_moves[x], -1))
        def _():
            for f in range(NUM_FIELDS):
                face_f[x, f * ck : (f + 1) * ck] = turned_rows([fields[f, plane]], 0)

    width = 256

    def collect(got, table, here, target, start=0):
        parts = [
            jnp.sum(got[n * ck : (n + 1) * ck] * table[:, here], axis=0, keepdims=True)
            for n in range(got.shape[0] // ck)
        ]
        for n, part in enumerate(parts):
            target(start + n, here, part)

    def put(f, here, value):
        sampled[f : f + 1, here] = value

    def sample(blocks):
        for s in blocks:
            here = slice(s * width, (s + 1) * width)
            for start in range(0, NUM_FIELDS, NUM_FIELDS // 2):
                part = slice(start * ck, (start + NUM_FIELDS // 2) * ck)
                got = nn(ft_hi[part], w_hi[:, here])
                got += nn(ft_hi[part], w_lo[:, here])
                got += nn(ft_lo[part], w_hi[:, here])
                collect(got, line, here, put, start)

    def ghosts():
        for x, places in enumerate(geo_in):

            @pl.when(exists(places.move, -1))
            def _():
                places.copy.wait_recv()
                there[x] = tent(cj, geor[x, 2:3]) * geor[x, x : x + 1]
                along[...] = tent(ck, geor[x, 3:4])
                high, low = split(along[...])
                alongs[x, 0:ck] = high
                alongs[x, ck : 2 * ck] = low
                high, low = split(there[x])
                w_there[0:cj] = high
                w_there[cj : 2 * cj] = high
                w_there[2 * cj : 3 * cj] = low

                def keep(f, here, value):
                    back[x, f : f + 1, here] = value

                for s in range(0, slots, width):
                    here = slice(s, s + width)
                    collect(nn(face_f[x], w_there[:, here]), along, here, keep)
                back_in[1 - x].copy.start()

    sample(range(1))
    heard(far, z_moves)
    for message in corner_in + rim_in + yz_in:
        message.start()

    early = lax.rem(me[0], 2) == 1
    blocks = slots // width

    @pl.when(early)
    def _():
        ghosts()
        sample(range(1, blocks))

    @pl.when(jnp.logical_not(early))
    def _():
        sample(range(1, blocks // 2))
        ghosts()
        sample(range(blocks // 2, blocks))

    arrive(y_in + xy_in)
    arrive(z_in + yz_in)
    flat = NUM_FIELDS * ci
    ends = jnp.concatenate(
        [yh[y].reshape(flat, ck) for y in range(2)] + [xyh[q] for q in range(4)], axis=0
    )
    count = ends.shape[0]
    high, low = split(ends)
    got = nn(jnp.concatenate([high, low], axis=0), lines[0:ck])
    got = got[0:count] + got[count:] + nn(high, lines[ck : 2 * ck])
    rest = None
    for q in range(4):
        first = 2 * flat + q * 8
        part = got[first : first + 8] * corner[q : q + 1]
        rest = part if rest is None else rest + part
    for f in range(NUM_FIELDS):
        total = sampled[f : f + 1] + rest[f : f + 1]
        for y, rim in enumerate((y_low, y_high)):
            first = y * flat + f * ci
            part = got[first : first + ci] * xt[0:ci]
            total += jnp.sum(part, axis=0, keepdims=True) * rim
        sampled[f : f + 1] = total

    lanes = lanes_of((8, 128))
    body = lanes < cj

    def half(tile, odd):
        return jnp.where(body, pltpu.roll(tile, 128 - cj, 1) if odd else tile, 0.0)

    def pick(tile, lane):
        return jnp.where(lanes == lane, tile, 0.0)

    def beyond(blocks, planes):
        count = 2 * planes.shape[0] * 8
        high, low = split(jnp.concatenate(blocks, axis=0))
        got = nn(jnp.concatenate([high, low], axis=0), yt[0:128])
        got = got[0:count] + got[count:] + nn(high, yt[128:256])
        for z, rim in enumerate((z_low, z_high)):
            total = None
            for b in range(planes.shape[0]):
                first = (z * planes.shape[0] + b) * 8
                part = got[first : first + 8] * planes[b : b + 1]
                total = part if total is None else total + part
            sampled[...] += total * rim

    blocks = []
    for z in range(2):
        for i in range(ci):
            first = i * cj // 128 * 128
            block = half(zh[z, :, first : first + 128], i * cj % 128 != 0)
            blocks.append(block + pick(yzh[z], cj + i) + pick(yzh[2 + z], cj + 8 + i))
    beyond(blocks, xt[0:ci])
    loaded(mot, 3)
    loaded(gauge.at[0 : 2 * slots // 1024], 4)
    for x, message in enumerate(back_in):

        @pl.when(exists(message.move, -1))
        def _():
            message.copy.wait_recv()
            sampled[0:NUM_FIELDS] += backr[x]

    arrive(rim_in + corner_in)
    blocks = []
    for z in range(2):
        for x in range(2):
            i = face(x, ci)
            block = half(xzh[2 * x + z], i * cj % 128 != 0)
            block += pick(xyzh[4 * x + z], cj + i) + pick(xyzh[4 * x + 2 + z], cj + 8 + i)
            blocks.append(block)
    beyond(blocks, xt[ci : ci + 2])

    gas = sampled[...]
    live = lanes_of((1, slots)) // TILE < tally[0]
    q = size[...]
    tp = heat[...]
    v = mot[...]
    drag = step_time / (0.5 * q)
    v_new = (v + drag * gas[0:3]) / (1.0 + drag)
    mass = q * jnp.sqrt(q)
    share = jnp.exp(4.0 * (tp - 1.0))
    decay = step_time * evap_rate * gas[5:6] * (share - gas[4:5])
    q_new = q - decay
    mass_new = q_new * jnp.sqrt(q_new)
    conduct = step_time * heat_rate * gas[5:6] / q
    tp_new = (tp + conduct * gas[3:4]) / (1.0 + conduct) - boiling_energy_drain * decay / q
    state[0:3] = jnp.where(live, v_new, v)
    state[3:4] = jnp.where(live, tp_new, tp)
    state[4:5] = jnp.where(live, q_new, q)
    terms[0:3] = jnp.where(live, mass * (v - v_new), 0.0)
    terms[3:4] = jnp.where(live, mass * (tp - tp_new), 0.0)
    terms[4:5] = jnp.where(live, mass - mass_new, 0.0)
    for message in x_out:
        message.start()

    stack = jnp.concatenate(
        [terms[...], jnp.zeros((8 - NUM_TERMS, slots), F32)], axis=0
    )
    for x in range(2):
        for y in range(2):
            row = 2 * (1 - x) + 1 - y
            for z, rim in enumerate((z_high, z_low)):
                part = stack * (corner[row : row + 1] * rim)
                part = jnp.sum(part, axis=1, keepdims=True)
                dxyzs[4 * x + 2 * y + z] = jnp.broadcast_to(part, (8, 128))
    for message in out:
        if 0 not in message.move:
            message.start()

    pieces = [xt[0:ci] * terms[c : c + 1] for c in range(NUM_TERMS)]
    pieces += [stack * xt[ci + 1 - x : ci + 2 - x] for x in range(2)]

    def fan(rims):
        return split(jnp.concatenate([piece * rim for rim in rims for piece in pieces], axis=0))

    def both(high, low, right):
        wide = nt(high, right)
        return wide[:, 0:128] + wide[:, 128:256] + nt(low, right[0:128])

    shape = (2, NUM_TERMS + 2, ci, 128)
    fan_hi[1], fan_lo[1] = fan((y_high, y_low))
    dys[...] = both(fan_hi[1], fan_lo[1], lines[...]).reshape(shape)
    for message in out:
        if message.move[2] == 0:
            message.start()
    fan_hi[0], fan_lo[0] = fan((z_high, z_low))
    dzs[...] = both(fan_hi[0], fan_lo[0], yt[...]).reshape(shape)
    for z in range(2):
        tile = jnp.zeros((8, 128), F32)
        for c in range(NUM_TERMS):
            keep = (lanes == cj + c) | (lanes == cj + 8 + c)
            tile = jnp.where(keep, dzs[z, c], tile)
        dyzs[z] = tile
    for message in out:
        if message.move[2] != 0 and 0 in message.move:
            message.start()

    for a in range(0, NUM_TERMS, 2):
        b = min(a + 2, NUM_TERMS)
        for c in range(a, b):
            high, low = split(line[...] * terms[c : c + 1])
            src_hi[c * ck : (c + 1) * ck] = high
            src_lo[c * ck : (c + 1) * ck] = low
        span = slice(a * ck, b * ck)
        if b - a == 2:
            got = nt(w_hi[...], src_hi[span])
            got += nt(w_hi[...], src_lo[span])
            got += nt(w_lo[...], src_hi[span])
        else:
            got = nt(w_hi[...], jnp.concatenate([src_hi[span], src_lo[span]], axis=0))
            got = got[:, 0:ck] + got[:, ck:] + nt(w_lo[...], src_hi[span])
        for c in range(a, b):
            dep[c] = got[:, (c - a) * ck : (c - a + 1) * ck].reshape(ci, cj, ck)

    for x, deposits in enumerate(x_out):
        plane = 0 if x == 0 else ci - 1

        @pl.when(exists(deposits.move, -1))
        def _():
            deposits.copy.wait_recv()
            high, low = split(
                jnp.concatenate([there[x] * termr[x, c : c + 1] for c in range(NUM_TERMS)], axis=0)
            )
            got = both(high, low, alongs[x])
            for c in range(NUM_TERMS):
                dep[c, plane] += got[c * cj : (c + 1) * cj]

    arrive(out)
    drain(send_sem.at[0], made, 1)
    for message in geo_in + back_in + x_out:
        message.leave()


def finish(
    part, old, dyr, dxyr, dzr, dxzr, dyzr, dxyzr, dep_out, state_out, dep, sem
):
    ci, cj, ck = dep.shape[1:]
    terms = dep.shape[0]
    side = pltpu.make_async_copy(old, state_out, sem.at[terms])
    side.start()
    lanes = lanes_of((8, 128))
    rows = lax.broadcasted_iota(jnp.int32, (8, 128), 0)
    ends = (0, ck - 1)

    def at_ends(first, second, where):
        return jnp.where(where == ends[0], first, jnp.where(where == ends[1], second, 0.0))

    corner = []
    for x in range(2):
        for y in range(2):
            lane = cj + 8 if y == 0 else cj
            first, second = (dxyzr[4 * x + 2 * y + z, :, lane : lane + 1] for z in range(2))
            corner.append(dxyr[2 * x + y] + at_ends(first, second, lanes))
    row = lax.broadcasted_iota(jnp.int32, (32, ci * ck), 0)
    row = jnp.where(row < 16, row, row - 16)
    lane = jnp.where(row < 8, row * ck, (row - 8) * ck + ck - 1)
    spot = jnp.where(lanes_of((32, ci * ck)) == lane, 1.0, 0.0).astype(BF16)
    outs = []
    for c in range(terms):
        block = []
        for z in range(2):
            total = dzr[z, c]
            for x in range(2):
                plane = 0 if x == 0 else ci - 1
                total += jnp.where(rows == plane, dxzr[2 * x + z, c : c + 1], 0.0)
            block.append(total)
        block = jnp.concatenate(block, axis=0)
        high = block.astype(BF16).astype(F32)
        turned = jnp.concatenate([high, block - high], axis=0).T[0:cj].astype(BF16)
        ends_of = nn(turned, spot)
        for i in range(ci):
            dep[c, i] = part[c, i] + ends_of[:, i * ck : (i + 1) * ck]
        for y in range(2):
            row = 0 if y == 0 else cj - 1
            lane = cj + 8 + c if y == 0 else cj + c
            first, second = (dyzr[2 * y + z, :, lane : lane + 1] for z in range(2))
            dep[c, :, row, :] += dyr[y, c] + at_ends(first, second, lanes)
            for x in range(2):
                plane = 0 if x == 0 else ci - 1
                dep[c, plane, row : row + 1, :] += corner[2 * x + y][c : c + 1]
        out = pltpu.make_async_copy(dep.at[c], dep_out.at[c], sem.at[c])
        out.start()
        outs.append(out)
    for out in outs:
        out.wait()
    side.wait()


def local(counts, vel, sca, pos, mot, heat, size, li, lj, lk, tally):
    ci, cj, ck = vel.shape[1:]
    slots = heat.shape[0]
    inner = ci * cj
    vmem = pl.BlockSpec(memory_space=pltpu.VMEM)
    hbm = pl.BlockSpec(memory_space=pltpu.HBM)
    row = lambda value: value.reshape(1, slots)
    pin = lambda value: pltpu.with_memory_space_constraint(value, pltpu.HBM)
    tile = (8, 128)
    f32 = lambda *shape: pltpu.VMEM(shape, F32)
    i32 = lambda *shape: pltpu.VMEM(shape, jnp.int32)
    b16 = lambda *shape: pltpu.VMEM(shape, BF16)
    struct = lambda *shape: jax.ShapeDtypeStruct(shape, F32)
    scratch = [
        f32(NUM_FIELDS, ci, cj, ck),
        f32(3, slots),
        f32(3, slots),
        f32(1, slots),
        f32(1, slots),
        i32(1, slots),
        i32(1, slots),
        i32(1, slots),
        b16(NUM_FIELDS * ck, inner),
        b16(NUM_FIELDS * ck, inner),
        b16(inner, slots),
        b16(inner, slots),
        f32(4, slots),
        f32(2 * ci, slots),
        b16(256, slots),
        f32(ck, slots),
        b16(2 * ck, slots),
        b16(NUM_TERMS * ck, slots),
        b16(NUM_TERMS * ck, slots),
        f32(8, slots),
        f32(4, slots),
        f32(2, NUM_FIELDS, slots),
        f32(NUM_TERMS, slots),
        f32(2, cj, slots),
        f32(ck, slots),
        b16(2, 2 * ck, slots),
        b16(3 * cj, slots),
        b16(2, NUM_FIELDS * ck, 3 * cj),
        f32(2, NUM_FIELDS, ci, ck),
        f32(4, *tile),
        f32(2, 8, inner),
        f32(4, *tile),
        f32(4, *tile),
        f32(8, *tile),
        f32(2, 4, slots),
        f32(2, NUM_FIELDS, slots),
        f32(2, NUM_TERMS, slots),
        f32(2, NUM_FIELDS, ci, ck),
        f32(4, *tile),
        f32(2, 8, inner),
        f32(2, *tile),
        f32(2, NUM_TERMS + 2, ci, ck),
        f32(2, NUM_TERMS + 2, ci, ck),
        f32(2, *tile),
        f32(8, *tile),
        b16(inner, 128),
        b16(2, 2 * (NUM_TERMS + 2) * ci, slots),
        b16(2, 2 * (NUM_TERMS + 2) * ci, slots),
        f32(256, *tile),
        pltpu.SemaphoreType.DMA((5,)),
        pltpu.SemaphoreType.DMA((7,)),
        pltpu.SemaphoreType.DMA((10,)),
        pltpu.SemaphoreType.REGULAR,
    ]
    results = (
        struct(NUM_TERMS, ci, cj, ck),
        struct(NUM_TERMS, slots),
        struct(2, NUM_TERMS, ci, ck),
        struct(4, *tile),
        struct(2, NUM_TERMS, ci, ck),
        struct(4, *tile),
        struct(4, *tile),
        struct(8, *tile),
    )
    arrays = (vel, sca, pos, mot, row(heat), row(size), row(li), row(lj), row(lk))
    parts = pl.pallas_call(
        functools.partial(kernel, counts),
        out_shape=results,
        in_specs=[hbm] * len(arrays) + [pl.BlockSpec(memory_space=pltpu.SMEM)],
        out_specs=(vmem,) * len(results),
        scratch_shapes=scratch,
        compiler_params=pltpu.CompilerParams(
            collective_id=0, has_side_effects=True, vmem_limit_bytes=32 * 2**20
        ),
    )(*[pin(value) for value in arrays], tally)
    return pl.pallas_call(
        finish,
        out_shape=results[0:2],
        in_specs=[vmem] * len(results),
        out_specs=(pl.BlockSpec(memory_space=pl.ANY),) * 2,
        scratch_shapes=[
            f32(NUM_TERMS, ci, cj, ck),
            pltpu.SemaphoreType.DMA((NUM_TERMS + 1,)),
        ],
        compiler_params=pltpu.CompilerParams(vmem_limit_bytes=12 * 2**20),
    )(*parts)


def solution(mesh):
    bricks = P(None, AXES[0], AXES[1], AXES[2])
    rows = P(None, AXES)
    flat = P(AXES)
    counts = tuple(mesh.shape[axis] for axis in AXES)
    return jax.shard_map(
        functools.partial(local, counts),
        mesh=mesh,
        in_specs=(bricks, bricks, rows, rows) + (flat,) * 6,
        out_specs=(bricks, rows),
        check_vma=False,
    )
```
